8 devices in a mesh: part: 1 (over z), loc: 2 (over y), grp: 4 (over x, core).
Axes of the slice: x: 2, y: 2, z: 1, core: 2. Of those that a mesh axis runs over, the one named last changes fastest.
Arguments:
- x_tok: bfloat16 [1024, 1280], P(('part', 'grp', 'loc'))
- expert_ids: int32 [1024, 6], P(('part', 'grp', 'loc'))
- gate_val: float32 [1024, 6], P(('part', 'grp', 'loc'))
- w_gate: bfloat16 [160, 1280, 384], P(('grp', 'loc'))
- w_up: bfloat16 [160, 1280, 384], P(('grp', 'loc'))
- w_down: bfloat16 [160, 384, 1280], P(('grp', 'loc'))
Outputs:
- output: bfloat16 [1024, 1280], P(('part', 'grp', 'loc'))
All inputs are finite; a program needn't handle non-finite values.
Results may differ from the reference program's by a relative error of at most 0.0117378.
Values are sent between devices in bfloat16 or wider.
A program may use at most 1 GiB of HBM per device.

```python
import jax
import jax.numpy as jnp
from jax import lax

D = 1280
FF = 384
EXPERTS = 160
TOP = 6
MAXG = 3
TOK_DEV = 128
GROUPS = 4
LOCS = 2

TOKENS = TOK_DEV * GROUPS * LOCS
PER_GROUP = EXPERTS // GROUPS
HIT_GROUPS = min(MAXG, GROUPS)
PER_HIT = TOP // HIT_GROUPS
CAP = 8 * (TOKENS * TOP // (4 * EXPERTS) + 1)
HOT_TOKENS = min(TOKENS, CAP * PER_GROUP // PER_HIT)


def draw_routing(route_key):
    key_grp, key_tok, key_exp = jax.random.split(route_key, 3)
    grp_order = jax.random.permutation(key_grp, GROUPS)
    tok_rank = jnp.arange(TOKENS)
    has_hot = tok_rank < HOT_TOKENS
    seq_base = jnp.where(has_hot, tok_rank * (HIT_GROUPS - 1), HOT_TOKENS * (HIT_GROUPS - 1) + (tok_rank - HOT_TOKENS) * HIT_GROUPS)
    choice = jnp.arange(HIT_GROUPS)
    other_pos = seq_base[:, None] + choice[None, :] - has_hot[:, None].astype(jnp.int32)
    other_grp = grp_order[1 + other_pos % (GROUPS - 1)]
    chosen = jnp.where(has_hot[:, None] & (choice[None, :] == 0), grp_order[0], other_grp)
    member = jnp.sum((chosen[:, :, None] == jnp.arange(GROUPS)[None, None, :]).astype(jnp.int32), axis=1)
    before = jnp.cumsum(member, axis=0) - member
    order_in = jnp.take_along_axis(before, chosen, axis=1)[:, :, None]
    pick_ids = jnp.arange(PER_HIT)[None, None, :]
    is_hot = (chosen == grp_order[0])[:, :, None]
    hot_seq = jnp.where(order_in < CAP, order_in * (PER_HIT - 1) + pick_ids - 1, CAP * (PER_HIT - 1) + (order_in - CAP) * PER_HIT + pick_ids)
    hot_slot = jnp.where((order_in < CAP) & (pick_ids == 0), 0, 1 + hot_seq % (PER_GROUP - 1))
    cold_slot = (order_in * PER_HIT + pick_ids) % PER_GROUP
    slot_pos = jnp.where(is_hot, hot_slot, cold_slot)
    grp_perm = jax.vmap(lambda sub_key: jax.random.permutation(sub_key, PER_GROUP))(jax.random.split(key_exp, GROUPS))
    local_ids = grp_perm[chosen[:, :, None], slot_pos]
    experts = (chosen[:, :, None] * PER_GROUP + local_ids).reshape(TOKENS, TOP)
    shuffle = jax.random.permutation(key_tok, TOKENS)
    return experts[shuffle].astype(jnp.int32)


def setup_inputs(seed: int = 0, part: int = 0) -> dict:
    root_key = jax.random.key(seed)
    key_part = jax.random.fold_in(root_key, part)
    key_x, key_route, key_gate = jax.random.split(key_part, 3)
    key_one, key_two, key_three = jax.random.split(jax.random.key(seed + 7919), 3)
    x_tok = jax.random.normal(key_x, (TOKENS, D), jnp.float32).astype(jnp.bfloat16)
    expert_ids = draw_routing(key_route)
    gate_val = jax.random.uniform(key_gate, (TOKENS, TOP), jnp.float32, 0.5, 1.5) * TOP ** -0.5
    w_gate = (jax.random.normal(key_one, (EXPERTS, D, FF), jnp.float32) * D ** -0.5).astype(jnp.bfloat16)
    w_up = (jax.random.normal(key_two, (EXPERTS, D, FF), jnp.float32) * D ** -0.5).astype(jnp.bfloat16)
    w_down = (jax.random.normal(key_three, (EXPERTS, FF, D), jnp.float32) * FF ** -0.5).astype(jnp.bfloat16)
    return {"x_tok": x_tok, "expert_ids": expert_ids, "gate_val": gate_val, "w_gate": w_gate, "w_up": w_up, "w_down": w_down}


def reference(x_tok, expert_ids, gate_val, w_gate, w_up, w_down):
    n_slots = TOKENS * TOP
    flat_ids = expert_ids.reshape(-1)
    sort_order = jnp.argsort(flat_ids, stable=True)
    sorted_ids = flat_ids[sort_order]
    counts = jnp.bincount(flat_ids, length=EXPERTS)
    starts = jnp.cumsum(counts) - counts
    slot_ids = sorted_ids * CAP + jnp.arange(n_slots) - starts[sorted_ids]
    src_tok = jnp.zeros(EXPERTS * CAP, jnp.int32).at[slot_ids].set((sort_order // TOP).astype(jnp.int32))
    src_gate = jnp.zeros(EXPERTS * CAP, jnp.float32).at[slot_ids].set(gate_val.reshape(-1)[sort_order])
    stacked = (src_tok.reshape(GROUPS, PER_GROUP, CAP), src_gate.reshape(GROUPS, PER_GROUP, CAP), w_gate.reshape(GROUPS, PER_GROUP, D, FF), w_up.reshape(GROUPS, PER_GROUP, D, FF), w_down.reshape(GROUPS, PER_GROUP, FF, D))

    def expert_step(group_acc, expert_in):
        tok_rows, row_gate, w_one, w_two, w_three = expert_in
        picked_rows = x_tok[tok_rows]
        up_gate = jnp.dot(picked_rows, w_one, preferred_element_type=jnp.float32)
        up_lin = jnp.dot(picked_rows, w_two, preferred_element_type=jnp.float32)
        hidden = (jax.nn.silu(up_gate) * up_lin).astype(jnp.bfloat16)
        out_rows = jnp.dot(hidden, w_three, preferred_element_type=jnp.float32)
        return group_acc.at[tok_rows].add(out_rows * row_gate[:, None]), None

    def group_step(y_acc, group_in):
        zero_acc = jnp.zeros((TOKENS, D), jnp.float32)
        group_sum = lax.scan(expert_step, zero_acc, group_in)[0]
        return y_acc + group_sum.astype(jnp.bfloat16).astype(jnp.float32), None

    y_sum = lax.scan(group_step, jnp.zeros((TOKENS, D), jnp.float32), stacked)[0]
    return y_sum.astype(jnp.bfloat16)
```

```python
import functools

import jax
import jax.numpy as jnp
from jax import lax
from jax.experimental import pallas as pl
from jax.experimental.pallas import tpu as pltpu
from jax.sharding import PartitionSpec as P

F32 = jnp.float32
BF16 = jnp.bfloat16
PACK = 5


def moe_kernel(dims, x_ref, meta_ref, wg_ref, wu_ref, wd_ref, y_ref,
               x_all, meta_all, pos_ref, ge_ref, cols_ref, gate_ref, oh_ref, packed, osp, q_ref,
               s_ref, h_ref, r_ref, gp_ref, parts, wgu, wdn,
               w_sem, xs_sem, xr_sem, ms_sem, mr_sem, ss_sem, rr_sem, gs_sem, pr_sem):
    n_loc, n_grp, n_exp, cap, top_k, n_slot = dims
    tok, d_model = x_ref.shape
    half = tok // 2
    ff = wg_ref.shape[2]
    n_dev = n_loc * n_grp
    n_tok = tok * n_dev
    rows = n_exp * cap
    l = lax.axis_index("loc")
    g = lax.axis_index("grp")
    gx, gc = g // 2, g % 2

    def rel(fx, fc, fl):
        return ((gx + fx) % 2) * 2 + (gc + fc) % 2, (l + fl) % 2

    def dev(fx, fc, fl):
        gg, ll = rel(fx, fc, fl)
        return {"grp": gg, "loc": ll}

    def block_of(fx, fc, fl):
        gg, ll = rel(fx, fc, fl)
        return gg * n_loc + ll

    def weight_copies(e, slot):
        return (
            pltpu.make_async_copy(wg_ref.at[e], wgu.at[slot, :, pl.ds(0, ff)], w_sem.at[slot, 0]),
            pltpu.make_async_copy(wu_ref.at[e], wgu.at[slot, :, pl.ds(ff, ff)], w_sem.at[slot, 1]),
            pltpu.make_async_copy(wd_ref.at[e], wdn.at[slot], w_sem.at[slot, 2]),
        )

    def start_weights(e, carry):
        for copy in weight_copies(e, e):
            copy.start()
        return carry

    lax.fori_loop(0, n_slot, start_weights, 0)

    rels = [(fx, fc, fl) for fx in (0, 1) for fc in (0, 1) for fl in (0, 1)][1:]
    barrier = pltpu.get_barrier_semaphore()
    for r in rels:
        pl.semaphore_signal(barrier, inc=1, device_id=dev(*r), device_id_type=pl.DeviceIdType.MESH)
    pl.semaphore_wait(barrier, len(rels))

    me = block_of(0, 0, 0)
    meta_all[me] = meta_ref[...]
    pending = []

    def send(src, dst, s_sem, r_sem, to):
        copy = pltpu.make_async_remote_copy(
            src_ref=src, dst_ref=dst, send_sem=s_sem, recv_sem=r_sem,
            device_id=dev(*to), device_id_type=pl.DeviceIdType.MESH)
        copy.start()
        pending.append(copy)
        return copy

    metas = [send(meta_ref, meta_all.at[me], ms_sem.at[i], mr_sem.at[i], r) for i, r in enumerate(rels)]

    def x_rows(block, part):
        return x_all.at[pl.ds(pl.multiple_of(block * tok + part * half, half), half), :]

    def r_idx(r):
        return r[0] * 4 + r[1] * 2 + r[2]

    XN, YN, PC, DG = (1, 0, 0), (0, 0, 1), (0, 1, 0), (1, 0, 1)
    n_sent = [0]

    def send_x(src, block, part, to, at):
        i = n_sent[0]
        n_sent[0] += 1
        return send(src, x_rows(block, part), xs_sem.at[i], xr_sem.at[r_idx(at) * 2 + part], to)

    def own(part):
        return x_ref.at[pl.ds(part * half, half), :]

    got = {}
    got[XN, 0] = send_x(own(0), me, 0, XN, XN)
    got[YN, 1] = send_x(own(1), me, 1, YN, YN)
    got[XN, 1] = send_x(own(1), me, 1, XN, XN)
    got[YN, 0] = send_x(own(0), me, 0, YN, YN)
    got[PC, 0] = send_x(own(0), me, 0, PC, PC)
    got[PC, 1] = send_x(own(1), me, 1, PC, PC)
    x_all[pl.ds(pl.multiple_of(me * tok, tok), tok), :] = x_ref[...]

    for copy in metas:
        copy.wait_recv()

    ids_t = jnp.concatenate([meta_all[d, 0:8, :] for d in range(n_dev)], axis=1)
    gts_t = jnp.concatenate([meta_all[d, 8:16, :] for d in range(n_dev)], axis=1)
    e_rows = 32
    e_iota = lax.broadcasted_iota(jnp.int32, (e_rows, n_tok), 0)
    e_ids = jnp.where(e_iota < n_exp, e_iota + me * n_exp, -5).astype(F32)
    mask = jnp.zeros((e_rows, n_tok), F32)
    gate_e = jnp.zeros((e_rows, n_tok), F32)
    for j in range(top_k):
        eq = ids_t[j:j + 1, :] == e_ids
        mask = mask + jnp.where(eq, 1.0, 0.0)
        gate_e = gate_e + jnp.where(eq, gts_t[j:j + 1, :], 0.0)
    blocks = [mask[:, d * tok:(d + 1) * tok] for d in range(n_dev)]
    tri = (lax.broadcasted_iota(jnp.int32, (tok, tok), 0) < lax.broadcasted_iota(jnp.int32, (tok, tok), 1))
    tri = jnp.where(tri, 1.0, 0.0).astype(BF16)
    prefix = jnp.dot(jnp.concatenate(blocks, axis=0).astype(BF16), tri, preferred_element_type=F32)
    offset = jnp.zeros((e_rows, 1), F32)
    pos = []
    for d in range(n_dev):
        pos.append(prefix[d * e_rows:(d + 1) * e_rows, :] + offset)
        offset = offset + jnp.sum(blocks[d], axis=1, keepdims=True)
    pos = jnp.concatenate(pos, axis=1)
    pos_ref[...] = jnp.where(mask > 0.0, pos, -1.0)
    ge_ref[...] = gate_e
    slot_id = e_iota.astype(F32) * float(cap) + pos + 1.0
    slot_rows = [jnp.sum(jnp.where(ids_t[j:j + 1, :] == e_ids, slot_id, 0.0), axis=0, keepdims=True) - 1.0
                 for j in range(top_k)]
    slot_rows += [jnp.full((1, n_tok), -1.0, F32)] * (8 - top_k)
    slot_t = jnp.concatenate(slot_rows, axis=0)
    for d in range(n_dev):
        cols_ref[pl.ds(d * tok, tok), :] = jnp.transpose(slot_t[:, d * tok:(d + 1) * tok])

    def forward(at, part, hops):
        block = block_of(*at)
        for to, seen_as in hops:
            got[seen_as, part] = send_x(x_rows(block, part), block, part, to, seen_as)

    def landed(at, part):
        got[at, part].wait_recv()

    PX, PY, PD = (1, 1, 0), (0, 1, 1), (1, 1, 1)
    landed(XN, 0)
    forward(XN, 0, [(YN, DG), (PC, PX)])
    landed(YN, 1)
    forward(YN, 1, [(XN, DG), (PC, PY)])
    landed(XN, 1)
    forward(XN, 1, [(PC, PX)])
    landed(YN, 0)
    forward(YN, 0, [(PC, PY)])
    landed(DG, 0)
    forward(DG, 0, [(PC, PD)])
    landed(DG, 1)
    forward(DG, 1, [(PC, PD)])
    for at in (PC, PX, PY, PD):
        for part in (0, 1):
            landed(at, part)

    step = 256

    def pack(p, carry):
        for i in range(PACK):
            e = p * PACK + i
            where = lax.broadcasted_iota(jnp.int32, (cap, n_tok), 0).astype(F32) == pos_ref[pl.ds(e, 1), :]
            oh_ref[pl.ds(i * cap, cap), :] = jnp.where(where, 1.0, 0.0).astype(BF16)
            gate_ref[pl.ds(pl.multiple_of(e * cap, 16), cap), :] = jnp.sum(
                jnp.where(where, ge_ref[pl.ds(e, 1), :], 0.0), axis=1, keepdims=True)
        base = pl.multiple_of(p * (PACK * cap), 16)
        for n in range(d_model // step):
            cols = pl.ds(n * step, step)
            packed[pl.ds(base, PACK * cap), cols] = jnp.dot(
                oh_ref[...], x_all[:, cols], preferred_element_type=F32).astype(BF16)
        return carry

    lax.fori_loop(0, n_exp // PACK, pack, 0)

    def expert(e, carry):
        slot = e % n_slot
        for copy in weight_copies(e, slot):
            copy.wait()
        at = pl.ds(pl.multiple_of(e * cap, 16), cap)
        uv = jnp.dot(packed[at, :], wgu[slot], preferred_element_type=F32)
        hid = (jax.nn.silu(uv[:, :ff]) * uv[:, ff:]).astype(BF16)
        out = jnp.dot(hid, wdn[slot], preferred_element_type=F32) * gate_ref[at, :]
        hi = out.astype(BF16)
        rest = out - hi.astype(F32)
        mid = rest.astype(BF16)
        osp[0, at, :] = hi
        osp[1, at, :] = mid
        osp[2, at, :] = (rest - mid.astype(F32)).astype(BF16)

        @pl.when(e + n_slot < n_exp)
        def _():
            for copy in weight_copies(e + n_slot, slot):
                copy.start()
        return carry

    lax.fori_loop(0, n_exp, expert, 0)

    def combine(block, dst):
        cols = cols_ref[pl.ds(pl.multiple_of(block * tok, tok), tok), :]
        lanes = lax.broadcasted_iota(jnp.int32, (tok, rows), 1).astype(F32)
        hit = cols[:, 0:1] == lanes
        for j in range(1, top_k):
            hit = hit | (cols[:, j:j + 1] == lanes)
        q_ref[...] = jnp.where(hit, 1.0, 0.0).astype(BF16)
        for n in range(d_model // step):
            at = pl.ds(n * step, step)
            total = jnp.dot(q_ref[...], osp[0, :, at], preferred_element_type=F32)
            total += jnp.dot(q_ref[...], osp[1, :, at], preferred_element_type=F32)
            total += jnp.dot(q_ref[...], osp[2, :, at], preferred_element_type=F32)
            dst[:, at] = total

    def home_grp(k):
        fx = 1 - k // 2
        fc = ((k + 1) // 2) % 2
        return ((gx + fx) % 2) * 2 + (gc + fc) % 2

    def y_copy(k):
        return pltpu.make_async_remote_copy(
            src_ref=s_ref.at[k], dst_ref=r_ref.at[k], send_sem=ss_sem.at[k], recv_sem=rr_sem.at[k],
            device_id=dev(*YN), device_id_type=pl.DeviceIdType.MESH)

    def away(k, carry):
        combine(home_grp(k) * n_loc + (1 - l), s_ref.at[k])
        y_copy(k).start()
        return carry

    def home(k, carry):
        combine(home_grp(k) * n_loc + l, h_ref.at[k])
        return carry

    lax.fori_loop(0, n_grp, away, 0)
    lax.fori_loop(0, n_grp, home, 0)

    flips = [(1, 0, 0), (1, 1, 0), (0, 1, 0)]
    returns = []
    for k in range(n_grp):
        y_copy(k).wait_recv()
        part = (h_ref[k] + r_ref[k]).astype(BF16)
        if k < 3:
            gp_ref[k] = part
            returns.append(send(gp_ref.at[k], parts.at[k], gs_sem.at[k], pr_sem.at[k], flips[k]))
        else:
            parts[k] = part
    for copy in returns:
        copy.wait_recv()
    total = parts[0].astype(F32)
    for k in range(1, n_grp):
        total = total + parts[k].astype(F32)
    y_ref[...] = total.astype(BF16)
    for copy in pending:
        copy.wait_send()
    for k in range(n_grp):
        y_copy(k).wait_send()


def solution(mesh):
    n_grp = mesh.shape["grp"]
    n_loc = mesh.shape["loc"]
    tok_spec = P(("part", "grp", "loc"), None)
    w_spec = P(("grp", "loc"), None, None)

    def device_step(x_tok, expert_ids, gate_val, w_gate, w_up, w_down):
        tok, d_model = x_tok.shape
        top_k = expert_ids.shape[1]
        n_exp, _, ff = w_gate.shape
        n_dev = n_grp * n_loc
        n_tok = tok * n_dev
        cap = 8 * (n_tok * top_k // (4 * n_exp * n_dev) + 1)
        rows = n_exp * cap
        n_slot = 9
        meta = jnp.zeros((16, tok), F32)
        meta = meta.at[0:top_k].set(expert_ids.T.astype(F32)).at[8:8 + top_k].set(gate_val.T)
        vmem = pltpu.VMEM
        dma = pltpu.SemaphoreType.DMA
        dims = (n_loc, n_grp, n_exp, cap, top_k, n_slot)
        return pl.pallas_call(
            functools.partial(moe_kernel, dims),
            out_shape=jax.ShapeDtypeStruct((tok, d_model), BF16),
            in_specs=[pl.BlockSpec(memory_space=vmem)] * 2 + [pl.BlockSpec(memory_space=pl.ANY)] * 3,
            out_specs=pl.BlockSpec(memory_space=vmem),
            scratch_shapes=[
                vmem((n_tok, d_model), BF16),
                vmem((n_dev, 16, tok), F32),
                vmem((32, n_tok), F32),
                vmem((32, n_tok), F32),
                vmem((n_tok, 8), F32),
                vmem((rows, 1), F32),
                vmem((PACK * cap, n_tok), BF16),
                vmem((rows, d_model), BF16),
                vmem((3, rows, d_model), BF16),
                vmem((tok, rows), BF16),
                vmem((n_grp, tok, d_model), F32),
                vmem((n_grp, tok, d_model), F32),
                vmem((n_grp, tok, d_model), F32),
                vmem((n_grp, tok, d_model), BF16),
                vmem((n_grp, tok, d_model), BF16),
                vmem((n_slot, d_model, 2 * ff), BF16),
                vmem((n_slot, ff, d_model), BF16),
                dma((n_slot, 3)),
                dma((14,)),
                dma((16,)),
                dma((7,)),
                dma((7,)),
                dma((n_grp,)),
                dma((n_grp,)),
                dma((n_grp,)),
                dma((n_grp,)),
            ],
            compiler_params=pltpu.CompilerParams(
                collective_id=0, has_side_effects=True, vmem_limit_bytes=67043328),
            name="moe",
        )(x_tok, meta, w_gate, w_up, w_down)

    return jax.shard_map(device_step, mesh=mesh, in_specs=(tok_spec, tok_spec, tok_spec, w_spec, w_spec, w_spec), out_specs=tok_spec, check_vma=False)
```

```python
import functools

import jax
import jax.numpy as jnp
from jax import lax
from jax.experimental import pallas as pl
from jax.experimental.pallas import tpu as pltpu
from jax.sharding import PartitionSpec as P

F32 = jnp.float32
BF16 = jnp.bfloat16
PACK = 5


YN, YP, DG, DP = (0, 0, 1), (0, 1, 1), (1, 0, 1), (1, 1, 1)
XN, XP, ME, PC = (1, 0, 0), (1, 1, 0), (0, 0, 0), (0, 1, 0)
ORDER = [YN, YP, DG, DP, XN, XP, ME, PC]


def flip(a, b):
    return tuple((i + j) % 2 for i, j in zip(a, b))


def moe_kernel(dims, x_ref, meta_ref, wg_ref, wu_ref, wd_ref, y_ref,
               x_all, meta_all, pos_ref, ge_ref, cols_ref, gate_ref, oh_ref, packed, osp, q_ref,
               c_ref, d_ref, rf_ref, rs_ref, gp_ref, gx_ref, wgu, wdn,
               w_sem, xs_sem, xr_sem, ms_sem, mr_sem, ds_sem, dr_sem, ts_sem, tr_sem):
    n_loc, n_grp, n_exp, cap, top_k, n_slot = dims
    tok, d_model = x_ref.shape
    half = tok // 2
    ff = wg_ref.shape[2]
    n_dev = n_loc * n_grp
    n_tok = tok * n_dev
    rows = n_exp * cap
    l = lax.axis_index("loc")
    g = lax.axis_index("grp")
    gx, gc = g // 2, g % 2

    def dev(to):
        fx, fc, fl = to
        return {"grp": ((gx + fx) % 2) * 2 + (gc + fc) % 2, "loc": (l + fl) % 2}

    def weight_copies(e, slot):
        return (
            pltpu.make_async_copy(wg_ref.at[e], wgu.at[slot, :, pl.ds(0, ff)], w_sem.at[slot, 0]),
            pltpu.make_async_copy(wu_ref.at[e], wgu.at[slot, :, pl.ds(ff, ff)], w_sem.at[slot, 1]),
            pltpu.make_async_copy(wd_ref.at[e], wdn.at[slot], w_sem.at[slot, 2]),
        )

    def start_weights(e, carry):
        for copy in weight_copies(e, e):
            copy.start()
        return carry

    lax.fori_loop(0, n_slot, start_weights, 0)

    peers = [r for r in ORDER if r != ME]
    barrier = pltpu.get_barrier_semaphore()
    for r in peers:
        pl.semaphore_signal(barrier, inc=1, device_id=dev(r), device_id_type=pl.DeviceIdType.MESH)
    pl.semaphore_wait(barrier, len(peers))

    pending = []

    def send(src, dst, s_sem, r_sem, to):
        copy = pltpu.make_async_remote_copy(
            src_ref=src, dst_ref=dst, send_sem=s_sem, recv_sem=r_sem,
            device_id=dev(to), device_id_type=pl.DeviceIdType.MESH)
        copy.start()
        pending.append(copy)
        return copy

    metas = [send(meta_ref, meta_all.at[ORDER.index(r)], ms_sem.at[i], mr_sem.at[i], r) for i, r in enumerate(peers)]

    def x_rows(at, part):
        return x_all.at[pl.ds(ORDER.index(at) * tok + part * half, half), :]

    got = {}

    def send_x(src, part, to, at):
        i = len(got)
        got[at, part] = send(src, x_rows(at, part), xs_sem.at[i], xr_sem.at[ORDER.index(at) * 2 + part], to)

    for part, to in ((0, XN), (1, YN), (1, XN), (0, YN), (0, PC), (1, PC)):
        send_x(x_ref.at[pl.ds(part * half, half), :], part, to, to)
    x_all[pl.ds(ORDER.index(ME) * tok, tok), :] = x_ref[...]
    meta_all[ORDER.index(ME)] = meta_ref[...]

    for copy in metas:
        copy.wait_recv()

    ids_t = jnp.concatenate([meta_all[d, 0:8, :] for d in range(n_dev)], axis=1)
    gts_t = jnp.concatenate([meta_all[d, 8:16, :] for d in range(n_dev)], axis=1)
    e_rows = 32
    e_iota = lax.broadcasted_iota(jnp.int32, (e_rows, n_tok), 0)
    e_ids = jnp.where(e_iota < n_exp, e_iota + (g * n_loc + l) * n_exp, -5).astype(F32)
    mask = jnp.zeros((e_rows, n_tok), F32)
    gate_e = jnp.zeros((e_rows, n_tok), F32)
    for j in range(top_k):
        eq = ids_t[j:j + 1, :] == e_ids
        mask = mask + jnp.where(eq, 1.0, 0.0)
        gate_e = gate_e + jnp.where(eq, gts_t[j:j + 1, :], 0.0)
    blocks = [mask[:, d * tok:(d + 1) * tok] for d in range(n_dev)]
    tri = (lax.broadcasted_iota(jnp.int32, (tok, tok), 0) < lax.broadcasted_iota(jnp.int32, (tok, tok), 1))
    tri = jnp.where(tri, 1.0, 0.0).astype(BF16)
    prefix = jnp.dot(jnp.concatenate(blocks, axis=0).astype(BF16), tri, preferred_element_type=F32)
    offset = jnp.zeros((e_rows, 1), F32)
    pos = []
    for d in range(n_dev):
        pos.append(prefix[d * e_rows:(d + 1) * e_rows, :] + offset)
        offset = offset + jnp.sum(blocks[d], axis=1, keepdims=True)
    pos = jnp.concatenate(pos, axis=1)
    pos_ref[...] = jnp.where(mask > 0.0, pos, -1.0)
    ge_ref[...] = gate_e
    slot_id = e_iota.astype(F32) * float(cap) + pos + 1.0
    slot_rows = [jnp.sum(jnp.where(ids_t[j:j + 1, :] == e_ids, slot_id, 0.0), axis=0, keepdims=True) - 1.0
                 for j in range(top_k)]

    def group_hit(grp):
        low = (lax.broadcasted_iota(jnp.int32, (1, n_tok), 1) * 0 + grp * (n_loc * n_exp)).astype(F32)
        hit = jnp.zeros((1, n_tok), F32)
        for j in range(top_k):
            inside = (ids_t[j:j + 1, :] >= low) & (ids_t[j:j + 1, :] < low + float(n_loc * n_exp))
            hit = jnp.where(inside, 1.0, hit)
        return hit

    own_hit = group_hit(g)
    slot_rows += [own_hit, own_hit * group_hit(gx * 2 + (gc + 1) % 2)]
    slot_t = jnp.concatenate(slot_rows, axis=0)
    for d in range(n_dev):
        cols_ref[pl.ds(d * tok, tok), :] = jnp.transpose(slot_t[:, d * tok:(d + 1) * tok])

    def forward(at, part, hops):
        for to in hops:
            send_x(x_rows(at, part), part, to, flip(at, to))

    def landed(at, part):
        got[at, part].wait_recv()

    landed(XN, 0)
    forward(XN, 0, [YN, PC])
    landed(YN, 1)
    forward(YN, 1, [XN, PC])
    landed(XN, 1)
    forward(XN, 1, [PC])
    landed(YN, 0)
    forward(YN, 0, [PC])
    landed(YP, 0)
    landed(YP, 1)

    step = 256

    def run_pass(number, first, count):
        toks = pl.ds(first, count)

        def pack(p, carry):
            for i in range(PACK):
                e = p * PACK + i
                where = lax.broadcasted_iota(jnp.int32, (cap, count), 0).astype(F32) == pos_ref[pl.ds(e, 1), toks]
                oh_ref[pl.ds(i * cap, cap), pl.ds(0, count)] = jnp.where(where, 1.0, 0.0).astype(BF16)
                gate_ref[pl.ds(pl.multiple_of(e * cap, 16), cap), :] = jnp.sum(
                    jnp.where(where, ge_ref[pl.ds(e, 1), toks], 0.0), axis=1, keepdims=True)
            base = pl.multiple_of(p * (PACK * cap), 16)
            for n in range(d_model // step):
                cols = pl.ds(n * step, step)
                packed[pl.ds(base, PACK * cap), cols] = jnp.dot(
                    oh_ref[:, pl.ds(0, count)], x_all[toks, cols], preferred_element_type=F32).astype(BF16)
            return carry

        lax.fori_loop(0, n_exp // PACK, pack, 0)

        def expert(e, carry):
            turn = e + number * n_exp
            slot = turn % n_slot
            for copy in weight_copies(e, slot):
                copy.wait()
            at = pl.ds(pl.multiple_of(e * cap, 16), cap)
            uv = jnp.dot(packed[at, :], wgu[slot], preferred_element_type=F32)
            hid = (jax.nn.silu(uv[:, :ff]) * uv[:, ff:]).astype(BF16)
            out = jnp.dot(hid, wdn[slot], preferred_element_type=F32) * gate_ref[at, :]
            hi = out.astype(BF16)
            rest = out - hi.astype(F32)
            mid = rest.astype(BF16)
            osp[0, at, :] = hi
            osp[1, at, :] = mid
            osp[2, at, :] = (rest - mid.astype(F32)).astype(BF16)

            @pl.when(turn + n_slot < 2 * n_exp)
            def _():
                for copy in weight_copies((turn + n_slot) % n_exp, slot):
                    copy.start()
            return carry

        lax.fori_loop(0, n_exp, expert, 0)

    def combine(blk):
        cols = cols_ref[pl.ds(pl.multiple_of(blk * tok, tok), tok), :]
        lanes = lax.broadcasted_iota(jnp.int32, (tok, rows), 1).astype(F32)
        hit = cols[:, 0:1] == lanes
        for j in range(1, top_k):
            hit = hit | (cols[:, j:j + 1] == lanes)
        q_ref[...] = jnp.where(hit, 1.0, 0.0).astype(BF16)
        for n in range(d_model // step):
            at = pl.ds(n * step, step)
            total = jnp.dot(q_ref[...], osp[0, :, at], preferred_element_type=F32)
            total += jnp.dot(q_ref[...], osp[1, :, at], preferred_element_type=F32)
            total += jnp.dot(q_ref[...], osp[2, :, at], preferred_element_type=F32)
            c_ref[blk, :, at] = total

    def swap_copy(h):
        return pltpu.make_async_remote_copy(
            src_ref=c_ref.at[2 * h + 1], dst_ref=d_ref.at[h], send_sem=ds_sem.at[h], recv_sem=dr_sem.at[h],
            device_id=dev(PC), device_id_type=pl.DeviceIdType.MESH)

    def combine_loop(count, pick):
        def body(i, carry):
            blk = pick(i)
            combine(blk)

            @pl.when(blk % 2 == 1)
            def _():
                swap_copy(blk // 2).start()
            return carry

        lax.fori_loop(0, count, body, 0)

    def split_rows(h):
        swap_copy(h).wait_recv()
        cols = cols_ref[pl.ds(2 * h * tok, tok), :]
        mine = c_ref[2 * h]
        other = d_ref[h]
        c_ref[2 * h] = jnp.where(cols[:, 6:7] > 0.5, mine, other)
        d_ref[h] = jnp.where(cols[:, 7:8] > 0.5, other, 0.0)

    def ship(i, src, dst, to):
        return send(src, dst, ts_sem.at[i], tr_sem.at[i], to)

    run_pass(0, 0, 2 * tok)
    landed(DG, 0)
    forward(DG, 0, [PC])
    landed(DG, 1)
    forward(DG, 1, [PC])
    combine_loop(2, lambda i: 1 - i)
    split_rows(0)
    first_own = ship(0, c_ref.at[0], rf_ref.at[0], YN)

    for at in (XP, PC, DP):
        landed(at, 0)
        landed(at, 1)
    run_pass(1, 2 * tok, n_tok - 2 * tok)
    combine_loop(2, lambda i: 3 - i)
    split_rows(1)
    first_far = ship(1, c_ref.at[2], rf_ref.at[1], YN)
    hop = ship(2, d_ref.at[1], rs_ref.at[0], XN)
    combine_loop(4, lambda i: 5 + 2 * i - (i // 2) * 5)
    hop.wait_recv()
    d_ref[0] = d_ref[0] + rs_ref[0]
    second = ship(3, d_ref.at[0], rs_ref.at[1], YN)
    split_rows(2)
    far_second = ship(4, d_ref.at[2], rs_ref.at[2], XN)
    split_rows(3)

    first_own.wait_recv()
    total = (c_ref[6] + rf_ref[0]).astype(BF16).astype(F32)
    c_ref[6] = total
    first_far.wait_recv()
    gp_ref[...] = (c_ref[4] + rf_ref[1]).astype(BF16)
    far_first = ship(5, gp_ref, gx_ref, XN)
    far_second.wait_recv()
    d_ref[3] = d_ref[3] + rs_ref[2]
    far_first.wait_recv()
    c_ref[6] = c_ref[6] + gx_ref[...].astype(F32)
    second.wait_recv()
    y_ref[...] = (c_ref[6] + (d_ref[3] + rs_ref[1]).astype(BF16).astype(F32)).astype(BF16)
    for copy in pending:
        copy.wait_send()
    for h in range(n_dev // 2):
        swap_copy(h).wait_send()


def solution(mesh):
    n_grp = mesh.shape["grp"]
    n_loc = mesh.shape["loc"]
    tok_spec = P(("part", "grp", "loc"), None)
    w_spec = P(("grp", "loc"), None, None)

    def device_step(x_tok, expert_ids, gate_val, w_gate, w_up, w_down):
        tok, d_model = x_tok.shape
        top_k = expert_ids.shape[1]
        n_exp, _, ff = w_gate.shape
        n_dev = n_grp * n_loc
        n_tok = tok * n_dev
        cap = 8 * (n_tok * top_k // (4 * n_exp * n_dev) + 1)
        rows = n_exp * cap
        n_slot = 9
        blank = jnp.zeros((tok, 8 - top_k), F32)
        meta = jnp.concatenate([expert_ids.astype(F32), blank, gate_val, blank], axis=1).T
        vmem = pltpu.VMEM
        dma = pltpu.SemaphoreType.DMA
        dims = (n_loc, n_grp, n_exp, cap, top_k, n_slot)
        return pl.pallas_call(
            functools.partial(moe_kernel, dims),
            out_shape=jax.ShapeDtypeStruct((tok, d_model), BF16),
            in_specs=[pl.BlockSpec(memory_space=vmem)] * 2 + [pl.BlockSpec(memory_space=pl.ANY)] * 3,
            out_specs=pl.BlockSpec(memory_space=vmem),
            scratch_shapes=[
                vmem((n_tok, d_model), BF16),
                vmem((n_dev, 16, tok), F32),
                vmem((32, n_tok), F32),
                vmem((32, n_tok), F32),
                vmem((n_tok, 8), F32),
                vmem((rows, 1), F32),
                vmem((PACK * cap, n_tok - 2 * tok), BF16),
                vmem((rows, d_model), BF16),
                vmem((3, rows, d_model), BF16),
                vmem((tok, rows), BF16),
                vmem((n_dev, tok, d_model), F32),
                vmem((n_dev // 2, tok, d_model), F32),
                vmem((2, tok, d_model), F32),
                vmem((3, tok, d_model), F32),
                vmem((tok, d_model), BF16),
                vmem((tok, d_model), BF16),
                vmem((n_slot, d_model, 2 * ff), BF16),
                vmem((n_slot, ff, d_model), BF16),
                dma((n_slot, 3)),
                dma((14,)),
                dma((16,)),
                dma((7,)),
                dma((7,)),
                dma((n_dev // 2,)),
                dma((n_dev // 2,)),
                dma((6,)),
                dma((6,)),
            ],
            compiler_params=pltpu.CompilerParams(
                collective_id=0, has_side_effects=True, vmem_limit_bytes=67043328),
            name="moe",
        )(x_tok, meta, w_gate, w_up, w_down)

    return jax.shard_map(device_step, mesh=mesh, in_specs=(tok_spec, tok_spec, tok_spec, w_spec, w_spec, w_spec), out_specs=tok_spec, check_vma=False)
```

```python
import functools

import jax
import jax.numpy as jnp
from jax import lax
from jax.experimental import pallas as pl
from jax.experimental.pallas import tpu as pltpu
from jax.sharding import PartitionSpec as P

F32 = jnp.float32
BF16 = jnp.bfloat16
PACK = 5
PAIR = 2


YN, YP, DG, DP = (0, 0, 1), (0, 1, 1), (1, 0, 1), (1, 1, 1)
XN, XP, ME, PC = (1, 0, 0), (1, 1, 0), (0, 0, 0), (0, 1, 0)
ORDER = [YN, YP, DG, DP, XN, XP, ME, PC]


def flip(a, b):
    return tuple((i + j) % 2 for i, j in zip(a, b))


def moe_kernel(dims, x_ref, ids_ref, gates_ref, wg_ref, wu_ref, wd_ref, y_ref,
               x_all, ids_all, gates_all, pos_ref, ge_ref, cols_ref, gate_ref, oh_ref, packed, hid_ref, osp, q_ref,
               c_ref, d_ref, rf_ref, rs_ref, gp_ref, gx_ref, wgu, wdn,
               w_sem, xs_sem, xr_sem, ms_sem, mr_sem, ds_sem, dr_sem, ts_sem, tr_sem):
    n_loc, n_grp, n_exp, cap, top_k, n_slot = dims
    tok, d_model = x_ref.shape
    half = tok // 2
    ff = wg_ref.shape[2]
    n_dev = n_loc * n_grp
    n_tok = tok * n_dev
    rows = n_exp * cap
    l = lax.axis_index("loc")
    g = lax.axis_index("grp")
    gx, gc = g // 2, g % 2

    def dev(to):
        fx, fc, fl = to
        return {"grp": ((gx + fx) % 2) * 2 + (gc + fc) % 2, "loc": (l + fl) % 2}

    def in_copies(e, slot):
        return (
            pltpu.make_async_copy(wg_ref.at[e], wgu.at[slot, :, pl.ds(0, ff)], w_sem.at[slot, 0]),
            pltpu.make_async_copy(wu_ref.at[e], wgu.at[slot, :, pl.ds(ff, ff)], w_sem.at[slot, 1]),
        )

    def out_copy(e, slot):
        return pltpu.make_async_copy(wd_ref.at[e], wdn.at[slot], w_sem.at[slot, 2])

    def start_weights(e, carry):
        for copy in in_copies(e, e):
            copy.start()
        out_copy(e, e).start()
        return carry

    lax.fori_loop(0, n_slot, start_weights, 0)

    peers = [r for r in ORDER if r != ME]
    barrier = pltpu.get_barrier_semaphore()
    for r in peers:
        pl.semaphore_signal(barrier, inc=1, device_id=dev(r), device_id_type=pl.DeviceIdType.MESH)
    pl.semaphore_wait(barrier, len(peers))

    pending = []

    def send(src, dst, s_sem, r_sem, to):
        copy = pltpu.make_async_remote_copy(
            src_ref=src, dst_ref=dst, send_sem=s_sem, recv_sem=r_sem,
            device_id=dev(to), device_id_type=pl.DeviceIdType.MESH)
        copy.start()
        pending.append(copy)
        return copy

    metas = []
    for i, r in enumerate(peers):
        for k, (src, dst) in enumerate(((ids_ref, ids_all), (gates_ref, gates_all))):
            metas.append(send(src, dst.at[ORDER.index(r)], ms_sem.at[i, k], mr_sem.at[i, k], r))

    def x_rows(at, part):
        return x_all.at[pl.ds(ORDER.index(at) * tok + part * half, half), :]

    got = {}

    def send_x(src, part, to, at):
        i = len(got)
        got[at, part] = send(src, x_rows(at, part), xs_sem.at[i], xr_sem.at[ORDER.index(at) * 2 + part], to)

    for part, to in ((0, XN), (1, YN), (1, XN), (0, YN), (0, PC), (1, PC)):
        send_x(x_ref.at[pl.ds(part * half, half), :], part, to, to)
    x_all[pl.ds(ORDER.index(ME) * tok, tok), :] = x_ref[...]
    ids_all[ORDER.index(ME)] = ids_ref[...]
    gates_all[ORDER.index(ME)] = gates_ref[...]

    for copy in metas:
        copy.wait_recv()

    ids_t = jnp.concatenate([ids_all[d] for d in range(n_dev)], axis=1).astype(F32)
    gts_t = jnp.concatenate([gates_all[d] for d in range(n_dev)], axis=1)
    e_rows = 32
    e_iota = lax.broadcasted_iota(jnp.int32, (e_rows, n_tok), 0)
    e_ids = jnp.where(e_iota < n_exp, e_iota + (g * n_loc + l) * n_exp, -5).astype(F32)
    mask = jnp.zeros((e_rows, n_tok), F32)
    gate_e = jnp.zeros((e_rows, n_tok), F32)
    for j in range(top_k):
        eq = ids_t[j:j + 1, :] == e_ids
        mask = mask + jnp.where(eq, 1.0, 0.0)
        gate_e = gate_e + jnp.where(eq, gts_t[j:j + 1, :], 0.0)
    blocks = [mask[:, d * tok:(d + 1) * tok] for d in range(n_dev)]
    tri = (lax.broadcasted_iota(jnp.int32, (tok, tok), 0) < lax.broadcasted_iota(jnp.int32, (tok, tok), 1))
    tri = jnp.where(tri, 1.0, 0.0).astype(BF16)
    prefix = jnp.dot(jnp.concatenate(blocks, axis=0).astype(BF16), tri, preferred_element_type=F32)
    offset = jnp.zeros((e_rows, 1), F32)
    pos = []
    for d in range(n_dev):
        pos.append(prefix[d * e_rows:(d + 1) * e_rows, :] + offset)
        offset = offset + jnp.sum(blocks[d], axis=1, keepdims=True)
    pos = jnp.concatenate(pos, axis=1)
    pos_ref[...] = jnp.where(mask > 0.0, pos, -1.0)
    ge_ref[...] = gate_e
    slot_id = e_iota.astype(F32) * float(cap) + pos + 1.0
    slot_rows = [jnp.sum(jnp.where(ids_t[j:j + 1, :] == e_ids, slot_id, 0.0), axis=0, keepdims=True) - 1.0
                 for j in range(top_k)]

    def group_hit(grp):
        low = (lax.broadcasted_iota(jnp.int32, (1, n_tok), 1) * 0 + grp * (n_loc * n_exp)).astype(F32)
        hit = jnp.zeros((1, n_tok), F32)
        for j in range(top_k):
            inside = (ids_t[j:j + 1, :] >= low) & (ids_t[j:j + 1, :] < low + float(n_loc * n_exp))
            hit = jnp.where(inside, 1.0, hit)
        return hit

    own_hit = group_hit(g)
    slot_rows += [own_hit, own_hit * group_hit(gx * 2 + (gc + 1) % 2)]
    slot_t = jnp.concatenate(slot_rows, axis=0)
    for d in range(n_dev):
        cols_ref[pl.ds(d * tok, tok), :] = jnp.transpose(slot_t[:, d * tok:(d + 1) * tok])

    def forward(at, part, hops):
        for to in hops:
            send_x(x_rows(at, part), part, to, flip(at, to))

    def landed(at, part):
        got[at, part].wait_recv()

    landed(XN, 0)
    forward(XN, 0, [YN, PC])
    landed(YN, 1)
    forward(YN, 1, [XN, PC])
    landed(XN, 1)
    forward(XN, 1, [PC])
    landed(YN, 0)
    forward(YN, 0, [PC])
    landed(YP, 0)
    landed(YP, 1)

    step = 256

    def run_pass(first, count):
        toks = pl.ds(first, count)

        def pack(p, carry):
            for i in range(PACK):
                e = p * PACK + i
                where = lax.broadcasted_iota(jnp.int32, (cap, count), 0).astype(F32) == pos_ref[pl.ds(e, 1), toks]
                oh_ref[pl.ds(i * cap, cap), pl.ds(0, count)] = jnp.where(where, 1.0, 0.0).astype(BF16)
                gate_ref[pl.ds(pl.multiple_of(e * cap, 16), cap), :] = jnp.sum(
                    jnp.where(where, ge_ref[pl.ds(e, 1), toks], 0.0), axis=1, keepdims=True)
            base = pl.multiple_of(p * (PACK * cap), 16)
            for n in range(d_model // step):
                cols = pl.ds(n * step, step)
                packed[pl.ds(base, PACK * cap), cols] = jnp.dot(
                    oh_ref[:, pl.ds(0, count)], x_all[toks, cols], preferred_element_type=F32).astype(BF16)
            return carry

        lax.fori_loop(0, n_exp // PACK, pack, 0)

        def ring(ref_copies, e):
            return ref_copies(e, e % n_slot)

        def first_dot(e, i):
            at = pl.ds(pl.multiple_of(e * cap, 16), cap)
            uv = jnp.dot(packed[at, :], wgu[e % n_slot], preferred_element_type=F32)
            return (jax.nn.silu(uv[:, :ff]) * uv[:, ff:]).astype(BF16)

        def second_dot(hid, e):
            at = pl.ds(pl.multiple_of(e * cap, 16), cap)
            out = jnp.dot(hid, wdn[e % n_slot], preferred_element_type=F32) * gate_ref[at, :]
            hi = out.astype(BF16)
            rest = out - hi.astype(F32)
            mid = rest.astype(BF16)
            osp[0, at, :] = hi
            osp[1, at, :] = mid
            osp[2, at, :] = (rest - mid.astype(F32)).astype(BF16)

        def wait_in(e):
            for copy in ring(in_copies, e):
                copy.wait()

        for i in range(PAIR):
            wait_in(i)
        for i in range(PAIR):
            hid_ref[i] = first_dot(i, i)

        def experts(p, carry):
            now = [p * PAIR + i for i in range(PAIR)]
            for e in now:
                wait_in(e + PAIR)
                ring(out_copy, e).wait()
            held = [hid_ref[i] for i in range(PAIR)]
            for i, e in enumerate(now):
                hid_ref[i] = first_dot(e + PAIR, i)
                second_dot(held[i], e)

            for e in now:
                @pl.when(e + PAIR + n_slot < n_exp)
                def _():
                    for copy in in_copies(e + PAIR + n_slot, (e + PAIR) % n_slot):
                        copy.start()

                @pl.when(e + n_slot < n_exp)
                def _():
                    out_copy(e + n_slot, e % n_slot).start()
            return carry

        for i in range(PAIR):
            if i + n_slot < n_exp:
                for copy in in_copies(i + n_slot, i):
                    copy.start()
        lax.fori_loop(0, n_exp // PAIR - 1, experts, 0)
        for i in range(PAIR):
            ring(out_copy, n_exp - PAIR + i).wait()
        for i in range(PAIR):
            second_dot(hid_ref[i], n_exp - PAIR + i)

    def combine(blk):
        cols = cols_ref[pl.ds(pl.multiple_of(blk * tok, tok), tok), :]
        lanes = lax.broadcasted_iota(jnp.int32, (tok, rows), 1).astype(F32)
        hit = cols[:, 0:1] == lanes
        for j in range(1, top_k):
            hit = hit | (cols[:, j:j + 1] == lanes)
        q_ref[...] = jnp.where(hit, 1.0, 0.0).astype(BF16)
        for n in range(d_model // step):
            at = pl.ds(n * step, step)
            total = jnp.dot(q_ref[...], osp[0, :, at], preferred_element_type=F32)
            total += jnp.dot(q_ref[...], osp[1, :, at], preferred_element_type=F32)
            total += jnp.dot(q_ref[...], osp[2, :, at], preferred_element_type=F32)
            c_ref[blk, :, at] = total

    def swap_copy(h):
        return pltpu.make_async_remote_copy(
            src_ref=c_ref.at[2 * h + 1], dst_ref=d_ref.at[h], send_sem=ds_sem.at[h], recv_sem=dr_sem.at[h],
            device_id=dev(PC), device_id_type=pl.DeviceIdType.MESH)

    def combine_loop(count, pick):
        def body(i, carry):
            blk = pick(i)
            combine(blk)

            @pl.when(blk % 2 == 1)
            def _():
                swap_copy(blk // 2).start()
            return carry

        lax.fori_loop(0, count, body, 0)

    def split_rows(h):
        swap_copy(h).wait_recv()
        cols = cols_ref[pl.ds(2 * h * tok, tok), :]
        mine = c_ref[2 * h]
        other = d_ref[h]
        c_ref[2 * h] = jnp.where(cols[:, 6:7] > 0.5, mine, other)
        d_ref[h] = jnp.where(cols[:, 7:8] > 0.5, other, 0.0)

    def ship(i, src, dst, to):
        return send(src, dst, ts_sem.at[i], tr_sem.at[i], to)

    landed(DG, 0)
    forward(DG, 0, [PC])
    landed(DG, 1)
    forward(DG, 1, [PC])
    for at in (XP, PC, DP):
        landed(at, 0)
        landed(at, 1)
    run_pass(0, n_tok)
    combine_loop(2, lambda i: 1 - i)
    split_rows(0)
    first_own = ship(0, c_ref.at[0], rf_ref.at[0], YN)
    combine_loop(2, lambda i: 3 - i)
    split_rows(1)
    first_far = ship(1, c_ref.at[2], rf_ref.at[1], YN)
    hop = ship(2, d_ref.at[1], rs_ref.at[0], XN)
    combine_loop(4, lambda i: 5 + 2 * i - (i // 2) * 5)
    hop.wait_recv()
    d_ref[0] = d_ref[0] + rs_ref[0]
    second = ship(3, d_ref.at[0], rs_ref.at[1], YN)
    split_rows(2)
    far_second = ship(4, d_ref.at[2], rs_ref.at[2], XN)
    split_rows(3)

    first_own.wait_recv()
    total = (c_ref[6] + rf_ref[0]).astype(BF16).astype(F32)
    c_ref[6] = total
    first_far.wait_recv()
    gp_ref[...] = (c_ref[4] + rf_ref[1]).astype(BF16)
    far_first = ship(5, gp_ref, gx_ref, XN)
    far_second.wait_recv()
    d_ref[3] = d_ref[3] + rs_ref[2]
    far_first.wait_recv()
    c_ref[6] = c_ref[6] + gx_ref[...].astype(F32)
    second.wait_recv()
    y_ref[...] = (c_ref[6] + (d_ref[3] + rs_ref[1]).astype(BF16).astype(F32)).astype(BF16)
    for copy in pending:
        copy.wait_send()
    for h in range(n_dev // 2):
        swap_copy(h).wait_send()


def solution(mesh):
    n_grp = mesh.shape["grp"]
    n_loc = mesh.shape["loc"]
    tok_spec = P(("part", "grp", "loc"), None)
    w_spec = P(("grp", "loc"), None, None)

    def device_step(x_tok, expert_ids, gate_val, w_gate, w_up, w_down):
        tok, d_model = x_tok.shape
        top_k = expert_ids.shape[1]
        n_exp, _, ff = w_gate.shape
        n_dev = n_grp * n_loc
        n_tok = tok * n_dev
        cap = 8 * (n_tok * top_k // (4 * n_exp * n_dev) + 1)
        rows = n_exp * cap
        n_slot = 9
        vmem = pltpu.VMEM
        dma = pltpu.SemaphoreType.DMA
        dims = (n_loc, n_grp, n_exp, cap, top_k, n_slot)
        return pl.pallas_call(
            functools.partial(moe_kernel, dims),
            out_shape=jax.ShapeDtypeStruct((tok, d_model), BF16),
            in_specs=[pl.BlockSpec(memory_space=vmem)] * 3 + [pl.BlockSpec(memory_space=pl.ANY)] * 3,
            out_specs=pl.BlockSpec(memory_space=vmem),
            scratch_shapes=[
                vmem((n_tok, d_model), BF16),
                vmem((n_dev, top_k, tok), jnp.int32),
                vmem((n_dev, top_k, tok), F32),
                vmem((32, n_tok), F32),
                vmem((32, n_tok), F32),
                vmem((n_tok, 8), F32),
                vmem((rows, 1), F32),
                vmem((PACK * cap, n_tok), BF16),
                vmem((rows, d_model), BF16),
                vmem((PAIR, cap, ff), BF16),
                vmem((3, rows, d_model), BF16),
                vmem((tok, rows), BF16),
                vmem((n_dev, tok, d_model), F32),
                vmem((n_dev // 2, tok, d_model), F32),
                vmem((2, tok, d_model), F32),
                vmem((3, tok, d_model), F32),
                vmem((tok, d_model), BF16),
                vmem((tok, d_model), BF16),
                vmem((n_slot, d_model, 2 * ff), BF16),
                vmem((n_slot, ff, d_model), BF16),
                dma((n_slot, 3)),
                dma((14,)),
                dma((16,)),
                dma((7, 2)),
                dma((7, 2)),
                dma((n_dev // 2,)),
                dma((n_dev // 2,)),
                dma((6,)),
                dma((6,)),
            ],
            compiler_params=pltpu.CompilerParams(
                collective_id=0, has_side_effects=True, vmem_limit_bytes=67043328),
            name="moe",
        )(x_tok, expert_ids.T, gate_val.T, w_gate, w_up, w_down)

    return jax.shard_map(device_step, mesh=mesh, in_specs=(tok_spec, tok_spec, tok_spec, w_spec, w_spec, w_spec), out_specs=tok_spec, check_vma=False)
```

```python
import functools

import jax
import jax.numpy as jnp
from jax import lax
from jax.experimental import pallas as pl
from jax.experimental.pallas import tpu as pltpu
from jax.sharding import PartitionSpec as P

F32 = jnp.float32
BF16 = jnp.bfloat16
PACK = 5
PAIR = 2


YN, YP, DG, DP = (0, 0, 1), (0, 1, 1), (1, 0, 1), (1, 1, 1)
XN, XP, ME, PC = (1, 0, 0), (1, 1, 0), (0, 0, 0), (0, 1, 0)
ORDER = [YN, YP, XN, XP, ME, PC, DG, DP]


def flip(a, b):
    return tuple((i + j) % 2 for i, j in zip(a, b))


def moe_kernel(dims, x_ref, ids_ref, gates_ref, wg_ref, wu_ref, wd_ref, y_ref,
               x_all, ids_all, gates_all, pos_ref, ge_ref, cols_ref, gate_ref, oh_ref, packed, hid_ref, osp, q_ref, qp_ref, qn_ref,
               c_ref, d_ref, rf_ref, rs_ref, gp_ref, gx_ref, wgu, wdn,
               in_sem, w_sem, xs_sem, xr_sem, ms_sem, mr_sem, ds_sem, dr_sem, ts_sem, tr_sem, ns_sem, nr_sem):
    n_loc, n_grp, n_exp, cap, top_k, n_slot = dims
    tok, d_model = x_ref.shape
    half = tok // 2
    own = ORDER.index(ME)
    ff = wg_ref.shape[2]
    n_dev = n_loc * n_grp
    n_tok = tok * n_dev
    rows = n_exp * cap
    l = lax.axis_index("loc")
    g = lax.axis_index("grp")
    gx, gc = g // 2, g % 2

    def dev(to):
        fx, fc, fl = to
        return {"grp": ((gx + fx) % 2) * 2 + (gc + fc) % 2, "loc": (l + fl) % 2}

    def in_copies(e, slot):
        return (
            pltpu.make_async_copy(wg_ref.at[e], wgu.at[slot, :, pl.ds(0, ff)], w_sem.at[slot, 0]),
            pltpu.make_async_copy(wu_ref.at[e], wgu.at[slot, :, pl.ds(ff, ff)], w_sem.at[slot, 1]),
        )

    def out_copy(e, slot):
        return pltpu.make_async_copy(wd_ref.at[e], wdn.at[slot], w_sem.at[slot, 2])

    def start_weights(e, carry):
        for copy in in_copies(e, e):
            copy.start()
        out_copy(e, e).start()
        return carry

    loads = [
        pltpu.make_async_copy(src, dst, in_sem.at[i]) for i, (src, dst) in enumerate((
            (x_ref, x_all.at[pl.ds(own * tok, tok), :]), (ids_ref, ids_all.at[own]), (gates_ref, gates_all.at[own])))]
    for copy in loads:
        copy.start()

    peers = [r for r in ORDER if r != ME]
    barrier = pltpu.get_barrier_semaphore()
    for r in peers:
        pl.semaphore_signal(barrier, inc=1, device_id=dev(r), device_id_type=pl.DeviceIdType.MESH)
    lax.fori_loop(0, n_slot, start_weights, 0)
    pl.semaphore_wait(barrier, len(peers))
    for copy in loads:
        copy.wait()

    pending = []

    class Sent:
        def __init__(self, *described):
            self.described = described
            self.copy().start()
            pending.append(self)

        def copy(self):
            src, dst, s_sem, r_sem, to = self.described
            return pltpu.make_async_remote_copy(
                src_ref=src(), dst_ref=dst(), send_sem=s_sem(), recv_sem=r_sem(),
                device_id=dev(to), device_id_type=pl.DeviceIdType.MESH)

        def wait_recv(self):
            self.copy().wait_recv()

        def wait_send(self):
            self.copy().wait_send()

    def send(src, dst, s_sem, r_sem, to):
        return Sent(lambda: src, lambda: dst, lambda: s_sem, lambda: r_sem, to)

    metas = []
    for i, r in enumerate(peers):
        for k, (src, dst) in enumerate(((ids_all.at[own], ids_all), (gates_all.at[own], gates_all))):
            metas.append(send(src, dst.at[ORDER.index(r)], ms_sem.at[i, k], mr_sem.at[i, k], r))

    def x_rows(at, part):
        return x_all.at[pl.ds(ORDER.index(at) * tok + part * half, half), :]

    got = {}

    def send_x(src, part, to, at):
        i = len(got)
        got[at, part] = Sent(lambda: x_rows(*src), lambda: x_rows(at, part), lambda: xs_sem.at[i],
                             lambda: xr_sem.at[ORDER.index(at) * 2 + part], to)

    for part, to in ((0, XN), (1, YN), (1, XN), (0, YN), (0, PC), (1, PC)):
        send_x((ME, part), part, to, to)

    for copy in metas:
        copy.wait_recv()

    ids_t = jnp.concatenate([ids_all[d] for d in range(n_dev)], axis=1).astype(F32)
    gts_t = jnp.concatenate([gates_all[d] for d in range(n_dev)], axis=1)
    e_rows = 32
    e_iota = lax.broadcasted_iota(jnp.int32, (e_rows, n_tok), 0)
    e_ids = jnp.where(e_iota < n_exp, e_iota + (g * n_loc + l) * n_exp, -5).astype(F32)
    mask = jnp.zeros((e_rows, n_tok), F32)
    gate_e = jnp.zeros((e_rows, n_tok), F32)
    for j in range(top_k):
        eq = ids_t[j:j + 1, :] == e_ids
        mask = mask + jnp.where(eq, 1.0, 0.0)
        gate_e = gate_e + jnp.where(eq, gts_t[j:j + 1, :], 0.0)
    blocks = [mask[:, d * tok:(d + 1) * tok] for d in range(n_dev)]
    tri = (lax.broadcasted_iota(jnp.int32, (tok, tok), 0) < lax.broadcasted_iota(jnp.int32, (tok, tok), 1))
    tri = jnp.where(tri, 1.0, 0.0).astype(BF16)
    prefix = jnp.dot(jnp.concatenate(blocks, axis=0).astype(BF16), tri, preferred_element_type=F32)
    offset = jnp.zeros((e_rows, 1), F32)
    pos = []
    for d in range(n_dev):
        pos.append(prefix[d * e_rows:(d + 1) * e_rows, :] + offset)
        offset = offset + jnp.sum(blocks[d], axis=1, keepdims=True)
    pos = jnp.concatenate(pos, axis=1)
    pos_ref[...] = jnp.where(mask > 0.0, pos, -1.0)
    ge_ref[...] = gate_e
    slot_id = e_iota.astype(F32) * float(cap) + pos + 1.0
    slot_rows = [jnp.sum(jnp.where(ids_t[j:j + 1, :] == e_ids, slot_id, 0.0), axis=0, keepdims=True) - 1.0
                 for j in range(top_k)]

    def group_hit(grp):
        low = (lax.broadcasted_iota(jnp.int32, (1, n_tok), 1) * 0 + grp * (n_loc * n_exp)).astype(F32)
        hit = jnp.zeros((1, n_tok), F32)
        for j in range(top_k):
            inside = (ids_t[j:j + 1, :] >= low) & (ids_t[j:j + 1, :] < low + float(n_loc * n_exp))
            hit = jnp.where(inside, 1.0, hit)
        return hit

    own_hit = group_hit(g)
    slot_rows += [own_hit, own_hit * group_hit(gx * 2 + (gc + 1) % 2)]
    slot_t = jnp.concatenate(slot_rows, axis=0)
    for d in range(n_dev):
        cols_ref[pl.ds(d * tok, tok), :] = jnp.transpose(slot_t[:, d * tok:(d + 1) * tok])

    def selection(blk):
        cols = cols_ref[pl.ds(blk * tok, tok), :]
        lanes = lax.broadcasted_iota(jnp.int32, (tok, rows), 1).astype(F32)
        hit = cols[:, 0:1] == lanes
        for j in range(1, top_k):
            hit = hit | (cols[:, j:j + 1] == lanes)
        return jnp.where(hit, 1.0, 0.0).astype(BF16)

    qp_ref[...] = selection(ORDER.index(YP))
    qn_ref[...] = selection(ORDER.index(YN))

    def forward(at, part, hops):
        for to in hops:
            send_x((at, part), part, to, flip(at, to))

    def landed(at, part):
        got[at, part].wait_recv()

    landed(XN, 0)
    forward(XN, 0, [YN, PC])
    landed(YN, 1)
    forward(YN, 1, [XN, PC])
    landed(XN, 1)
    forward(XN, 1, [PC])
    landed(YN, 0)
    forward(YN, 0, [PC])
    landed(YP, 0)
    landed(YP, 1)

    step = 256

    def pack(first, count, add, midway):
        toks = pl.ds(first, count)

        def body(p, carry):
            for i in range(PACK):
                e = p * PACK + i
                where = lax.broadcasted_iota(jnp.int32, (cap, count), 0).astype(F32) == pos_ref[pl.ds(e, 1), toks]
                oh_ref[pl.ds(i * cap, cap), pl.ds(0, count)] = jnp.where(where, 1.0, 0.0).astype(BF16)
                gate = jnp.sum(jnp.where(where, ge_ref[pl.ds(e, 1), toks], 0.0), axis=1, keepdims=True)
                at = pl.ds(pl.multiple_of(e * cap, 16), cap)
                gate_ref[at, :] = gate_ref[at, :] + gate if add else gate
            at = pl.ds(pl.multiple_of(p * (PACK * cap), 16), PACK * cap)
            for n in range(d_model // step):
                cols = pl.ds(n * step, step)
                part = jnp.dot(oh_ref[:, pl.ds(0, count)], x_all[toks, cols], preferred_element_type=F32)
                if add:
                    part = part + packed[at, cols].astype(F32)
                packed[at, cols] = part.astype(BF16)
            if midway is not None:
                @pl.when(p == 1)
                def _():
                    midway()
            return carry

        lax.fori_loop(0, n_exp // PACK, body, 0)

    def diagonal():
        for part in (0, 1):
            landed(DG, part)
            forward(DG, part, [PC])

    for at in (XP, PC):
        landed(at, 0)
        landed(at, 1)
    pack(0, n_tok - 2 * tok, False, diagonal)
    landed(DP, 0)
    landed(DP, 1)
    pack(n_tok - 2 * tok, 2 * tok, True, None)

    def ring(ref_copies, e):
        return ref_copies(e, e % n_slot)

    def first_dot(e, i):
        at = pl.ds(pl.multiple_of(e * cap, 16), cap)
        uv = jnp.dot(packed[at, :], wgu[e % n_slot], preferred_element_type=F32)
        return (jax.nn.silu(uv[:, :ff]) * uv[:, ff:]).astype(BF16)

    def second_dot(hid, e):
        at = pl.ds(pl.multiple_of(e * cap, 16), cap)
        out = jnp.dot(hid, wdn[e % n_slot], preferred_element_type=F32) * gate_ref[at, :]
        hi = out.astype(BF16)
        rest = out - hi.astype(F32)
        mid = rest.astype(BF16)
        osp[0, at, :] = hi
        osp[1, at, :] = mid
        osp[2, at, :] = (rest - mid.astype(F32)).astype(BF16)

    def wait_in(e):
        for copy in ring(in_copies, e):
            copy.wait()

    for i in range(PAIR):
        wait_in(i)
    for i in range(PAIR):
        hid_ref[i] = first_dot(i, i)

    def experts(p, carry):
        now = [p * PAIR + i for i in range(PAIR)]
        for e in now:
            wait_in(e + PAIR)
            ring(out_copy, e).wait()
        held = [hid_ref[i] for i in range(PAIR)]
        for i, e in enumerate(now):
            hid_ref[i] = first_dot(e + PAIR, i)
            second_dot(held[i], e)

        for e in now:
            @pl.when(e + PAIR + n_slot < n_exp)
            def _():
                for copy in in_copies(e + PAIR + n_slot, (e + PAIR) % n_slot):
                    copy.start()

            @pl.when(e + n_slot < n_exp)
            def _():
                out_copy(e + n_slot, e % n_slot).start()
        return carry

    for i in range(PAIR):
        if i + n_slot < n_exp:
            for copy in in_copies(i + n_slot, i):
                copy.start()
    lax.fori_loop(0, n_exp // PAIR - 1, experts, 0)
    for i in range(PAIR):
        ring(out_copy, n_exp - PAIR + i).wait()
    for i in range(PAIR):
        second_dot(hid_ref[i], n_exp - PAIR + i)

    def combine(q, blk, chunks):
        for n in chunks:
            at = pl.ds(n * step, step)
            total = jnp.dot(q[...], osp[0, :, at], preferred_element_type=F32)
            total += jnp.dot(q[...], osp[1, :, at], preferred_element_type=F32)
            total += jnp.dot(q[...], osp[2, :, at], preferred_element_type=F32)
            c_ref[blk, :, at] = total

    def swap_copy(h):
        return pltpu.make_async_remote_copy(
            src_ref=c_ref.at[2 * h + 1], dst_ref=d_ref.at[h], send_sem=ds_sem.at[h], recv_sem=dr_sem.at[h],
            device_id=dev(PC), device_id_type=pl.DeviceIdType.MESH)

    def combine_loop(count, pick):
        def body(i, carry):
            blk = pick(i)
            q_ref[...] = selection(pl.multiple_of(blk, 1))
            combine(q_ref, blk, range(d_model // step))

            @pl.when(blk % 2 == 1)
            def _():
                swap_copy(blk // 2).start()
            return carry

        lax.fori_loop(0, count, body, 0)

    everything = pl.ds(0, d_model)

    def split_rows(h, at):
        cols = cols_ref[pl.ds(2 * h * tok, tok), :]
        mine = c_ref[2 * h, :, at]
        other = d_ref[h, :, at]
        c_ref[2 * h, :, at] = jnp.where(cols[:, 6:7] > 0.5, mine, other)
        d_ref[h, :, at] = jnp.where(cols[:, 7:8] > 0.5, other, 0.0)

    def ship(i, src, dst, to):
        return send(src, dst, ts_sem.at[i], tr_sem.at[i], to)

    first_own = []
    for i, chunks in enumerate((range(0, 2), range(2, d_model // step))):
        at = pl.ds(chunks[0] * step, len(chunks) * step)
        combine(qp_ref, ORDER.index(YP), chunks)
        swap = send(c_ref.at[ORDER.index(YP), :, at], d_ref.at[0, :, at], ns_sem.at[i], nr_sem.at[i], PC)
        combine(qn_ref, ORDER.index(YN), chunks)
        swap.wait_recv()
        split_rows(0, at)
        first_own.append(send(c_ref.at[0, :, at], rf_ref.at[0, :, at], ns_sem.at[2 + i], nr_sem.at[2 + i], YN))
    combine_loop(2, lambda i: 7 - i)
    swap_copy(3).wait_recv()
    split_rows(3, everything)
    first_far = ship(1, c_ref.at[6], rf_ref.at[1], YN)
    hop = ship(2, d_ref.at[3], rs_ref.at[0], XN)
    combine_loop(4, lambda i: 3 + 2 * i - (i // 2) * 5)
    hop.wait_recv()
    d_ref[0] = d_ref[0] + rs_ref[0]
    second = ship(3, d_ref.at[0], rs_ref.at[1], YN)
    for h in (1, 2):
        swap_copy(h).wait_recv()
        split_rows(h, everything)
        if h == 1:
            far_second = ship(4, d_ref.at[1], rs_ref.at[2], XN)

    for copy in first_own:
        copy.wait_recv()
    c_ref[4] = (c_ref[4] + rf_ref[0]).astype(BF16).astype(F32)
    first_far.wait_recv()
    gp_ref[...] = (c_ref[2] + rf_ref[1]).astype(BF16)
    far_first = ship(5, gp_ref, gx_ref, XN)
    far_second.wait_recv()
    d_ref[2] = d_ref[2] + rs_ref[2]
    far_first.wait_recv()
    c_ref[4] = c_ref[4] + gx_ref[...].astype(F32)
    second.wait_recv()
    y_ref[...] = (c_ref[4] + (d_ref[2] + rs_ref[1]).astype(BF16).astype(F32)).astype(BF16)
    for copy in pending:
        copy.wait_send()
    for h in range(1, n_dev // 2):
        swap_copy(h).wait_send()


def solution(mesh):
    n_grp = mesh.shape["grp"]
    n_loc = mesh.shape["loc"]
    tok_spec = P(("part", "grp", "loc"), None)
    w_spec = P(("grp", "loc"), None, None)

    def device_step(x_tok, expert_ids, gate_val, w_gate, w_up, w_down):
        tok, d_model = x_tok.shape
        top_k = expert_ids.shape[1]
        n_exp, _, ff = w_gate.shape
        n_dev = n_grp * n_loc
        n_tok = tok * n_dev
        cap = 8 * (n_tok * top_k // (4 * n_exp * n_dev) + 1)
        rows = n_exp * cap
        n_slot = 9
        vmem = pltpu.VMEM
        dma = pltpu.SemaphoreType.DMA
        dims = (n_loc, n_grp, n_exp, cap, top_k, n_slot)
        return pl.pallas_call(
            functools.partial(moe_kernel, dims),
            out_shape=jax.ShapeDtypeStruct((tok, d_model), BF16),
            in_specs=[pl.BlockSpec(memory_space=pl.ANY)] * 6,
            out_specs=pl.BlockSpec(memory_space=vmem),
            scratch_shapes=[
                vmem((n_tok, d_model), BF16),
                vmem((n_dev, top_k, tok), jnp.int32),
                vmem((n_dev, top_k, tok), F32),
                vmem((32, n_tok), F32),
                vmem((32, n_tok), F32),
                vmem((n_tok, 8), F32),
                vmem((rows, 1), F32),
                vmem((PACK * cap, n_tok), BF16),
                vmem((rows, d_model), BF16),
                vmem((PAIR, cap, ff), BF16),
                vmem((3, rows, d_model), BF16),
                vmem((tok, rows), BF16),
                vmem((tok, rows), BF16),
                vmem((tok, rows), BF16),
                vmem((n_dev, tok, d_model), F32),
                vmem((n_dev // 2, tok, d_model), F32),
                vmem((2, tok, d_model), F32),
                vmem((3, tok, d_model), F32),
                vmem((tok, d_model), BF16),
                vmem((tok, d_model), BF16),
                vmem((n_slot, d_model, 2 * ff), BF16),
                vmem((n_slot, ff, d_model), BF16),
                dma((3,)),
                dma((n_slot, 3)),
                dma((14,)),
                dma((16,)),
                dma((7, 2)),
                dma((7, 2)),
                dma((n_dev // 2,)),
                dma((n_dev // 2,)),
                dma((6,)),
                dma((6,)),
                dma((4,)),
                dma((4,)),
            ],
            compiler_params=pltpu.CompilerParams(
                collective_id=0, has_side_effects=True, vmem_limit_bytes=67043328),
            name="moe",
        )(x_tok, expert_ids.T, gate_val.T, w_gate, w_up, w_down)

    return jax.shard_map(device_step, mesh=mesh, in_specs=(tok_spec, tok_spec, tok_spec, w_spec, w_spec, w_spec), out_specs=tok_spec, check_vma=False)
```

```python
import functools

import jax
import jax.numpy as jnp
from jax import lax
from jax.experimental import pallas as pl
from jax.experimental.pallas import tpu as pltpu
from jax.sharding import PartitionSpec as P

F32 = jnp.float32
BF16 = jnp.bfloat16
PACK = 5
PAIR = 2


YN, YP, DG, DP = (0, 0, 1), (0, 1, 1), (1, 0, 1), (1, 1, 1)
XN, XP, ME, PC = (1, 0, 0), (1, 1, 0), (0, 0, 0), (0, 1, 0)
ORDER = [YN, YP, XN, XP, ME, PC, DG, DP]


def flip(a, b):
    return tuple((i + j) % 2 for i, j in zip(a, b))


def moe_kernel(dims, x_ref, ids_ref, gates_ref, wg_ref, wu_ref, wd_ref, y_ref,
               x_all, ids_all, gates_all, pos_ref, ge_ref, cols_ref, gate_ref, oh_ref, packed, hid_ref, osp, q_ref, qp_ref, qn_ref,
               c_ref, d_ref, rf_ref, rs_ref, gp_ref, gx_ref, wgu, wdn,
               in_sem, w_sem, xs_sem, xr_sem, ms_sem, mr_sem, ds_sem, dr_sem, ts_sem, tr_sem, ns_sem, nr_sem):
    n_loc, n_grp, n_exp, cap, top_k, n_slot = dims
    tok, d_model = x_ref.shape
    half = tok // 2
    own = ORDER.index(ME)
    ff = wg_ref.shape[2]
    n_dev = n_loc * n_grp
    n_tok = tok * n_dev
    rows = n_exp * cap
    l = lax.axis_index("loc")
    g = lax.axis_index("grp")
    gx, gc = g // 2, g % 2

    def dev(to):
        fx, fc, fl = to
        return {"grp": ((gx + fx) % 2) * 2 + (gc + fc) % 2, "loc": (l + fl) % 2}

    def in_copies(e, slot):
        return (
            pltpu.make_async_copy(wg_ref.at[e], wgu.at[slot, :, pl.ds(0, ff)], w_sem.at[slot, 0]),
            pltpu.make_async_copy(wu_ref.at[e], wgu.at[slot, :, pl.ds(ff, ff)], w_sem.at[slot, 1]),
        )

    def out_copy(e, slot):
        return pltpu.make_async_copy(wd_ref.at[e], wdn.at[slot], w_sem.at[slot, 2])

    def start_weights(e, carry):
        for copy in in_copies(e, e):
            copy.start()
        out_copy(e, e).start()
        return carry

    loads = [
        pltpu.make_async_copy(src, dst, in_sem.at[i]) for i, (src, dst) in enumerate((
            (x_ref, x_all.at[pl.ds(own * tok, tok), :]), (ids_ref, ids_all.at[own]), (gates_ref, gates_all.at[own])))]
    for copy in loads:
        copy.start()

    peers = [r for r in ORDER if r != ME]
    barrier = pltpu.get_barrier_semaphore()
    for r in peers:
        pl.semaphore_signal(barrier, inc=1, device_id=dev(r), device_id_type=pl.DeviceIdType.MESH)
    lax.fori_loop(0, n_slot, start_weights, 0)
    pl.semaphore_wait(barrier, len(peers))
    for copy in loads:
        copy.wait()

    pending = []

    class Sent:
        def __init__(self, *described):
            self.described = described
            self.copy().start()
            pending.append(self)

        def copy(self):
            src, dst, s_sem, r_sem, to = self.described
            return pltpu.make_async_remote_copy(
                src_ref=src(), dst_ref=dst(), send_sem=s_sem(), recv_sem=r_sem(),
                device_id=dev(to), device_id_type=pl.DeviceIdType.MESH)

        def wait_recv(self):
            self.copy().wait_recv()

        def wait_send(self):
            self.copy().wait_send()

    def send(src, dst, s_sem, r_sem, to):
        return Sent(lambda: src, lambda: dst, lambda: s_sem, lambda: r_sem, to)

    metas = []
    for i, r in enumerate(peers):
        for k, (src, dst) in enumerate(((ids_all.at[own], ids_all), (gates_all.at[own], gates_all))):
            metas.append(send(src, dst.at[ORDER.index(r)], ms_sem.at[i, k], mr_sem.at[i, k], r))

    def x_rows(at, part):
        return x_all.at[pl.ds(ORDER.index(at) * tok + part * half, half), :]

    got = {}

    def send_x(src, part, to, at):
        i = len(got)
        got[at, part] = Sent(lambda: x_rows(*src), lambda: x_rows(at, part), lambda: xs_sem.at[i],
                             lambda: xr_sem.at[ORDER.index(at) * 2 + part], to)

    for part, to in ((0, XN), (1, YN), (1, XN), (0, YN), (0, PC), (1, PC)):
        send_x((ME, part), part, to, to)

    for copy in metas:
        copy.wait_recv()

    ids_t = jnp.concatenate([ids_all[d] for d in range(n_dev)], axis=1).astype(F32)
    gts_t = jnp.concatenate([gates_all[d] for d in range(n_dev)], axis=1)
    e_rows = 32
    e_iota = lax.broadcasted_iota(jnp.int32, (e_rows, n_tok), 0)
    e_ids = jnp.where(e_iota < n_exp, e_iota + (g * n_loc + l) * n_exp, -5).astype(F32)
    mask = jnp.zeros((e_rows, n_tok), F32)
    gate_e = jnp.zeros((e_rows, n_tok), F32)
    for j in range(top_k):
        eq = ids_t[j:j + 1, :] == e_ids
        mask = mask + jnp.where(eq, 1.0, 0.0)
        gate_e = gate_e + jnp.where(eq, gts_t[j:j + 1, :], 0.0)
    blocks = [mask[:, d * tok:(d + 1) * tok] for d in range(n_dev)]
    tri = (lax.broadcasted_iota(jnp.int32, (tok, tok), 0) < lax.broadcasted_iota(jnp.int32, (tok, tok), 1))
    tri = jnp.where(tri, 1.0, 0.0).astype(BF16)
    prefix = jnp.dot(jnp.concatenate(blocks, axis=0).astype(BF16), tri, preferred_element_type=F32)
    offset = jnp.zeros((e_rows, 1), F32)
    pos = []
    for d in range(n_dev):
        pos.append(prefix[d * e_rows:(d + 1) * e_rows, :] + offset)
        offset = offset + jnp.sum(blocks[d], axis=1, keepdims=True)
    pos = jnp.concatenate(pos, axis=1)
    pos_ref[...] = jnp.where(mask > 0.0, pos, -1.0)
    ge_ref[...] = gate_e
    slot_id = e_iota.astype(F32) * float(cap) + pos + 1.0
    slot_rows = [jnp.sum(jnp.where(ids_t[j:j + 1, :] == e_ids, slot_id, 0.0), axis=0, keepdims=True) - 1.0
                 for j in range(top_k)]

    def group_hit(grp):
        low = (lax.broadcasted_iota(jnp.int32, (1, n_tok), 1) * 0 + grp * (n_loc * n_exp)).astype(F32)
        hit = jnp.zeros((1, n_tok), F32)
        for j in range(top_k):
            inside = (ids_t[j:j + 1, :] >= low) & (ids_t[j:j + 1, :] < low + float(n_loc * n_exp))
            hit = jnp.where(inside, 1.0, hit)
        return hit

    own_hit = group_hit(g)
    slot_rows += [own_hit, own_hit * group_hit(gx * 2 + (gc + 1) % 2)]
    slot_t = jnp.concatenate(slot_rows, axis=0)
    for d in range(n_dev):
        cols_ref[pl.ds(d * tok, tok), :] = jnp.transpose(slot_t[:, d * tok:(d + 1) * tok])

    def selection(blk):
        cols = cols_ref[pl.ds(pl.multiple_of(blk * tok, tok), tok), :]
        lanes = lax.broadcasted_iota(jnp.int32, (tok, rows), 1).astype(F32)
        hit = cols[:, 0:1] == lanes
        for j in range(1, top_k):
            hit = hit | (cols[:, j:j + 1] == lanes)
        return jnp.where(hit, 1.0, 0.0).astype(BF16)

    qp_ref[...] = selection(ORDER.index(DP))
    qn_ref[...] = selection(ORDER.index(DG))

    def forward(at, part, hops):
        for to in hops:
            send_x((at, part), part, to, flip(at, to))

    def landed(at, part):
        got[at, part].wait_recv()

    landed(XN, 0)
    forward(XN, 0, [YN, PC])
    landed(YN, 1)
    forward(YN, 1, [XN, PC])
    landed(XN, 1)
    forward(XN, 1, [PC])
    landed(YN, 0)
    forward(YN, 0, [PC])
    landed(YP, 0)
    landed(YP, 1)

    step = 256

    def pack(first, count, add, midway):
        toks = pl.ds(first, count)

        def body(p, carry):
            for i in range(PACK):
                e = p * PACK + i
                where = lax.broadcasted_iota(jnp.int32, (cap, count), 0).astype(F32) == pos_ref[pl.ds(e, 1), toks]
                oh_ref[pl.ds(i * cap, cap), pl.ds(0, count)] = jnp.where(where, 1.0, 0.0).astype(BF16)
                gate = jnp.sum(jnp.where(where, ge_ref[pl.ds(e, 1), toks], 0.0), axis=1, keepdims=True)
                at = pl.ds(pl.multiple_of(e * cap, 16), cap)
                gate_ref[at, :] = gate_ref[at, :] + gate if add else gate
            at = pl.ds(pl.multiple_of(p * (PACK * cap), 16), PACK * cap)
            for n in range(d_model // step):
                cols = pl.ds(n * step, step)
                part = jnp.dot(oh_ref[:, pl.ds(0, count)], x_all[toks, cols], preferred_element_type=F32)
                if add:
                    part = part + packed[at, cols].astype(F32)
                packed[at, cols] = part.astype(BF16)
            if midway is not None:
                @pl.when(p == 1)
                def _():
                    midway()
            return carry

        lax.fori_loop(0, n_exp // PACK, body, 0)

    def diagonal():
        for part in (0, 1):
            landed(DG, part)
            forward(DG, part, [PC])

    for at in (XP, PC):
        landed(at, 0)
        landed(at, 1)
    pack(0, n_tok - 2 * tok, False, diagonal)
    landed(DP, 0)
    landed(DP, 1)
    pack(n_tok - 2 * tok, 2 * tok, True, None)

    def ring(ref_copies, e):
        return ref_copies(e, e % n_slot)

    def first_dot(e, i):
        at = pl.ds(pl.multiple_of(e * cap, 16), cap)
        uv = jnp.dot(packed[at, :], wgu[e % n_slot], preferred_element_type=F32)
        return (jax.nn.silu(uv[:, :ff]) * uv[:, ff:]).astype(BF16)

    def second_dot(hid, e):
        at = pl.ds(pl.multiple_of(e * cap, 16), cap)
        out = jnp.dot(hid, wdn[e % n_slot], preferred_element_type=F32) * gate_ref[at, :]
        hi = out.astype(BF16)
        rest = out - hi.astype(F32)
        mid = rest.astype(BF16)
        osp[0, at, :] = hi
        osp[1, at, :] = mid
        osp[2, at, :] = (rest - mid.astype(F32)).astype(BF16)

    def wait_in(e):
        for copy in ring(in_copies, e):
            copy.wait()

    for i in range(PAIR):
        wait_in(i)
    for i in range(PAIR):
        hid_ref[i] = first_dot(i, i)

    def experts(p, carry):
        now = [p * PAIR + i for i in range(PAIR)]
        for e in now:
            wait_in(e + PAIR)
            ring(out_copy, e).wait()
        held = [hid_ref[i] for i in range(PAIR)]
        for i, e in enumerate(now):
            hid_ref[i] = first_dot(e + PAIR, i)
            second_dot(held[i], e)

        for e in now:
            @pl.when(e + PAIR + n_slot < n_exp)
            def _():
                for copy in in_copies(e + PAIR + n_slot, (e + PAIR) % n_slot):
                    copy.start()

            @pl.when(e + n_slot < n_exp)
            def _():
                out_copy(e + n_slot, e % n_slot).start()
        return carry

    for i in range(PAIR):
        if i + n_slot < n_exp:
            for copy in in_copies(i + n_slot, i):
                copy.start()
    lax.fori_loop(0, n_exp // PAIR - 1, experts, 0)
    for i in range(PAIR):
        ring(out_copy, n_exp - PAIR + i).wait()
    for i in range(PAIR):
        second_dot(hid_ref[i], n_exp - PAIR + i)

    def combine(q, blk, chunks):
        for n in chunks:
            at = pl.ds(n * step, step)
            total = jnp.dot(q[...], osp[0, :, at], preferred_element_type=F32)
            total += jnp.dot(q[...], osp[1, :, at], preferred_element_type=F32)
            total += jnp.dot(q[...], osp[2, :, at], preferred_element_type=F32)
            c_ref[blk, :, at] = total

    def swap_copy(h):
        return pltpu.make_async_remote_copy(
            src_ref=c_ref.at[2 * h + 1], dst_ref=d_ref.at[h], send_sem=ds_sem.at[h], recv_sem=dr_sem.at[h],
            device_id=dev(PC), device_id_type=pl.DeviceIdType.MESH)

    everything = pl.ds(0, d_model)

    def split_rows(h, at):
        cols = cols_ref[pl.ds(pl.multiple_of(2 * h * tok, tok), tok), :]
        mine = c_ref[2 * h, :, at]
        other = d_ref[h, :, at]
        c_ref[2 * h, :, at] = jnp.where(cols[:, 6:7] > 0.5, mine, other)
        d_ref[h, :, at] = jnp.where(cols[:, 7:8] > 0.5, other, 0.0)

    def ship(i, src, dst, to):
        return Sent(src, dst, lambda: ts_sem.at[i], lambda: tr_sem.at[i], to)

    first_far = []
    hop = []
    far = ORDER.index(DG)
    for i, chunks in enumerate((range(0, 2), range(2, d_model // step))):
        at = pl.ds(chunks[0] * step, len(chunks) * step)
        combine(qp_ref, far + 1, chunks)
        swap = send(c_ref.at[far + 1, :, at], d_ref.at[far // 2, :, at], ns_sem.at[i, 0], nr_sem.at[i, 0], PC)
        combine(qn_ref, far, chunks)
        swap.wait_recv()
        split_rows(far // 2, at)
        first_far.append(send(c_ref.at[far, :, at], rf_ref.at[1, :, at], ns_sem.at[i, 1], nr_sem.at[i, 1], YN))
        hop.append(send(d_ref.at[far // 2, :, at], rs_ref.at[0, :, at], ns_sem.at[i, 2], nr_sem.at[i, 2], XN))

    shipped = {}

    def others(i, carry):
        blk = i + 1 - 2 * (i % 2)
        q_ref[...] = selection(blk)
        combine(q_ref, blk, range(d_model // step))

        @pl.when(i % 2 == 0)
        def _():
            swap_copy(i // 2).start()

        @pl.when(i % 2 == 1)
        def _():
            swap_copy(i // 2).wait_recv()
            split_rows(i // 2, everything)

        @pl.when(i == 1)
        def _():
            shipped["first_own"] = ship(0, lambda: c_ref.at[0], lambda: rf_ref.at[0], YN)

        @pl.when(i == 3)
        def _():
            shipped["far_second"] = ship(4, lambda: d_ref.at[1], lambda: rs_ref.at[2], XN)
        return carry

    lax.fori_loop(0, n_dev - 2, others, 0)

    for copy in first_far:
        copy.wait_recv()
    gp_ref[...] = (c_ref[2] + rf_ref[1]).astype(BF16)
    far_first = ship(5, lambda: gp_ref, lambda: gx_ref, XN)
    for copy in hop:
        copy.wait_recv()
    d_ref[0] = d_ref[0] + rs_ref[0]
    second = ship(3, lambda: d_ref.at[0], lambda: rs_ref.at[1], YN)

    shipped["first_own"].wait_recv()
    c_ref[4] = (c_ref[4] + rf_ref[0]).astype(BF16).astype(F32)
    shipped["far_second"].wait_recv()
    d_ref[2] = d_ref[2] + rs_ref[2]
    far_first.wait_recv()
    c_ref[4] = c_ref[4] + gx_ref[...].astype(F32)
    second.wait_recv()
    y_ref[...] = (c_ref[4] + (d_ref[2] + rs_ref[1]).astype(BF16).astype(F32)).astype(BF16)
    for copy in pending:
        copy.wait_send()
    for h in range(n_dev // 2 - 1):
        swap_copy(h).wait_send()


def solution(mesh):
    n_grp = mesh.shape["grp"]
    n_loc = mesh.shape["loc"]
    tok_spec = P(("part", "grp", "loc"), None)
    w_spec = P(("grp", "loc"), None, None)

    def device_step(x_tok, expert_ids, gate_val, w_gate, w_up, w_down):
        tok, d_model = x_tok.shape
        top_k = expert_ids.shape[1]
        n_exp, _, ff = w_gate.shape
        n_dev = n_grp * n_loc
        n_tok = tok * n_dev
        cap = 8 * (n_tok * top_k // (4 * n_exp * n_dev) + 1)
        rows = n_exp * cap
        n_slot = 9
        vmem = pltpu.VMEM
        dma = pltpu.SemaphoreType.DMA
        dims = (n_loc, n_grp, n_exp, cap, top_k, n_slot)
        return pl.pallas_call(
            functools.partial(moe_kernel, dims),
            out_shape=jax.ShapeDtypeStruct((tok, d_model), BF16),
            in_specs=[pl.BlockSpec(memory_space=pl.ANY)] * 6,
            out_specs=pl.BlockSpec(memory_space=vmem),
            scratch_shapes=[
                vmem((n_tok, d_model), BF16),
                vmem((n_dev, top_k, tok), jnp.int32),
                vmem((n_dev, top_k, tok), F32),
                vmem((32, n_tok), F32),
                vmem((32, n_tok), F32),
                vmem((n_tok, 8), F32),
                vmem((rows, 1), F32),
                vmem((PACK * cap, n_tok), BF16),
                vmem((rows, d_model), BF16),
                vmem((PAIR, cap, ff), BF16),
                vmem((3, rows, d_model), BF16),
                vmem((tok, rows), BF16),
                vmem((tok, rows), BF16),
                vmem((tok, rows), BF16),
                vmem((n_dev, tok, d_model), F32),
                vmem((n_dev // 2, tok, d_model), F32),
                vmem((2, tok, d_model), F32),
                vmem((3, tok, d_model), F32),
                vmem((tok, d_model), BF16),
                vmem((tok, d_model), BF16),
                vmem((n_slot, d_model, 2 * ff), BF16),
                vmem((n_slot, ff, d_model), BF16),
                dma((3,)),
                dma((n_slot, 3)),
                dma((14,)),
                dma((16,)),
                dma((7, 2)),
                dma((7, 2)),
                dma((n_dev // 2,)),
                dma((n_dev // 2,)),
                dma((6,)),
                dma((6,)),
                dma((2, 3)),
                dma((2, 3)),
            ],
            compiler_params=pltpu.CompilerParams(
                collective_id=0, has_side_effects=True, vmem_limit_bytes=67043328),
            name="moe",
        )(x_tok, expert_ids.T, gate_val.T, w_gate, w_up, w_down)

    return jax.shard_map(device_step, mesh=mesh, in_specs=(tok_spec, tok_spec, tok_spec, w_spec, w_spec, w_spec), out_specs=tok_spec, check_vma=False)
```

```python
import functools

import jax
import jax.numpy as jnp
from jax import lax
from jax.experimental import pallas as pl
from jax.experimental.pallas import tpu as pltpu
from jax.sharding import PartitionSpec as P

F32 = jnp.float32
BF16 = jnp.bfloat16
PACK = 5
PAIR = 2
PARTS = [(0,), (1, 2), (3, 4)]


YN, YP, DG, DP = (0, 0, 1), (0, 1, 1), (1, 0, 1), (1, 1, 1)
XN, XP, ME, PC = (1, 0, 0), (1, 1, 0), (0, 0, 0), (0, 1, 0)
ORDER = [YN, YP, XN, XP, ME, PC, DG, DP]


def flip(a, b):
    return tuple((i + j) % 2 for i, j in zip(a, b))


def moe_kernel(dims, x_ref, ids_ref, gates_ref, wg_ref, wu_ref, wd_ref, y_ref,
               x_all, ids_own, gates_own, meta_all, pos_ref, ge_ref, cols_ref, gate_ref, oh_ref, packed, hid_ref, osp, qp_ref, qn_ref,
               c_ref, d_ref, rf_ref, rs_ref, gp_ref, gx_ref, wgu, wdn,
               in_sem, w_sem, o_sem, xs_sem, xr_sem, ms_sem, mr_sem, ds_sem, dr_sem, ts_sem, tr_sem, ns_sem, nr_sem):
    n_loc, n_grp, n_exp, cap, top_k, n_in, n_out = dims
    tok, d_model = x_ref.shape
    half = tok // 2
    own = ORDER.index(ME)
    ff = wg_ref.shape[2]
    n_dev = n_loc * n_grp
    n_tok = tok * n_dev
    rows = n_exp * cap
    l = lax.axis_index("loc")
    g = lax.axis_index("grp")
    gx, gc = g // 2, g % 2

    def dev(to):
        fx, fc, fl = to
        return {"grp": ((gx + fx) % 2) * 2 + (gc + fc) % 2, "loc": (l + fl) % 2}

    def in_copies(e):
        slot = e % n_in
        return (
            pltpu.make_async_copy(wg_ref.at[e], wgu.at[slot, :, pl.ds(0, ff)], w_sem.at[slot, 0]),
            pltpu.make_async_copy(wu_ref.at[e], wgu.at[slot, :, pl.ds(ff, ff)], w_sem.at[slot, 1]),
        )

    def out_copy(e):
        slot = e % n_out
        return pltpu.make_async_copy(wd_ref.at[e], wdn.at[slot], o_sem.at[slot])

    def start_weights(e, carry):
        for copy in in_copies(e):
            copy.start()

        @pl.when(e < n_out)
        def _():
            out_copy(e).start()
        return carry

    loads = [
        pltpu.make_async_copy(src, dst, in_sem.at[i]) for i, (src, dst) in enumerate((
            (x_ref, x_all.at[pl.ds(own * tok, tok), :]), (ids_ref, ids_own), (gates_ref, gates_own)))]
    for copy in loads:
        copy.start()

    peers = [r for r in ORDER if r != ME]
    barrier = pltpu.get_barrier_semaphore()
    for r in peers:
        pl.semaphore_signal(barrier, inc=1, device_id=dev(r), device_id_type=pl.DeviceIdType.MESH)
    lax.fori_loop(0, n_in, start_weights, 0)
    for copy in loads:
        copy.wait()
    meta_all[own] = jnp.zeros_like(meta_all[own])
    meta_all[own, 0:top_k, :] = ids_own[...].astype(F32)
    meta_all[own, 8:8 + top_k, :] = gates_own[...]
    pl.semaphore_wait(barrier, len(peers))

    pending = []

    class Sent:
        def __init__(self, *described):
            self.described = described
            self.copy().start()
            pending.append(self)

        def copy(self):
            src, dst, s_sem, r_sem, to = self.described
            return pltpu.make_async_remote_copy(
                src_ref=src(), dst_ref=dst(), send_sem=s_sem(), recv_sem=r_sem(),
                device_id=dev(to), device_id_type=pl.DeviceIdType.MESH)

        def wait_recv(self):
            self.copy().wait_recv()

        def wait_send(self):
            self.copy().wait_send()

    def send(src, dst, s_sem, r_sem, to):
        return Sent(lambda: src, lambda: dst, lambda: s_sem, lambda: r_sem, to)

    def x_rows(at, part):
        return x_all.at[pl.ds(ORDER.index(at) * tok + part * half, half), :]

    got = {}

    def send_x(src, part, to, at):
        i = len(got)
        got[at, part] = Sent(lambda: x_rows(*src), lambda: x_rows(at, part), lambda: xs_sem.at[i],
                             lambda: xr_sem.at[ORDER.index(at) * 2 + part], to)

    send_x((ME, 0), 0, XN, XN)
    send_x((ME, 1), 1, YN, YN)
    metas = [send(meta_all.at[own], meta_all.at[ORDER.index(r)], ms_sem.at[i], mr_sem.at[i], r)
             for i, r in enumerate(peers)]
    for part, to in ((1, XN), (0, YN), (0, PC), (1, PC)):
        send_x((ME, part), part, to, to)

    for copy in metas:
        copy.wait_recv()

    ids_t = jnp.concatenate([meta_all[d, 0:8, :] for d in range(n_dev)], axis=1)
    gts_t = jnp.concatenate([meta_all[d, 8:16, :] for d in range(n_dev)], axis=1)
    e_rows = 32
    e_iota = lax.broadcasted_iota(jnp.int32, (e_rows, n_tok), 0)
    e_ids = jnp.where(e_iota < n_exp, e_iota + (g * n_loc + l) * n_exp, -5).astype(F32)
    mask = jnp.zeros((e_rows, n_tok), F32)
    gate_e = jnp.zeros((e_rows, n_tok), F32)
    for j in range(top_k):
        eq = ids_t[j:j + 1, :] == e_ids
        mask = mask + jnp.where(eq, 1.0, 0.0)
        gate_e = gate_e + jnp.where(eq, gts_t[j:j + 1, :], 0.0)
    blocks = [mask[:, d * tok:(d + 1) * tok] for d in range(n_dev)]
    tri = (lax.broadcasted_iota(jnp.int32, (tok, tok), 0) < lax.broadcasted_iota(jnp.int32, (tok, tok), 1))
    tri = jnp.where(tri, 1.0, 0.0).astype(BF16)
    prefix = jnp.dot(jnp.concatenate(blocks, axis=0).astype(BF16), tri, preferred_element_type=F32)
    offset = jnp.zeros((e_rows, 1), F32)
    pos = []
    for d in range(n_dev):
        pos.append(prefix[d * e_rows:(d + 1) * e_rows, :] + offset)
        offset = offset + jnp.sum(blocks[d], axis=1, keepdims=True)
    pos = jnp.concatenate(pos, axis=1)
    pos_ref[...] = jnp.where(mask > 0.0, pos, -1.0)
    ge_ref[...] = gate_e
    slot_id = e_iota.astype(F32) * float(cap) + pos + 1.0
    slot_rows = [jnp.sum(jnp.where(ids_t[j:j + 1, :] == e_ids, slot_id, 0.0), axis=0, keepdims=True) - 1.0
                 for j in range(top_k)]

    def group_hit(grp):
        low = (lax.broadcasted_iota(jnp.int32, (1, n_tok), 1) * 0 + grp * (n_loc * n_exp)).astype(F32)
        hit = jnp.zeros((1, n_tok), F32)
        for j in range(top_k):
            inside = (ids_t[j:j + 1, :] >= low) & (ids_t[j:j + 1, :] < low + float(n_loc * n_exp))
            hit = jnp.where(inside, 1.0, hit)
        return hit

    own_hit = group_hit(g)
    slot_rows += [own_hit, own_hit * group_hit(gx * 2 + (gc + 1) % 2)]
    slot_t = jnp.concatenate(slot_rows, axis=0)
    for d in range(n_dev):
        cols_ref[pl.ds(d * tok, tok), :] = jnp.transpose(slot_t[:, d * tok:(d + 1) * tok])

    def selection(blk):
        cols = cols_ref[pl.ds(pl.multiple_of(blk * tok, tok), tok), :]
        lanes = lax.broadcasted_iota(jnp.int32, (tok, rows), 1).astype(F32)
        hit = cols[:, 0:1] == lanes
        for j in range(1, top_k):
            hit = hit | (cols[:, j:j + 1] == lanes)
        return jnp.where(hit, 1.0, 0.0).astype(BF16)

    qp_ref[...] = selection(ORDER.index(DP))
    qn_ref[...] = selection(ORDER.index(DG))

    def forward(at, part, hops):
        for to in hops:
            send_x((at, part), part, to, flip(at, to))

    def landed(at, part):
        got[at, part].wait_recv()

    landed(XN, 0)
    forward(XN, 0, [YN, PC])
    landed(YN, 1)
    forward(YN, 1, [XN, PC])
    landed(XN, 1)
    forward(XN, 1, [PC])
    landed(YN, 0)
    forward(YN, 0, [PC])
    landed(YP, 0)
    landed(YP, 1)

    step = 256

    def pack(first, count, add, midway):
        toks = pl.ds(first, count)

        def body(p, carry):
            for i in range(PACK):
                e = p * PACK + i
                where = lax.broadcasted_iota(jnp.int32, (cap, count), 0).astype(F32) == pos_ref[pl.ds(e, 1), toks]
                oh_ref[pl.ds(i * cap, cap), pl.ds(0, count)] = jnp.where(where, 1.0, 0.0).astype(BF16)
                gate = jnp.sum(jnp.where(where, ge_ref[pl.ds(e, 1), toks], 0.0), axis=1, keepdims=True)
                at = pl.ds(pl.multiple_of(e * cap, 16), cap)
                gate_ref[at, :] = gate_ref[at, :] + gate if add else gate
            at = pl.ds(pl.multiple_of(p * (PACK * cap), 16), PACK * cap)
            for n in range(d_model // step):
                cols = pl.ds(n * step, step)
                part = jnp.dot(oh_ref[:, pl.ds(0, count)], x_all[toks, cols], preferred_element_type=F32)
                if add:
                    part = part + packed[at, cols].astype(F32)
                packed[at, cols] = part.astype(BF16)
            if midway is not None:
                @pl.when(p == 1)
                def _():
                    midway()
            return carry

        lax.fori_loop(0, n_exp // PACK, body, 0)

    def diagonal():
        for part in (0, 1):
            landed(DG, part)
            forward(DG, part, [PC])

    for at in (XP, PC):
        landed(at, 0)
        landed(at, 1)
    pack(0, n_tok - 2 * tok, False, diagonal)
    landed(DP, 0)
    landed(DP, 1)
    pack(n_tok - 2 * tok, 2 * tok, True, None)

    def first_dot(e, i):
        at = pl.ds(pl.multiple_of(e * cap, 16), cap)
        uv = jnp.dot(packed[at, :], wgu[e % n_in], preferred_element_type=F32)
        return (jax.nn.silu(uv[:, :ff]) * uv[:, ff:]).astype(BF16)

    def second_dot(hid, e):
        at = pl.ds(pl.multiple_of(e * cap, 16), cap)
        out = jnp.dot(hid, wdn[e % n_out], preferred_element_type=F32) * gate_ref[at, :]
        hi = out.astype(BF16)
        rest = out - hi.astype(F32)
        mid = rest.astype(BF16)
        osp[0, at, :] = hi
        osp[1, at, :] = mid
        osp[2, at, :] = (rest - mid.astype(F32)).astype(BF16)

    def wait_in(e):
        for copy in in_copies(e):
            copy.wait()

    for i in range(PAIR):
        wait_in(i)
    for i in range(PAIR):
        hid_ref[i] = first_dot(i, i)

    def experts(p, carry):
        now = [p * PAIR + i for i in range(PAIR)]
        for e in now:
            wait_in(e + PAIR)
            out_copy(e).wait()
        held = [hid_ref[i] for i in range(PAIR)]
        for i, e in enumerate(now):
            second_dot(held[i], e)
            hid_ref[i] = first_dot(e + PAIR, i)

        for e in now:
            @pl.when(e + PAIR + n_in < n_exp)
            def _():
                for copy in in_copies(e + PAIR + n_in):
                    copy.start()

            @pl.when(e + n_out < n_exp)
            def _():
                out_copy(e + n_out).start()
        return carry

    for i in range(PAIR):
        if i + n_in < n_exp:
            for copy in in_copies(i + n_in):
                copy.start()
    lax.fori_loop(0, n_exp // PAIR - 1, experts, 0)
    for i in range(PAIR):
        out_copy(n_exp - PAIR + i).wait()
    for i in range(PAIR):
        second_dot(hid_ref[i], n_exp - PAIR + i)

    def combine(q, buf, chunks):
        for n in chunks:
            at = pl.ds(n * step, step)
            total = jnp.dot(q[...], osp[0, :, at], preferred_element_type=F32)
            total += jnp.dot(q[...], osp[1, :, at], preferred_element_type=F32)
            total += jnp.dot(q[...], osp[2, :, at], preferred_element_type=F32)
            c_ref[buf, :, at] = total

    def swap_copy(h):
        return pltpu.make_async_remote_copy(
            src_ref=c_ref.at[n_dev // 2 + (h + 1) % 2], dst_ref=d_ref.at[h], send_sem=ds_sem.at[h], recv_sem=dr_sem.at[h],
            device_id=dev(PC), device_id_type=pl.DeviceIdType.MESH)

    everything = pl.ds(0, d_model)

    def split_rows(h, at):
        cols = cols_ref[pl.ds(pl.multiple_of(2 * h * tok, tok), tok), :]
        mine = c_ref[h, :, at]
        other = d_ref[h, :, at]
        c_ref[h, :, at] = jnp.where(cols[:, 6:7] > 0.5, mine, other)
        d_ref[h, :, at] = jnp.where(cols[:, 7:8] > 0.5, other, 0.0)

    def ship(i, src, dst, to):
        return Sent(src, dst, lambda: ts_sem.at[i], lambda: tr_sem.at[i], to)

    first_far = []
    hop = []
    far = ORDER.index(DG) // 2
    swaps = []
    for i, chunks in enumerate(PARTS):
        at = pl.ds(chunks[0] * step, len(chunks) * step)
        combine(qp_ref, n_dev // 2, chunks)
        swaps.append(send(c_ref.at[n_dev // 2, :, at], d_ref.at[far, :, at], ns_sem.at[i, 0], nr_sem.at[i, 0], PC))
        combine(qn_ref, far, chunks)
        swaps[i].wait_recv()
        split_rows(far, at)
        first_far.append(send(c_ref.at[far, :, at], rf_ref.at[1, :, at], ns_sem.at[i, 1], nr_sem.at[i, 1], YN))
        hop.append(send(d_ref.at[far, :, at], rs_ref.at[0, :, at], ns_sem.at[i, 2], nr_sem.at[i, 2], XN))
    for copy in swaps:
        copy.wait_send()
        pending.remove(copy)

    shipped = {}

    def others(i, carry):
        h = i // 2

        @pl.when(i == 4)
        def _():
            swap_copy(0).wait_send()

        qp_ref[...] = selection(i + 1 - 2 * (i % 2))
        combine(qp_ref, (i % 2) * h + (1 - i % 2) * (n_dev // 2 + (h + 1) % 2), range(d_model // step))

        @pl.when(i % 2 == 0)
        def _():
            swap_copy(h).start()

        @pl.when(i % 2 == 1)
        def _():
            swap_copy(h).wait_recv()
            split_rows(h, everything)

        @pl.when(i == 1)
        def _():
            shipped["first_own"] = ship(0, lambda: c_ref.at[0], lambda: rf_ref.at[0], YN)

        @pl.when(i == 3)
        def _():
            shipped["far_second"] = ship(4, lambda: d_ref.at[1], lambda: rs_ref.at[2], XN)
        return carry

    lax.fori_loop(0, n_dev - 2, others, 0)

    for copy in first_far:
        copy.wait_recv()
    gp_ref[...] = (c_ref[1] + rf_ref[1]).astype(BF16)
    far_first = ship(5, lambda: gp_ref, lambda: gx_ref, XN)
    for copy in hop:
        copy.wait_recv()
    d_ref[0] = d_ref[0] + rs_ref[0]
    second = ship(3, lambda: d_ref.at[0], lambda: rs_ref.at[1], YN)

    shipped["first_own"].wait_recv()
    c_ref[2] = (c_ref[2] + rf_ref[0]).astype(BF16).astype(F32)
    shipped["far_second"].wait_recv()
    d_ref[2] = d_ref[2] + rs_ref[2]
    far_first.wait_recv()
    c_ref[2] = c_ref[2] + gx_ref[...].astype(F32)
    second.wait_recv()
    y_ref[...] = (c_ref[2] + (d_ref[2] + rs_ref[1]).astype(BF16).astype(F32)).astype(BF16)
    for copy in pending:
        copy.wait_send()
    for h in range(1, n_dev // 2 - 1):
        swap_copy(h).wait_send()


def solution(mesh):
    n_grp = mesh.shape["grp"]
    n_loc = mesh.shape["loc"]
    tok_spec = P(("part", "grp", "loc"), None)
    w_spec = P(("grp", "loc"), None, None)

    def device_step(x_tok, expert_ids, gate_val, w_gate, w_up, w_down):
        tok, d_model = x_tok.shape
        top_k = expert_ids.shape[1]
        n_exp, _, ff = w_gate.shape
        n_dev = n_grp * n_loc
        n_tok = tok * n_dev
        cap = 8 * (n_tok * top_k // (4 * n_exp * n_dev) + 1)
        rows = n_exp * cap
        n_in, n_out = 11, 10
        vmem = pltpu.VMEM
        dma = pltpu.SemaphoreType.DMA
        dims = (n_loc, n_grp, n_exp, cap, top_k, n_in, n_out)
        return pl.pallas_call(
            functools.partial(moe_kernel, dims),
            out_shape=jax.ShapeDtypeStruct((tok, d_model), BF16),
            in_specs=[pl.BlockSpec(memory_space=pl.ANY)] * 6,
            out_specs=pl.BlockSpec(memory_space=vmem),
            scratch_shapes=[
                vmem((n_tok, d_model), BF16),
                vmem((top_k, tok), jnp.int32),
                vmem((top_k, tok), F32),
                vmem((n_dev, 16, tok), F32),
                vmem((32, n_tok), F32),
                vmem((32, n_tok), F32),
                vmem((n_tok, 8), F32),
                vmem((rows, 1), F32),
                vmem((PACK * cap, n_tok), BF16),
                vmem((rows, d_model), BF16),
                vmem((PAIR, cap, ff), BF16),
                vmem((3, rows, d_model), BF16),
                vmem((tok, rows), BF16),
                vmem((tok, rows), BF16),
                vmem((n_dev // 2 + 2, tok, d_model), F32),
                vmem((n_dev // 2, tok, d_model), F32),
                vmem((2, tok, d_model), F32),
                vmem((3, tok, d_model), F32),
                vmem((tok, d_model), BF16),
                vmem((tok, d_model), BF16),
                vmem((n_in, d_model, 2 * ff), BF16),
                vmem((n_out, ff, d_model), BF16),
                dma((3,)),
                dma((n_in, 2)),
                dma((n_out,)),
                dma((14,)),
                dma((16,)),
                dma((7,)),
                dma((7,)),
                dma((n_dev // 2,)),
                dma((n_dev // 2,)),
                dma((6,)),
                dma((6,)),
                dma((3, 3)),
                dma((3, 3)),
            ],
            compiler_params=pltpu.CompilerParams(
                collective_id=0, has_side_effects=True, vmem_limit_bytes=67043328),
            name="moe",
        )(x_tok, expert_ids.T, gate_val.T, w_gate, w_up, w_down)

    return jax.shard_map(device_step, mesh=mesh, in_specs=(tok_spec, tok_spec, tok_spec, w_spec, w_spec, w_spec), out_specs=tok_spec, check_vma=False)
```

```python
import functools

import jax
import jax.numpy as jnp
from jax import lax
from jax.experimental import pallas as pl
from jax.experimental.pallas import tpu as pltpu
from jax.sharding import PartitionSpec as P

F32 = jnp.float32
BF16 = jnp.bfloat16
PACK = 5
PAIR = 2
PARTS = [(0,), (1, 2), (3, 4)]


YN, YP, DG, DP = (0, 0, 1), (0, 1, 1), (1, 0, 1), (1, 1, 1)
XN, XP, ME, PC = (1, 0, 0), (1, 1, 0), (0, 0, 0), (0, 1, 0)
ORDER = [YN, YP, XN, XP, ME, PC, DG, DP]


def flip(a, b):
    return tuple((i + j) % 2 for i, j in zip(a, b))


def moe_kernel(dims, x_ref, ids_ref, gates_ref, wg_ref, wu_ref, wd_ref, y_ref,
               x_all, ids_own, gates_own, meta_all, pos_ref, ge_ref, cols_ref, gate_ref, oh_ref, packed, hid_ref, osp, qp_ref, qn_ref,
               c_ref, d_ref, rf_ref, rs_ref, gp_ref, gx_ref, wgu, wdn,
               in_sem, w_sem, o_sem, xs_sem, xr_sem, ms_sem, mr_sem, ds_sem, dr_sem, ts_sem, tr_sem, ns_sem, nr_sem):
    n_loc, n_grp, n_exp, cap, top_k, n_in, n_out = dims
    tok, d_model = x_ref.shape
    half = tok // 2
    own = ORDER.index(ME)
    ff = wg_ref.shape[2]
    n_dev = n_loc * n_grp
    n_tok = tok * n_dev
    rows = n_exp * cap
    l = lax.axis_index("loc")
    g = lax.axis_index("grp")
    gx, gc = g // 2, g % 2

    def dev(to):
        fx, fc, fl = to
        return {"grp": ((gx + fx) % 2) * 2 + (gc + fc) % 2, "loc": (l + fl) % 2}

    def in_copies(e):
        slot = e % n_in
        return (
            pltpu.make_async_copy(wg_ref.at[e], wgu.at[slot, :, pl.ds(0, ff)], w_sem.at[slot, 0]),
            pltpu.make_async_copy(wu_ref.at[e], wgu.at[slot, :, pl.ds(ff, ff)], w_sem.at[slot, 1]),
        )

    def out_copy(e):
        slot = e % n_out
        return pltpu.make_async_copy(wd_ref.at[e], wdn.at[slot], o_sem.at[slot])

    def start_weights(e, carry):
        for copy in in_copies(e):
            copy.start()

        @pl.when(e < n_out)
        def _():
            out_copy(e).start()
        return carry

    loads = [
        pltpu.make_async_copy(src, dst, in_sem.at[i]) for i, (src, dst) in enumerate((
            (x_ref, x_all.at[pl.ds(own * tok, tok), :]), (ids_ref, ids_own), (gates_ref, gates_own)))]
    for copy in loads:
        copy.start()

    peers = [r for r in ORDER if r != ME]
    barrier = pltpu.get_barrier_semaphore()
    for r in peers:
        pl.semaphore_signal(barrier, inc=1, device_id=dev(r), device_id_type=pl.DeviceIdType.MESH)
    lax.fori_loop(0, n_in, start_weights, 0)
    for copy in loads:
        copy.wait()
    meta_all[own] = jnp.zeros_like(meta_all[own])
    meta_all[own, 0:top_k, :] = ids_own[...].astype(F32)
    meta_all[own, 8:8 + top_k, :] = gates_own[...]
    pl.semaphore_wait(barrier, len(peers))

    pending = []

    class Sent:
        def __init__(self, *described):
            self.described = described
            self.copy().start()
            pending.append(self)

        def copy(self):
            src, dst, s_sem, r_sem, to = self.described
            return pltpu.make_async_remote_copy(
                src_ref=src(), dst_ref=dst(), send_sem=s_sem(), recv_sem=r_sem(),
                device_id=dev(to), device_id_type=pl.DeviceIdType.MESH)

        def wait_recv(self):
            self.copy().wait_recv()

        def wait_send(self):
            self.copy().wait_send()

    def send(src, dst, s_sem, r_sem, to):
        return Sent(lambda: src, lambda: dst, lambda: s_sem, lambda: r_sem, to)

    def x_rows(at, part):
        return x_all.at[pl.ds(ORDER.index(at) * tok + part * half, half), :]

    got = {}

    def send_x(src, part, to, at):
        i = len(got)
        got[at, part] = Sent(lambda: x_rows(*src), lambda: x_rows(at, part), lambda: xs_sem.at[i],
                             lambda: xr_sem.at[ORDER.index(at) * 2 + part], to)

    send_x((ME, 0), 0, XN, XN)
    send_x((ME, 1), 1, YN, YN)
    metas = [send(meta_all.at[own], meta_all.at[ORDER.index(r)], ms_sem.at[i], mr_sem.at[i], r)
             for i, r in enumerate(peers)]
    for part, to in ((1, XN), (0, YN), (0, PC), (1, PC)):
        send_x((ME, part), part, to, to)

    def forward(at, part, hops):
        for to in hops:
            send_x((at, part), part, to, flip(at, to))

    def landed(at, part):
        got[at, part].wait_recv()

    landed(XN, 0)
    forward(XN, 0, [YN, PC])
    landed(YN, 1)
    forward(YN, 1, [XN, PC])

    for copy in metas:
        copy.wait_recv()

    ids_t = jnp.concatenate([meta_all[d, 0:8, :] for d in range(n_dev)], axis=1)
    gts_t = jnp.concatenate([meta_all[d, 8:16, :] for d in range(n_dev)], axis=1)
    e_rows = 32
    e_iota = lax.broadcasted_iota(jnp.int32, (e_rows, n_tok), 0)
    e_ids = jnp.where(e_iota < n_exp, e_iota + (g * n_loc + l) * n_exp, -5).astype(F32)
    mask = jnp.zeros((e_rows, n_tok), F32)
    gate_e = jnp.zeros((e_rows, n_tok), F32)
    for j in range(top_k):
        eq = ids_t[j:j + 1, :] == e_ids
        mask = mask + jnp.where(eq, 1.0, 0.0)
        gate_e = gate_e + jnp.where(eq, gts_t[j:j + 1, :], 0.0)
    blocks = [mask[:, d * tok:(d + 1) * tok] for d in range(n_dev)]
    tri = (lax.broadcasted_iota(jnp.int32, (tok, tok), 0) < lax.broadcasted_iota(jnp.int32, (tok, tok), 1))
    tri = jnp.where(tri, 1.0, 0.0).astype(BF16)
    prefix = jnp.dot(jnp.concatenate(blocks, axis=0).astype(BF16), tri, preferred_element_type=F32)
    offset = jnp.zeros((e_rows, 1), F32)
    pos = []
    for d in range(n_dev):
        pos.append(prefix[d * e_rows:(d + 1) * e_rows, :] + offset)
        offset = offset + jnp.sum(blocks[d], axis=1, keepdims=True)
    pos = jnp.concatenate(pos, axis=1)
    pos_ref[...] = jnp.where(mask > 0.0, pos, -1.0)
    ge_ref[...] = gate_e
    slot_id = e_iota.astype(F32) * float(cap) + pos + 1.0
    slot_rows = [jnp.sum(jnp.where(ids_t[j:j + 1, :] == e_ids, slot_id, 0.0), axis=0, keepdims=True) - 1.0
                 for j in range(top_k)]

    def group_hit(grp):
        low = (lax.broadcasted_iota(jnp.int32, (1, n_tok), 1) * 0 + grp * (n_loc * n_exp)).astype(F32)
        hit = jnp.zeros((1, n_tok), F32)
        for j in range(top_k):
            inside = (ids_t[j:j + 1, :] >= low) & (ids_t[j:j + 1, :] < low + float(n_loc * n_exp))
            hit = jnp.where(inside, 1.0, hit)
        return hit

    own_hit = group_hit(g)
    slot_rows += [own_hit, own_hit * group_hit(gx * 2 + (gc + 1) % 2)]
    slot_t = jnp.concatenate(slot_rows, axis=0)
    for d in range(n_dev):
        cols_ref[pl.ds(d * tok, tok), :] = jnp.transpose(slot_t[:, d * tok:(d + 1) * tok])

    def selection(blk):
        cols = cols_ref[pl.ds(pl.multiple_of(blk * tok, tok), tok), :]
        lanes = lax.broadcasted_iota(jnp.int32, (tok, rows), 1).astype(F32)
        hit = cols[:, 0:1] == lanes
        for j in range(1, top_k):
            hit = hit | (cols[:, j:j + 1] == lanes)
        return jnp.where(hit, 1.0, 0.0).astype(BF16)

    qp_ref[...] = selection(ORDER.index(DP))
    qn_ref[...] = selection(ORDER.index(DG))

    landed(XN, 1)
    forward(XN, 1, [PC])
    landed(YN, 0)
    forward(YN, 0, [PC])
    landed(YP, 0)
    landed(YP, 1)

    step = 256

    def pack(first, count, add, midway):
        toks = pl.ds(first, count)

        def body(p, carry):
            for i in range(PACK):
                e = p * PACK + i
                where = lax.broadcasted_iota(jnp.int32, (cap, count), 0).astype(F32) == pos_ref[pl.ds(e, 1), toks]
                oh_ref[pl.ds(i * cap, cap), pl.ds(0, count)] = jnp.where(where, 1.0, 0.0).astype(BF16)
                gate = jnp.sum(jnp.where(where, ge_ref[pl.ds(e, 1), toks], 0.0), axis=1, keepdims=True)
                at = pl.ds(pl.multiple_of(e * cap, 16), cap)
                gate_ref[at, :] = gate_ref[at, :] + gate if add else gate
            at = pl.ds(pl.multiple_of(p * (PACK * cap), 16), PACK * cap)
            for n in range(d_model // step):
                cols = pl.ds(n * step, step)
                part = jnp.dot(oh_ref[:, pl.ds(0, count)], x_all[toks, cols], preferred_element_type=F32)
                if add:
                    part = part + packed[at, cols].astype(F32)
                packed[at, cols] = part.astype(BF16)
            if midway is not None:
                @pl.when(p == 1)
                def _():
                    midway()
            return carry

        lax.fori_loop(0, n_exp // PACK, body, 0)

    def diagonal():
        for part in (0, 1):
            landed(DG, part)
            forward(DG, part, [PC])

    for at in (XP, PC):
        landed(at, 0)
        landed(at, 1)
    pack(0, n_tok - 2 * tok, False, diagonal)
    landed(DP, 0)
    landed(DP, 1)
    pack(n_tok - 2 * tok, 2 * tok, True, None)

    def first_dot(e, i):
        at = pl.ds(pl.multiple_of(e * cap, 16), cap)
        uv = jnp.dot(packed[at, :], wgu[e % n_in], preferred_element_type=F32)
        return (jax.nn.silu(uv[:, :ff]) * uv[:, ff:]).astype(BF16)

    def second_dot(hid, e):
        at = pl.ds(pl.multiple_of(e * cap, 16), cap)
        out = jnp.dot(hid, wdn[e % n_out], preferred_element_type=F32) * gate_ref[at, :]
        hi = out.astype(BF16)
        rest = out - hi.astype(F32)
        mid = rest.astype(BF16)
        osp[0, at, :] = hi
        osp[1, at, :] = mid
        osp[2, at, :] = (rest - mid.astype(F32)).astype(BF16)

    def wait_in(e):
        for copy in in_copies(e):
            copy.wait()

    for i in range(PAIR):
        wait_in(i)
    for i in range(PAIR):
        hid_ref[i] = first_dot(i, i)

    def experts(p, carry):
        now = [p * PAIR + i for i in range(PAIR)]
        for e in now:
            wait_in(e + PAIR)
            out_copy(e).wait()
        held = [hid_ref[i] for i in range(PAIR)]
        for i, e in enumerate(now):
            second_dot(held[i], e)
            hid_ref[i] = first_dot(e + PAIR, i)

        for e in now:
            @pl.when(e + PAIR + n_in < n_exp)
            def _():
                for copy in in_copies(e + PAIR + n_in):
                    copy.start()

            @pl.when(e + n_out < n_exp)
            def _():
                out_copy(e + n_out).start()
        return carry

    for i in range(PAIR):
        if i + n_in < n_exp:
            for copy in in_copies(i + n_in):
                copy.start()
    lax.fori_loop(0, n_exp // PAIR - 1, experts, 0)
    for i in range(PAIR):
        out_copy(n_exp - PAIR + i).wait()
    for i in range(PAIR):
        second_dot(hid_ref[i], n_exp - PAIR + i)

    def combine(q, buf, chunks):
        for n in chunks:
            at = pl.ds(n * step, step)
            total = jnp.dot(q[...], osp[0, :, at], preferred_element_type=F32)
            total += jnp.dot(q[...], osp[1, :, at], preferred_element_type=F32)
            total += jnp.dot(q[...], osp[2, :, at], preferred_element_type=F32)
            c_ref[buf, :, at] = total

    def swap_copy(h):
        return pltpu.make_async_remote_copy(
            src_ref=c_ref.at[n_dev // 2 + (h + 1) % 2], dst_ref=d_ref.at[h], send_sem=ds_sem.at[h], recv_sem=dr_sem.at[h],
            device_id=dev(PC), device_id_type=pl.DeviceIdType.MESH)

    everything = pl.ds(0, d_model)

    def split_rows(h, at):
        cols = cols_ref[pl.ds(pl.multiple_of(2 * h * tok, tok), tok), :]
        mine = c_ref[h, :, at]
        other = d_ref[h, :, at]
        c_ref[h, :, at] = jnp.where(cols[:, 6:7] > 0.5, mine, other)
        d_ref[h, :, at] = jnp.where(cols[:, 7:8] > 0.5, other, 0.0)

    def ship(i, src, dst, to):
        return Sent(src, dst, lambda: ts_sem.at[i], lambda: tr_sem.at[i], to)

    first_far = []
    hop = []
    far = ORDER.index(DG) // 2
    swaps = []
    for i, chunks in enumerate(PARTS):
        at = pl.ds(chunks[0] * step, len(chunks) * step)
        combine(qp_ref, n_dev // 2, chunks)
        swaps.append(send(c_ref.at[n_dev // 2, :, at], d_ref.at[far, :, at], ns_sem.at[i, 0], nr_sem.at[i, 0], PC))
        combine(qn_ref, far, chunks)
        swaps[i].wait_recv()
        split_rows(far, at)
        first_far.append(send(c_ref.at[far, :, at], rf_ref.at[1, :, at], ns_sem.at[i, 1], nr_sem.at[i, 1], YN))
        hop.append(send(d_ref.at[far, :, at], rs_ref.at[0, :, at], ns_sem.at[i, 2], nr_sem.at[i, 2], XN))
    for copy in swaps:
        copy.wait_send()
        pending.remove(copy)

    shipped = {}

    def others(i, carry):
        h = i // 2

        @pl.when(i == 4)
        def _():
            swap_copy(0).wait_send()

        qp_ref[...] = selection(i + 1 - 2 * (i % 2))
        combine(qp_ref, (i % 2) * h + (1 - i % 2) * (n_dev // 2 + (h + 1) % 2), range(d_model // step))

        @pl.when(i % 2 == 0)
        def _():
            swap_copy(h).start()

        @pl.when(i % 2 == 1)
        def _():
            swap_copy(h).wait_recv()
            split_rows(h, everything)

        @pl.when(i == 1)
        def _():
            shipped["first_own"] = ship(0, lambda: c_ref.at[0], lambda: rf_ref.at[0], YN)

        @pl.when(i == 3)
        def _():
            shipped["far_second"] = ship(4, lambda: d_ref.at[1], lambda: rs_ref.at[2], XN)
        return carry

    lax.fori_loop(0, n_dev - 2, others, 0)

    for copy in first_far:
        copy.wait_recv()
    gp_ref[...] = (c_ref[1] + rf_ref[1]).astype(BF16)
    far_first = ship(5, lambda: gp_ref, lambda: gx_ref, XN)
    for copy in hop:
        copy.wait_recv()
    d_ref[0] = d_ref[0] + rs_ref[0]
    second = ship(3, lambda: d_ref.at[0], lambda: rs_ref.at[1], YN)

    shipped["first_own"].wait_recv()
    c_ref[2] = (c_ref[2] + rf_ref[0]).astype(BF16).astype(F32)
    shipped["far_second"].wait_recv()
    d_ref[2] = d_ref[2] + rs_ref[2]
    far_first.wait_recv()
    c_ref[2] = c_ref[2] + gx_ref[...].astype(F32)
    second.wait_recv()
    y_ref[...] = (c_ref[2] + (d_ref[2] + rs_ref[1]).astype(BF16).astype(F32)).astype(BF16)
    for copy in pending:
        copy.wait_send()
    for h in range(1, n_dev // 2 - 1):
        swap_copy(h).wait_send()


def solution(mesh):
    n_grp = mesh.shape["grp"]
    n_loc = mesh.shape["loc"]
    tok_spec = P(("part", "grp", "loc"), None)
    w_spec = P(("grp", "loc"), None, None)

    def device_step(x_tok, expert_ids, gate_val, w_gate, w_up, w_down):
        tok, d_model = x_tok.shape
        top_k = expert_ids.shape[1]
        n_exp, _, ff = w_gate.shape
        n_dev = n_grp * n_loc
        n_tok = tok * n_dev
        cap = 8 * (n_tok * top_k // (4 * n_exp * n_dev) + 1)
        rows = n_exp * cap
        n_in, n_out = 11, 10
        vmem = pltpu.VMEM
        dma = pltpu.SemaphoreType.DMA
        dims = (n_loc, n_grp, n_exp, cap, top_k, n_in, n_out)
        return pl.pallas_call(
            functools.partial(moe_kernel, dims),
            out_shape=jax.ShapeDtypeStruct((tok, d_model), BF16),
            in_specs=[pl.BlockSpec(memory_space=pl.ANY)] * 6,
            out_specs=pl.BlockSpec(memory_space=vmem),
            scratch_shapes=[
                vmem((n_tok, d_model), BF16),
                vmem((top_k, tok), jnp.int32),
                vmem((top_k, tok), F32),
                vmem((n_dev, 16, tok), F32),
                vmem((32, n_tok), F32),
                vmem((32, n_tok), F32),
                vmem((n_tok, 8), F32),
                vmem((rows, 1), F32),
                vmem((PACK * cap, n_tok), BF16),
                vmem((rows, d_model), BF16),
                vmem((PAIR, cap, ff), BF16),
                vmem((3, rows, d_model), BF16),
                vmem((tok, rows), BF16),
                vmem((tok, rows), BF16),
                vmem((n_dev // 2 + 2, tok, d_model), F32),
                vmem((n_dev // 2, tok, d_model), F32),
                vmem((2, tok, d_model), F32),
                vmem((3, tok, d_model), F32),
                vmem((tok, d_model), BF16),
                vmem((tok, d_model), BF16),
                vmem((n_in, d_model, 2 * ff), BF16),
                vmem((n_out, ff, d_model), BF16),
                dma((3,)),
                dma((n_in, 2)),
                dma((n_out,)),
                dma((14,)),
                dma((16,)),
                dma((7,)),
                dma((7,)),
                dma((n_dev // 2,)),
                dma((n_dev // 2,)),
                dma((6,)),
                dma((6,)),
                dma((3, 3)),
                dma((3, 3)),
            ],
            compiler_params=pltpu.CompilerParams(
                collective_id=0, has_side_effects=True, vmem_limit_bytes=67043328),
            name="moe",
        )(x_tok, expert_ids.T, gate_val.T, w_gate, w_up, w_down)

    return jax.shard_map(device_step, mesh=mesh, in_specs=(tok_spec, tok_spec, tok_spec, w_spec, w_spec, w_spec), out_specs=tok_spec, check_vma=False)
```

```python
import functools

import jax
import jax.numpy as jnp
from jax import lax
from jax.experimental import pallas as pl
from jax.experimental.pallas import tpu as pltpu
from jax.sharding import PartitionSpec as P

F32 = jnp.float32
BF16 = jnp.bfloat16
PACK = 5
PAIR = 4
PARTS = [(0,), (1, 2), (3, 4)]


YN, YP, DG, DP = (0, 0, 1), (0, 1, 1), (1, 0, 1), (1, 1, 1)
XN, XP, ME, PC = (1, 0, 0), (1, 1, 0), (0, 0, 0), (0, 1, 0)
ORDER = [YN, YP, XN, XP, ME, PC, DG, DP]


def flip(a, b):
    return tuple((i + j) % 2 for i, j in zip(a, b))


def moe_kernel(dims, x_ref, ids_ref, gates_ref, wg_ref, wu_ref, wd_ref, y_ref,
               x_all, ids_own, gates_own, meta_all, pos_ref, ge_ref, cols_ref, gate_ref, oh_ref, packed, hid_ref, osp, qp_ref, qn_ref,
               c_ref, d_ref, rf_ref, rs_ref, gp_ref, gx_ref, wgu, wdn,
               in_sem, w_sem, o_sem, xs_sem, xr_sem, ms_sem, mr_sem, ds_sem, dr_sem, ts_sem, tr_sem, ns_sem, nr_sem):
    n_loc, n_grp, n_exp, cap, top_k, n_in, n_out = dims
    tok, d_model = x_ref.shape
    half = tok // 2
    own = ORDER.index(ME)
    ff = wg_ref.shape[2]
    n_dev = n_loc * n_grp
    n_tok = tok * n_dev
    rows = n_exp * cap
    l = lax.axis_index("loc")
    g = lax.axis_index("grp")
    gx, gc = g // 2, g % 2

    def dev(to):
        fx, fc, fl = to
        return {"grp": ((gx + fx) % 2) * 2 + (gc + fc) % 2, "loc": (l + fl) % 2}

    def in_copies(e):
        slot = e % n_in
        return (
            pltpu.make_async_copy(wg_ref.at[e], wgu.at[slot, :, pl.ds(0, ff)], w_sem.at[slot, 0]),
            pltpu.make_async_copy(wu_ref.at[e], wgu.at[slot, :, pl.ds(ff, ff)], w_sem.at[slot, 1]),
        )

    def out_copy(e):
        slot = e % n_out
        return pltpu.make_async_copy(wd_ref.at[e], wdn.at[slot], o_sem.at[slot])

    def start_weights(e, carry):
        for copy in in_copies(e):
            copy.start()

        @pl.when(e < n_out)
        def _():
            out_copy(e).start()
        return carry

    loads = [
        pltpu.make_async_copy(src, dst, in_sem.at[i]) for i, (src, dst) in enumerate((
            (x_ref, x_all.at[pl.ds(own * tok, tok), :]), (ids_ref, ids_own), (gates_ref, gates_own)))]
    for copy in loads:
        copy.start()

    peers = [r for r in ORDER if r != ME]
    barrier = pltpu.get_barrier_semaphore()
    for r in peers:
        pl.semaphore_signal(barrier, inc=1, device_id=dev(r), device_id_type=pl.DeviceIdType.MESH)
    lax.fori_loop(0, n_in, start_weights, 0)
    for copy in loads:
        copy.wait()
    meta_all[own] = jnp.zeros_like(meta_all[own])
    meta_all[own, 0:top_k, :] = ids_own[...].astype(F32)
    meta_all[own, 8:8 + top_k, :] = gates_own[...]
    pl.semaphore_wait(barrier, len(peers))

    pending = []

    class Sent:
        def __init__(self, *described):
            self.described = described
            self.copy().start()
            pending.append(self)

        def copy(self):
            src, dst, s_sem, r_sem, to = self.described
            return pltpu.make_async_remote_copy(
                src_ref=src(), dst_ref=dst(), send_sem=s_sem(), recv_sem=r_sem(),
                device_id=dev(to), device_id_type=pl.DeviceIdType.MESH)

        def wait_recv(self):
            self.copy().wait_recv()

        def wait_send(self):
            self.copy().wait_send()

    def send(src, dst, s_sem, r_sem, to):
        return Sent(lambda: src, lambda: dst, lambda: s_sem, lambda: r_sem, to)

    def x_rows(at, part):
        return x_all.at[pl.ds(ORDER.index(at) * tok + part * half, half), :]

    got = {}

    def send_x(src, part, to, at):
        i = len(got)
        got[at, part] = Sent(lambda: x_rows(*src), lambda: x_rows(at, part), lambda: xs_sem.at[i],
                             lambda: xr_sem.at[ORDER.index(at) * 2 + part], to)

    send_x((ME, 0), 0, XN, XN)
    send_x((ME, 1), 1, YN, YN)
    metas = [send(meta_all.at[own], meta_all.at[ORDER.index(r)], ms_sem.at[i], mr_sem.at[i], r)
             for i, r in enumerate(peers)]
    for part, to in ((1, XN), (0, YN), (0, PC), (1, PC)):
        send_x((ME, part), part, to, to)

    def forward(at, part, hops):
        for to in hops:
            send_x((at, part), part, to, flip(at, to))

    def landed(at, part):
        got[at, part].wait_recv()

    landed(XN, 0)
    forward(XN, 0, [YN, PC])
    landed(YN, 1)
    forward(YN, 1, [XN, PC])

    for copy in metas:
        copy.wait_recv()

    ids_t = jnp.concatenate([meta_all[d, 0:8, :] for d in range(n_dev)], axis=1)
    gts_t = jnp.concatenate([meta_all[d, 8:16, :] for d in range(n_dev)], axis=1)
    e_rows = 32
    e_iota = lax.broadcasted_iota(jnp.int32, (e_rows, n_tok), 0)
    e_ids = jnp.where(e_iota < n_exp, e_iota + (g * n_loc + l) * n_exp, -5).astype(F32)
    mask = jnp.zeros((e_rows, n_tok), F32)
    gate_e = jnp.zeros((e_rows, n_tok), F32)
    for j in range(top_k):
        eq = ids_t[j:j + 1, :] == e_ids
        mask = mask + jnp.where(eq, 1.0, 0.0)
        gate_e = gate_e + jnp.where(eq, gts_t[j:j + 1, :], 0.0)
    blocks = [mask[:, d * tok:(d + 1) * tok] for d in range(n_dev)]
    tri = (lax.broadcasted_iota(jnp.int32, (tok, tok), 0) < lax.broadcasted_iota(jnp.int32, (tok, tok), 1))
    tri = jnp.where(tri, 1.0, 0.0).astype(BF16)
    prefix = jnp.dot(jnp.concatenate(blocks, axis=0).astype(BF16), tri, preferred_element_type=F32)
    offset = jnp.zeros((e_rows, 1), F32)
    pos = []
    for d in range(n_dev):
        pos.append(prefix[d * e_rows:(d + 1) * e_rows, :] + offset)
        offset = offset + jnp.sum(blocks[d], axis=1, keepdims=True)
    pos = jnp.concatenate(pos, axis=1)
    pos_ref[...] = jnp.where(mask > 0.0, pos, -1.0)
    ge_ref[...] = gate_e
    slot_id = e_iota.astype(F32) * float(cap) + pos + 1.0
    slot_rows = [jnp.sum(jnp.where(ids_t[j:j + 1, :] == e_ids, slot_id, 0.0), axis=0, keepdims=True) - 1.0
                 for j in range(top_k)]

    def group_hit(grp):
        low = (lax.broadcasted_iota(jnp.int32, (1, n_tok), 1) * 0 + grp * (n_loc * n_exp)).astype(F32)
        hit = jnp.zeros((1, n_tok), F32)
        for j in range(top_k):
            inside = (ids_t[j:j + 1, :] >= low) & (ids_t[j:j + 1, :] < low + float(n_loc * n_exp))
            hit = jnp.where(inside, 1.0, hit)
        return hit

    own_hit = group_hit(g)
    slot_rows += [own_hit, own_hit * group_hit(gx * 2 + (gc + 1) % 2)]
    slot_t = jnp.concatenate(slot_rows, axis=0)
    for d in range(n_dev):
        cols_ref[pl.ds(d * tok, tok), :] = jnp.transpose(slot_t[:, d * tok:(d + 1) * tok])

    def selection(blk):
        cols = cols_ref[pl.ds(pl.multiple_of(blk * tok, tok), tok), :]
        lanes = lax.broadcasted_iota(jnp.int32, (tok, rows), 1).astype(F32)
        hit = cols[:, 0:1] == lanes
        for j in range(1, top_k):
            hit = hit | (cols[:, j:j + 1] == lanes)
        return jnp.where(hit, 1.0, 0.0).astype(BF16)

    qp_ref[...] = selection(ORDER.index(DP))
    qn_ref[...] = selection(ORDER.index(DG))

    step = 256

    def pack(first, count, add, midway):
        toks = pl.ds(first, count)

        def body(p, carry):
            for i in range(PACK):
                e = p * PACK + i
                where = lax.broadcasted_iota(jnp.int32, (cap, count), 0).astype(F32) == pos_ref[pl.ds(e, 1), toks]
                oh_ref[pl.ds(i * cap, cap), pl.ds(0, count)] = jnp.where(where, 1.0, 0.0).astype(BF16)
                gate = jnp.sum(jnp.where(where, ge_ref[pl.ds(e, 1), toks], 0.0), axis=1, keepdims=True)
                at = pl.ds(pl.multiple_of(e * cap, 16), cap)
                gate_ref[at, :] = gate_ref[at, :] + gate if add else gate
            at = pl.ds(pl.multiple_of(p * (PACK * cap), 16), PACK * cap)
            for n in range(d_model // step):
                cols = pl.ds(n * step, step)
                part = jnp.dot(oh_ref[:, pl.ds(0, count)], x_all[toks, cols], preferred_element_type=F32)
                if add:
                    part = part + packed[at, cols].astype(F32)
                packed[at, cols] = part.astype(BF16)
            if midway is not None:
                @pl.when(p == 1)
                def _():
                    midway()
            return carry

        lax.fori_loop(0, n_exp // PACK, body, 0)

    def early():
        landed(XN, 1)
        forward(XN, 1, [PC])
        landed(YN, 0)
        forward(YN, 0, [PC])

    def diagonal():
        for part in (0, 1):
            landed(DG, part)
            forward(DG, part, [PC])

    landed(PC, 0)
    landed(PC, 1)
    pack(4 * tok, 2 * tok, False, early)
    landed(YP, 0)
    landed(YP, 1)
    landed(XP, 0)
    landed(XP, 1)
    pack(0, 4 * tok, True, diagonal)
    landed(DP, 0)
    landed(DP, 1)
    pack(n_tok - 2 * tok, 2 * tok, True, None)

    def first_dot(e, i):
        at = pl.ds(pl.multiple_of(e * cap, 16), cap)
        uv = jnp.dot(packed[at, :], wgu[e % n_in], preferred_element_type=F32)
        return (jax.nn.silu(uv[:, :ff]) * uv[:, ff:]).astype(BF16)

    def second_dot(hid, e):
        at = pl.ds(pl.multiple_of(e * cap, 16), cap)
        out = jnp.dot(hid, wdn[e % n_out], preferred_element_type=F32) * gate_ref[at, :]
        hi = out.astype(BF16)
        rest = out - hi.astype(F32)
        mid = rest.astype(BF16)
        osp[0, at, :] = hi
        osp[1, at, :] = mid
        osp[2, at, :] = (rest - mid.astype(F32)).astype(BF16)

    def wait_in(e):
        for copy in in_copies(e):
            copy.wait()

    for i in range(PAIR):
        wait_in(i)
    for i in range(PAIR):
        hid_ref[i] = first_dot(i, i)

    def experts(p, carry):
        now = [p * PAIR + i for i in range(PAIR)]
        for e in now:
            wait_in(e + PAIR)
            out_copy(e).wait()
        held = [hid_ref[i] for i in range(PAIR)]
        for i, e in enumerate(now):
            second_dot(held[i], e)
            hid_ref[i] = first_dot(e + PAIR, i)

        for e in now:
            @pl.when(e + PAIR + n_in < n_exp)
            def _():
                for copy in in_copies(e + PAIR + n_in):
                    copy.start()

            @pl.when(e + n_out < n_exp)
            def _():
                out_copy(e + n_out).start()
        return carry

    for i in range(PAIR):
        if i + n_in < n_exp:
            for copy in in_copies(i + n_in):
                copy.start()
    lax.fori_loop(0, n_exp // PAIR - 1, experts, 0)
    for i in range(PAIR):
        out_copy(n_exp - PAIR + i).wait()
    for i in range(PAIR):
        second_dot(hid_ref[i], n_exp - PAIR + i)

    def combine(q, buf, chunks):
        for n in chunks:
            at = pl.ds(n * step, step)
            total = jnp.dot(q[...], osp[0, :, at], preferred_element_type=F32)
            total += jnp.dot(q[...], osp[1, :, at], preferred_element_type=F32)
            total += jnp.dot(q[...], osp[2, :, at], preferred_element_type=F32)
            c_ref[buf, :, at] = total

    def swap_copy(h):
        return pltpu.make_async_remote_copy(
            src_ref=c_ref.at[n_dev // 2 + (h + 1) % 2], dst_ref=d_ref.at[h], send_sem=ds_sem.at[h], recv_sem=dr_sem.at[h],
            device_id=dev(PC), device_id_type=pl.DeviceIdType.MESH)

    everything = pl.ds(0, d_model)

    def split_rows(h, at):
        cols = cols_ref[pl.ds(pl.multiple_of(2 * h * tok, tok), tok), :]
        mine = c_ref[h, :, at]
        other = d_ref[h, :, at]
        c_ref[h, :, at] = jnp.where(cols[:, 6:7] > 0.5, mine, other)
        d_ref[h, :, at] = jnp.where(cols[:, 7:8] > 0.5, other, 0.0)

    def ship(i, src, dst, to):
        return Sent(src, dst, lambda: ts_sem.at[i], lambda: tr_sem.at[i], to)

    first_far = []
    hop = []
    far = ORDER.index(DG) // 2
    swaps = []
    for i, chunks in enumerate(PARTS):
        at = pl.ds(chunks[0] * step, len(chunks) * step)
        combine(qp_ref, n_dev // 2, chunks)
        swaps.append(send(c_ref.at[n_dev // 2, :, at], d_ref.at[far, :, at], ns_sem.at[i, 0], nr_sem.at[i, 0], PC))
        combine(qn_ref, far, chunks)
        swaps[i].wait_recv()
        split_rows(far, at)
        first_far.append(send(c_ref.at[far, :, at], rf_ref.at[1, :, at], ns_sem.at[i, 1], nr_sem.at[i, 1], YN))
        hop.append(send(d_ref.at[far, :, at], rs_ref.at[0, :, at], ns_sem.at[i, 2], nr_sem.at[i, 2], XN))
    for copy in swaps:
        copy.wait_send()
        pending.remove(copy)

    shipped = {}

    def others(i, carry):
        h = i // 2

        @pl.when(i == 4)
        def _():
            swap_copy(0).wait_send()

        qp_ref[...] = selection(i + 1 - 2 * (i % 2))
        combine(qp_ref, (i % 2) * h + (1 - i % 2) * (n_dev // 2 + (h + 1) % 2), range(d_model // step))

        @pl.when(i % 2 == 0)
        def _():
            swap_copy(h).start()

        @pl.when(i % 2 == 1)
        def _():
            swap_copy(h).wait_recv()
            split_rows(h, everything)

        @pl.when(i == 1)
        def _():
            shipped["first_own"] = ship(0, lambda: c_ref.at[0], lambda: rf_ref.at[0], YN)

        @pl.when(i == 3)
        def _():
            shipped["far_second"] = ship(4, lambda: d_ref.at[1], lambda: rs_ref.at[2], XN)
        return carry

    lax.fori_loop(0, n_dev - 2, others, 0)

    for copy in first_far:
        copy.wait_recv()
    gp_ref[...] = (c_ref[1] + rf_ref[1]).astype(BF16)
    far_first = ship(5, lambda: gp_ref, lambda: gx_ref, XN)
    for copy in hop:
        copy.wait_recv()
    d_ref[0] = d_ref[0] + rs_ref[0]
    second = ship(3, lambda: d_ref.at[0], lambda: rs_ref.at[1], YN)

    shipped["first_own"].wait_recv()
    c_ref[2] = (c_ref[2] + rf_ref[0]).astype(BF16).astype(F32)
    shipped["far_second"].wait_recv()
    d_ref[2] = d_ref[2] + rs_ref[2]
    far_first.wait_recv()
    c_ref[2] = c_ref[2] + gx_ref[...].astype(F32)
    second.wait_recv()
    y_ref[...] = (c_ref[2] + (d_ref[2] + rs_ref[1]).astype(BF16).astype(F32)).astype(BF16)
    for copy in pending:
        copy.wait_send()
    for h in range(1, n_dev // 2 - 1):
        swap_copy(h).wait_send()


def solution(mesh):
    n_grp = mesh.shape["grp"]
    n_loc = mesh.shape["loc"]
    tok_spec = P(("part", "grp", "loc"), None)
    w_spec = P(("grp", "loc"), None, None)

    def device_step(x_tok, expert_ids, gate_val, w_gate, w_up, w_down):
        tok, d_model = x_tok.shape
        top_k = expert_ids.shape[1]
        n_exp, _, ff = w_gate.shape
        n_dev = n_grp * n_loc
        n_tok = tok * n_dev
        cap = 8 * (n_tok * top_k // (4 * n_exp * n_dev) + 1)
        rows = n_exp * cap
        n_in, n_out = 11, 10
        vmem = pltpu.VMEM
        dma = pltpu.SemaphoreType.DMA
        dims = (n_loc, n_grp, n_exp, cap, top_k, n_in, n_out)
        return pl.pallas_call(
            functools.partial(moe_kernel, dims),
            out_shape=jax.ShapeDtypeStruct((tok, d_model), BF16),
            in_specs=[pl.BlockSpec(memory_space=pl.ANY)] * 6,
            out_specs=pl.BlockSpec(memory_space=vmem),
            scratch_shapes=[
                vmem((n_tok, d_model), BF16),
                vmem((top_k, tok), jnp.int32),
                vmem((top_k, tok), F32),
                vmem((n_dev, 16, tok), F32),
                vmem((32, n_tok), F32),
                vmem((32, n_tok), F32),
                vmem((n_tok, 8), F32),
                vmem((rows, 1), F32),
                vmem((PACK * cap, n_tok), BF16),
                vmem((rows, d_model), BF16),
                vmem((PAIR, cap, ff), BF16),
                vmem((3, rows, d_model), BF16),
                vmem((tok, rows), BF16),
                vmem((tok, rows), BF16),
                vmem((n_dev // 2 + 2, tok, d_model), F32),
                vmem((n_dev // 2, tok, d_model), F32),
                vmem((2, tok, d_model), F32),
                vmem((3, tok, d_model), F32),
                vmem((tok, d_model), BF16),
                vmem((tok, d_model), BF16),
                vmem((n_in, d_model, 2 * ff), BF16),
                vmem((n_out, ff, d_model), BF16),
                dma((3,)),
                dma((n_in, 2)),
                dma((n_out,)),
                dma((14,)),
                dma((16,)),
                dma((7,)),
                dma((7,)),
                dma((n_dev // 2,)),
                dma((n_dev // 2,)),
                dma((6,)),
                dma((6,)),
                dma((3, 3)),
                dma((3, 3)),
            ],
            compiler_params=pltpu.CompilerParams(
                collective_id=0, has_side_effects=True, vmem_limit_bytes=67043328),
            name="moe",
        )(x_tok, expert_ids.T, gate_val.T, w_gate, w_up, w_down)

    return jax.shard_map(device_step, mesh=mesh, in_specs=(tok_spec, tok_spec, tok_spec, w_spec, w_spec, w_spec), out_specs=tok_spec, check_vma=False)
```

```python
import functools

import jax
import jax.numpy as jnp
from jax import lax
from jax.experimental import pallas as pl
from jax.experimental.pallas import tpu as pltpu
from jax.sharding import PartitionSpec as P

F32 = jnp.float32
BF16 = jnp.bfloat16
PACK = 5
PAIR = 2
PARTS = [(0,), (1, 2), (3, 4)]


YN, YP, DG, DP = (0, 0, 1), (0, 1, 1), (1, 0, 1), (1, 1, 1)
XN, XP, ME, PC = (1, 0, 0), (1, 1, 0), (0, 0, 0), (0, 1, 0)
ORDER = [YN, YP, XN, XP, ME, PC, DG, DP]


def flip(a, b):
    return tuple((i + j) % 2 for i, j in zip(a, b))


def moe_kernel(dims, x_ref, ids_ref, gates_ref, wg_ref, wu_ref, wd_ref, y_ref,
               x_all, ids_own, gates_own, meta_all, pos_ref, ge_ref, cols_ref, gate_ref, oh_ref, packed, hid_ref, osp, qp_ref, qn_ref,
               c_ref, d_ref, rf_ref, rs_ref, gp_ref, gx_ref, wgu, wdn,
               in_sem, w_sem, o_sem, xs_sem, xr_sem, ms_sem, mr_sem, ds_sem, dr_sem, ts_sem, tr_sem, ns_sem, nr_sem):
    n_loc, n_grp, n_exp, cap, top_k, n_in, n_out = dims
    tok, d_model = x_ref.shape
    half = tok // 2
    own = ORDER.index(ME)
    ff = wg_ref.shape[2]
    n_dev = n_loc * n_grp
    n_tok = tok * n_dev
    rows = n_exp * cap
    l = lax.axis_index("loc")
    g = lax.axis_index("grp")
    gx, gc = g // 2, g % 2

    def dev(to):
        fx, fc, fl = to
        return {"grp": ((gx + fx) % 2) * 2 + (gc + fc) % 2, "loc": (l + fl) % 2}

    def in_copies(e):
        slot = e % n_in
        return (
            pltpu.make_async_copy(wg_ref.at[e], wgu.at[slot, :, pl.ds(0, ff)], w_sem.at[slot, 0]),
            pltpu.make_async_copy(wu_ref.at[e], wgu.at[slot, :, pl.ds(ff, ff)], w_sem.at[slot, 1]),
        )

    def out_copy(e):
        slot = e % n_out
        return pltpu.make_async_copy(wd_ref.at[e], wdn.at[slot], o_sem.at[slot])

    def start_weights(e, carry):
        for copy in in_copies(e):
            copy.start()

        @pl.when(e < n_out)
        def _():
            out_copy(e).start()
        return carry

    loads = [
        pltpu.make_async_copy(src, dst, in_sem.at[i]) for i, (src, dst) in enumerate((
            (x_ref, x_all.at[pl.ds(own * tok, tok), :]), (ids_ref, ids_own), (gates_ref, gates_own)))]
    for copy in loads:
        copy.start()

    peers = [r for r in ORDER if r != ME]
    barrier = pltpu.get_barrier_semaphore()
    for r in peers:
        pl.semaphore_signal(barrier, inc=1, device_id=dev(r), device_id_type=pl.DeviceIdType.MESH)
    lax.fori_loop(0, n_in, start_weights, 0)
    for copy in loads:
        copy.wait()
    meta_all[own] = jnp.zeros_like(meta_all[own])
    meta_all[own, 0:top_k, :] = ids_own[...].astype(F32)
    meta_all[own, 8:8 + top_k, :] = gates_own[...]
    pl.semaphore_wait(barrier, len(peers))

    pending = []

    class Sent:
        def __init__(self, *described):
            self.described = described
            self.copy().start()
            pending.append(self)

        def copy(self):
            src, dst, s_sem, r_sem, to = self.described
            return pltpu.make_async_remote_copy(
                src_ref=src(), dst_ref=dst(), send_sem=s_sem(), recv_sem=r_sem(),
                device_id=dev(to), device_id_type=pl.DeviceIdType.MESH)

        def wait_recv(self):
            self.copy().wait_recv()

        def wait_send(self):
            self.copy().wait_send()

    def send(src, dst, s_sem, r_sem, to):
        return Sent(lambda: src, lambda: dst, lambda: s_sem, lambda: r_sem, to)

    def x_rows(at, part):
        return x_all.at[pl.ds(ORDER.index(at) * tok + part * half, half), :]

    got = {}

    def send_x(src, part, to, at):
        i = len(got)
        got[at, part] = Sent(lambda: x_rows(*src), lambda: x_rows(at, part), lambda: xs_sem.at[i],
                             lambda: xr_sem.at[ORDER.index(at) * 2 + part], to)

    send_x((ME, 0), 0, XN, XN)
    send_x((ME, 1), 1, YN, YN)
    metas = [send(meta_all.at[own], meta_all.at[ORDER.index(r)], ms_sem.at[i], mr_sem.at[i], r)
             for i, r in enumerate(peers)]
    for part, to in ((1, XN), (0, YN), (0, PC), (1, PC)):
        send_x((ME, part), part, to, to)

    def forward(at, part, hops):
        for to in hops:
            send_x((at, part), part, to, flip(at, to))

    def landed(at, part):
        got[at, part].wait_recv()

    landed(XN, 0)
    forward(XN, 0, [YN, PC])
    landed(YN, 1)
    forward(YN, 1, [XN, PC])

    for copy in metas:
        copy.wait_recv()

    ids_t = jnp.concatenate([meta_all[d, 0:8, :] for d in range(n_dev)], axis=1)
    gts_t = jnp.concatenate([meta_all[d, 8:16, :] for d in range(n_dev)], axis=1)
    e_rows = 32
    e_iota = lax.broadcasted_iota(jnp.int32, (e_rows, n_tok), 0)
    e_ids = jnp.where(e_iota < n_exp, e_iota + (g * n_loc + l) * n_exp, -5).astype(F32)
    mask = jnp.zeros((e_rows, n_tok), F32)
    gate_e = jnp.zeros((e_rows, n_tok), F32)
    for j in range(top_k):
        eq = ids_t[j:j + 1, :] == e_ids
        mask = mask + jnp.where(eq, 1.0, 0.0)
        gate_e = gate_e + jnp.where(eq, gts_t[j:j + 1, :], 0.0)
    blocks = [mask[:, d * tok:(d + 1) * tok] for d in range(n_dev)]
    tri = (lax.broadcasted_iota(jnp.int32, (tok, tok), 0) < lax.broadcasted_iota(jnp.int32, (tok, tok), 1))
    tri = jnp.where(tri, 1.0, 0.0).astype(BF16)
    prefix = jnp.dot(jnp.concatenate(blocks, axis=0).astype(BF16), tri, preferred_element_type=F32)
    offset = jnp.zeros((e_rows, 1), F32)
    pos = []
    for d in range(n_dev):
        pos.append(prefix[d * e_rows:(d + 1) * e_rows, :] + offset)
        offset = offset + jnp.sum(blocks[d], axis=1, keepdims=True)
    pos = jnp.concatenate(pos, axis=1)
    pos_ref[...] = jnp.where(mask > 0.0, pos, -1.0)
    ge_ref[...] = gate_e
    slot_id = e_iota.astype(F32) * float(cap) + pos + 1.0
    slot_rows = [jnp.sum(jnp.where(ids_t[j:j + 1, :] == e_ids, slot_id, 0.0), axis=0, keepdims=True) - 1.0
                 for j in range(top_k)]

    def group_hit(grp):
        low = (lax.broadcasted_iota(jnp.int32, (1, n_tok), 1) * 0 + grp * (n_loc * n_exp)).astype(F32)
        hit = jnp.zeros((1, n_tok), F32)
        for j in range(top_k):
            inside = (ids_t[j:j + 1, :] >= low) & (ids_t[j:j + 1, :] < low + float(n_loc * n_exp))
            hit = jnp.where(inside, 1.0, hit)
        return hit

    own_hit = group_hit(g)
    slot_rows += [own_hit, own_hit * group_hit(gx * 2 + (gc + 1) % 2)]
    slot_t = jnp.concatenate(slot_rows, axis=0)
    for d in range(n_dev):
        cols_ref[pl.ds(d * tok, tok), :] = jnp.transpose(slot_t[:, d * tok:(d + 1) * tok])

    def selection(blk):
        cols = cols_ref[pl.ds(pl.multiple_of(blk * tok, tok), tok), :]
        lanes = lax.broadcasted_iota(jnp.int32, (tok, rows), 1).astype(F32)
        hit = cols[:, 0:1] == lanes
        for j in range(1, top_k):
            hit = hit | (cols[:, j:j + 1] == lanes)
        return jnp.where(hit, 1.0, 0.0).astype(BF16)

    qp_ref[...] = selection(ORDER.index(DP))
    qn_ref[...] = selection(ORDER.index(DG))

    step = 256

    def pack(first, count, add, midway):
        toks = pl.ds(first, count)

        def body(p, carry):
            for i in range(PACK):
                e = p * PACK + i
                where = lax.broadcasted_iota(jnp.int32, (cap, count), 0).astype(F32) == pos_ref[pl.ds(e, 1), toks]
                oh_ref[pl.ds(i * cap, cap), pl.ds(0, count)] = jnp.where(where, 1.0, 0.0).astype(BF16)
                gate = jnp.sum(jnp.where(where, ge_ref[pl.ds(e, 1), toks], 0.0), axis=1, keepdims=True)
                at = pl.ds(pl.multiple_of(e * cap, 16), cap)
                gate_ref[at, :] = gate_ref[at, :] + gate if add else gate
            at = pl.ds(pl.multiple_of(p * (PACK * cap), 16), PACK * cap)
            for n in range(d_model // step):
                cols = pl.ds(n * step, step)
                part = jnp.dot(oh_ref[:, pl.ds(0, count)], x_all[toks, cols], preferred_element_type=F32)
                if add:
                    part = part + packed[at, cols].astype(F32)
                packed[at, cols] = part.astype(BF16)
            if midway is not None:
                @pl.when(p == 1)
                def _():
                    midway()
            return carry

        lax.fori_loop(0, n_exp // PACK, body, 0)

    def early():
        landed(XN, 1)
        forward(XN, 1, [PC])
        landed(YN, 0)
        forward(YN, 0, [PC])

    def diagonal():
        for part in (0, 1):
            landed(DG, part)
            forward(DG, part, [PC])

    landed(PC, 0)
    landed(PC, 1)
    pack(4 * tok, 2 * tok, False, early)
    landed(YP, 0)
    landed(YP, 1)
    landed(XP, 0)
    landed(XP, 1)
    pack(0, 4 * tok, True, diagonal)
    landed(DP, 0)
    landed(DP, 1)
    pack(n_tok - 2 * tok, 2 * tok, True, None)

    def first_dot(e, i):
        at = pl.ds(pl.multiple_of(e * cap, 16), cap)
        uv = jnp.dot(packed[at, :], wgu[e % n_in], preferred_element_type=F32)
        return (jax.nn.silu(uv[:, :ff]) * uv[:, ff:]).astype(BF16)

    def second_dot(hid, e):
        at = pl.ds(pl.multiple_of(e * cap, 16), cap)
        out = jnp.dot(hid, wdn[e % n_out], preferred_element_type=F32) * gate_ref[at, :]
        hi = out.astype(BF16)
        rest = out - hi.astype(F32)
        mid = rest.astype(BF16)
        osp[0, at, :] = hi
        osp[1, at, :] = mid
        osp[2, at, :] = (rest - mid.astype(F32)).astype(BF16)

    def wait_in(e):
        for copy in in_copies(e):
            copy.wait()

    for i in range(PAIR):
        wait_in(i)
    for i in range(PAIR):
        hid_ref[i] = first_dot(i, i)

    def experts(p, carry):
        now = [p * PAIR + i for i in range(PAIR)]
        for e in now:
            wait_in(e + PAIR)
            out_copy(e).wait()
        held = [hid_ref[i] for i in range(PAIR)]
        for i, e in enumerate(now):
            second_dot(held[i], e)
            hid_ref[i] = first_dot(e + PAIR, i)

        for e in now:
            @pl.when(e + PAIR + n_in < n_exp)
            def _():
                for copy in in_copies(e + PAIR + n_in):
                    copy.start()

            @pl.when(e + n_out < n_exp)
            def _():
                out_copy(e + n_out).start()
        return carry

    for i in range(PAIR):
        if i + n_in < n_exp:
            for copy in in_copies(i + n_in):
                copy.start()
    lax.fori_loop(0, n_exp // PAIR - 1, experts, 0)
    for i in range(PAIR):
        out_copy(n_exp - PAIR + i).wait()
    for i in range(PAIR):
        second_dot(hid_ref[i], n_exp - PAIR + i)

    def combine(q, buf, chunks):
        for n in chunks:
            at = pl.ds(n * step, step)
            total = jnp.dot(q[...], osp[0, :, at], preferred_element_type=F32)
            total += jnp.dot(q[...], osp[1, :, at], preferred_element_type=F32)
            total += jnp.dot(q[...], osp[2, :, at], preferred_element_type=F32)
            c_ref[buf, :, at] = total

    def swap_copy(h):
        return pltpu.make_async_remote_copy(
            src_ref=c_ref.at[n_dev // 2 + (h + 1) % 2], dst_ref=d_ref.at[h], send_sem=ds_sem.at[h], recv_sem=dr_sem.at[h],
            device_id=dev(PC), device_id_type=pl.DeviceIdType.MESH)

    everything = pl.ds(0, d_model)

    def split_rows(h, at):
        cols = cols_ref[pl.ds(pl.multiple_of(2 * h * tok, tok), tok), :]
        mine = c_ref[h, :, at]
        other = d_ref[h, :, at]
        c_ref[h, :, at] = jnp.where(cols[:, 6:7] > 0.5, mine, other)
        d_ref[h, :, at] = jnp.where(cols[:, 7:8] > 0.5, other, 0.0)

    def ship(i, src, dst, to):
        return Sent(src, dst, lambda: ts_sem.at[i], lambda: tr_sem.at[i], to)

    first_far = []
    hop = []
    far = ORDER.index(DG) // 2
    swaps = []
    for i, chunks in enumerate(PARTS):
        at = pl.ds(chunks[0] * step, len(chunks) * step)
        combine(qp_ref, n_dev // 2, chunks)
        swaps.append(send(c_ref.at[n_dev // 2, :, at], d_ref.at[far, :, at], ns_sem.at[i, 0], nr_sem.at[i, 0], PC))
        combine(qn_ref, far, chunks)
        swaps[i].wait_recv()
        split_rows(far, at)
        first_far.append(send(c_ref.at[far, :, at], rf_ref.at[1, :, at], ns_sem.at[i, 1], nr_sem.at[i, 1], YN))
        hop.append(send(d_ref.at[far, :, at], rs_ref.at[0, :, at], ns_sem.at[i, 2], nr_sem.at[i, 2], XN))
    for copy in swaps:
        copy.wait_send()
        pending.remove(copy)

    shipped = {}

    def others(i, carry):
        h = i // 2

        @pl.when(i == 4)
        def _():
            swap_copy(0).wait_send()

        qp_ref[...] = selection(i + 1 - 2 * (i % 2))
        combine(qp_ref, (i % 2) * h + (1 - i % 2) * (n_dev // 2 + (h + 1) % 2), range(d_model // step))

        @pl.when(i % 2 == 0)
        def _():
            swap_copy(h).start()

        @pl.when(i % 2 == 1)
        def _():
            swap_copy(h).wait_recv()
            split_rows(h, everything)

        @pl.when(i == 1)
        def _():
            shipped["first_own"] = ship(0, lambda: c_ref.at[0], lambda: rf_ref.at[0], YN)

        @pl.when(i == 3)
        def _():
            shipped["far_second"] = ship(4, lambda: d_ref.at[1], lambda: rs_ref.at[2], XN)
        return carry

    lax.fori_loop(0, n_dev - 2, others, 0)

    for copy in first_far:
        copy.wait_recv()
    gp_ref[...] = (c_ref[1] + rf_ref[1]).astype(BF16)
    far_first = ship(5, lambda: gp_ref, lambda: gx_ref, XN)
    for copy in hop:
        copy.wait_recv()
    d_ref[0] = d_ref[0] + rs_ref[0]
    second = ship(3, lambda: d_ref.at[0], lambda: rs_ref.at[1], YN)

    shipped["first_own"].wait_recv()
    c_ref[2] = (c_ref[2] + rf_ref[0]).astype(BF16).astype(F32)
    shipped["far_second"].wait_recv()
    d_ref[2] = d_ref[2] + rs_ref[2]
    far_first.wait_recv()
    c_ref[2] = c_ref[2] + gx_ref[...].astype(F32)
    second.wait_recv()
    y_ref[...] = (c_ref[2] + (d_ref[2] + rs_ref[1]).astype(BF16).astype(F32)).astype(BF16)
    for copy in pending:
        copy.wait_send()
    for h in range(1, n_dev // 2 - 1):
        swap_copy(h).wait_send()


def solution(mesh):
    n_grp = mesh.shape["grp"]
    n_loc = mesh.shape["loc"]
    tok_spec = P(("part", "grp", "loc"), None)
    w_spec = P(("grp", "loc"), None, None)

    def device_step(x_tok, expert_ids, gate_val, w_gate, w_up, w_down):
        tok, d_model = x_tok.shape
        top_k = expert_ids.shape[1]
        n_exp, _, ff = w_gate.shape
        n_dev = n_grp * n_loc
        n_tok = tok * n_dev
        cap = 8 * (n_tok * top_k // (4 * n_exp * n_dev) + 1)
        rows = n_exp * cap
        n_in, n_out = 11, 10
        vmem = pltpu.VMEM
        dma = pltpu.SemaphoreType.DMA
        dims = (n_loc, n_grp, n_exp, cap, top_k, n_in, n_out)
        return pl.pallas_call(
            functools.partial(moe_kernel, dims),
            out_shape=jax.ShapeDtypeStruct((tok, d_model), BF16),
            in_specs=[pl.BlockSpec(memory_space=pl.ANY)] * 6,
            out_specs=pl.BlockSpec(memory_space=vmem),
            scratch_shapes=[
                vmem((n_tok, d_model), BF16),
                vmem((top_k, tok), jnp.int32),
                vmem((top_k, tok), F32),
                vmem((n_dev, 16, tok), F32),
                vmem((32, n_tok), F32),
                vmem((32, n_tok), F32),
                vmem((n_tok, 8), F32),
                vmem((rows, 1), F32),
                vmem((PACK * cap, n_tok), BF16),
                vmem((rows, d_model), BF16),
                vmem((PAIR, cap, ff), BF16),
                vmem((3, rows, d_model), BF16),
                vmem((tok, rows), BF16),
                vmem((tok, rows), BF16),
                vmem((n_dev // 2 + 2, tok, d_model), F32),
                vmem((n_dev // 2, tok, d_model), F32),
                vmem((2, tok, d_model), F32),
                vmem((3, tok, d_model), F32),
                vmem((tok, d_model), BF16),
                vmem((tok, d_model), BF16),
                vmem((n_in, d_model, 2 * ff), BF16),
                vmem((n_out, ff, d_model), BF16),
                dma((3,)),
                dma((n_in, 2)),
                dma((n_out,)),
                dma((14,)),
                dma((16,)),
                dma((7,)),
                dma((7,)),
                dma((n_dev // 2,)),
                dma((n_dev // 2,)),
                dma((6,)),
                dma((6,)),
                dma((3, 3)),
                dma((3, 3)),
            ],
            compiler_params=pltpu.CompilerParams(
                collective_id=0, has_side_effects=True, vmem_limit_bytes=67043328),
            name="moe",
        )(x_tok, expert_ids.T, gate_val.T, w_gate, w_up, w_down)

    return jax.shard_map(device_step, mesh=mesh, in_specs=(tok_spec, tok_spec, tok_spec, w_spec, w_spec, w_spec), out_specs=tok_spec, check_vma=False)
```

```python
import functools

import jax
import jax.numpy as jnp
from jax import lax
from jax.experimental import pallas as pl
from jax.experimental.pallas import tpu as pltpu
from jax.sharding import PartitionSpec as P

F32 = jnp.float32
BF16 = jnp.bfloat16
PACK = 5
PAIR = 2
PARTS = [(0,), (1, 2), (3, 4)]


YN, YP, DG, DP = (0, 0, 1), (0, 1, 1), (1, 0, 1), (1, 1, 1)
XN, XP, ME, PC = (1, 0, 0), (1, 1, 0), (0, 0, 0), (0, 1, 0)
ORDER = [YN, YP, XN, XP, ME, PC, DG, DP]


def flip(a, b):
    return tuple((i + j) % 2 for i, j in zip(a, b))


def moe_kernel(dims, x_ref, ids_ref, gates_ref, wg_ref, wu_ref, wd_ref, y_ref,
               x_all, ids_own, gates_own, meta_all, pos_ref, ge_ref, cols_ref, gate_ref, oh_ref, packed, hid_ref, osp, qp_ref, qn_ref,
               c_ref, d_ref, rf_ref, rs_ref, gp_ref, gx_ref, wgu, wdn,
               in_sem, w_sem, o_sem, xs_sem, xr_sem, ms_sem, mr_sem, ds_sem, dr_sem, ts_sem, tr_sem, ns_sem, nr_sem):
    n_loc, n_grp, n_exp, cap, top_k, n_in, n_out = dims
    tok, d_model = x_ref.shape
    half = tok // 2
    own = ORDER.index(ME)
    ff = wg_ref.shape[2]
    n_dev = n_loc * n_grp
    n_tok = tok * n_dev
    rows = n_exp * cap
    l = lax.axis_index("loc")
    g = lax.axis_index("grp")
    gx, gc = g // 2, g % 2

    def dev(to):
        fx, fc, fl = to
        return {"grp": ((gx + fx) % 2) * 2 + (gc + fc) % 2, "loc": (l + fl) % 2}

    def in_copies(e):
        slot = e % n_in
        return (
            pltpu.make_async_copy(wg_ref.at[e], wgu.at[slot, :, pl.ds(0, ff)], w_sem.at[slot, 0]),
            pltpu.make_async_copy(wu_ref.at[e], wgu.at[slot, :, pl.ds(ff, ff)], w_sem.at[slot, 1]),
        )

    def out_copy(e):
        slot = e % n_out
        return pltpu.make_async_copy(wd_ref.at[e], wdn.at[slot], o_sem.at[slot])

    def start_weights(e, carry):
        for copy in in_copies(e):
            copy.start()

        @pl.when(e < n_out)
        def _():
            out_copy(e).start()
        return carry

    loads = [
        pltpu.make_async_copy(src, dst, in_sem.at[i]) for i, (src, dst) in enumerate((
            (x_ref, x_all.at[pl.ds(own * tok, tok), :]), (ids_ref, ids_own), (gates_ref, gates_own)))]
    for copy in loads:
        copy.start()

    peers = [r for r in ORDER if r != ME]
    barrier = pltpu.get_barrier_semaphore()
    for r in peers:
        pl.semaphore_signal(barrier, inc=1, device_id=dev(r), device_id_type=pl.DeviceIdType.MESH)
    lax.fori_loop(0, n_in, start_weights, 0)
    for copy in loads:
        copy.wait()
    meta_all[own] = jnp.zeros_like(meta_all[own])
    meta_all[own, 0:top_k, :] = ids_own[...].astype(F32)
    meta_all[own, 8:8 + top_k, :] = gates_own[...]
    pl.semaphore_wait(barrier, len(peers))

    pending = []

    class Sent:
        def __init__(self, *described):
            self.described = described
            self.copy().start()
            pending.append(self)

        def copy(self):
            src, dst, s_sem, r_sem, to = self.described
            return pltpu.make_async_remote_copy(
                src_ref=src(), dst_ref=dst(), send_sem=s_sem(), recv_sem=r_sem(),
                device_id=dev(to), device_id_type=pl.DeviceIdType.MESH)

        def wait_recv(self):
            self.copy().wait_recv()

        def wait_send(self):
            self.copy().wait_send()

    def send(src, dst, s_sem, r_sem, to):
        return Sent(lambda: src, lambda: dst, lambda: s_sem, lambda: r_sem, to)

    def x_rows(at, part):
        return x_all.at[pl.ds(ORDER.index(at) * tok + part * half, half), :]

    got = {}

    def send_x(src, part, to, at):
        i = len(got)
        got[at, part] = Sent(lambda: x_rows(*src), lambda: x_rows(at, part), lambda: xs_sem.at[i],
                             lambda: xr_sem.at[ORDER.index(at) * 2 + part], to)

    send_x((ME, 0), 0, XN, XN)
    send_x((ME, 1), 1, YN, YN)
    metas = [send(meta_all.at[own], meta_all.at[ORDER.index(r)], ms_sem.at[i], mr_sem.at[i], r)
             for i, r in enumerate(peers)]
    for part, to in ((1, XN), (0, YN), (0, PC), (1, PC)):
        send_x((ME, part), part, to, to)

    def forward(at, part, hops):
        for to in hops:
            send_x((at, part), part, to, flip(at, to))

    def landed(at, part):
        got[at, part].wait_recv()

    landed(XN, 0)
    forward(XN, 0, [YN, PC])
    landed(YN, 1)
    forward(YN, 1, [XN, PC])

    for copy in metas:
        copy.wait_recv()

    ids_t = jnp.concatenate([meta_all[d, 0:8, :] for d in range(n_dev)], axis=1)
    gts_t = jnp.concatenate([meta_all[d, 8:16, :] for d in range(n_dev)], axis=1)
    e_rows = 32
    e_iota = lax.broadcasted_iota(jnp.int32, (e_rows, n_tok), 0)
    e_ids = jnp.where(e_iota < n_exp, e_iota + (g * n_loc + l) * n_exp, -5).astype(F32)
    mask = jnp.zeros((e_rows, n_tok), F32)
    gate_e = jnp.zeros((e_rows, n_tok), F32)
    for j in range(top_k):
        eq = ids_t[j:j + 1, :] == e_ids
        mask = mask + jnp.where(eq, 1.0, 0.0)
        gate_e = gate_e + jnp.where(eq, gts_t[j:j + 1, :], 0.0)
    blocks = [mask[:, d * tok:(d + 1) * tok] for d in range(n_dev)]
    tri = (lax.broadcasted_iota(jnp.int32, (tok, tok), 0) < lax.broadcasted_iota(jnp.int32, (tok, tok), 1))
    tri = jnp.where(tri, 1.0, 0.0).astype(BF16)
    prefix = jnp.dot(jnp.concatenate(blocks, axis=0).astype(BF16), tri, preferred_element_type=F32)
    offset = jnp.zeros((e_rows, 1), F32)
    pos = []
    for d in range(n_dev):
        pos.append(prefix[d * e_rows:(d + 1) * e_rows, :] + offset)
        offset = offset + jnp.sum(blocks[d], axis=1, keepdims=True)
    pos = jnp.concatenate(pos, axis=1)
    pos_ref[...] = jnp.where(mask > 0.0, pos, -1.0)
    ge_ref[...] = gate_e
    slot_id = e_iota.astype(F32) * float(cap) + pos + 1.0
    slot_rows = [jnp.sum(jnp.where(ids_t[j:j + 1, :] == e_ids, slot_id, 0.0), axis=0, keepdims=True) - 1.0
                 for j in range(top_k)]

    def group_hit(grp):
        low = (lax.broadcasted_iota(jnp.int32, (1, n_tok), 1) * 0 + grp * (n_loc * n_exp)).astype(F32)
        hit = jnp.zeros((1, n_tok), F32)
        for j in range(top_k):
            inside = (ids_t[j:j + 1, :] >= low) & (ids_t[j:j + 1, :] < low + float(n_loc * n_exp))
            hit = jnp.where(inside, 1.0, hit)
        return hit

    own_hit = group_hit(g)
    slot_rows += [own_hit, own_hit * group_hit(gx * 2 + (gc + 1) % 2)]
    slot_t = jnp.concatenate(slot_rows, axis=0)
    for d in range(n_dev):
        cols_ref[pl.ds(d * tok, tok), :] = jnp.transpose(slot_t[:, d * tok:(d + 1) * tok])

    def selection(blk):
        cols = cols_ref[pl.ds(pl.multiple_of(blk * tok, tok), tok), :]
        lanes = lax.broadcasted_iota(jnp.int32, (tok, rows), 1).astype(F32)
        hit = cols[:, 0:1] == lanes
        for j in range(1, top_k):
            hit = hit | (cols[:, j:j + 1] == lanes)
        return jnp.where(hit, 1.0, 0.0).astype(BF16)

    qp_ref[...] = selection(ORDER.index(DP))
    qn_ref[...] = selection(ORDER.index(DG))

    step = 256

    def pack(first, count, add, midway):
        toks = pl.ds(first, count)

        def body(p, carry):
            for i in range(PACK):
                e = p * PACK + i
                where = lax.broadcasted_iota(jnp.int32, (cap, count), 0).astype(F32) == pos_ref[pl.ds(e, 1), toks]
                oh_ref[pl.ds(i * cap, cap), pl.ds(0, count)] = jnp.where(where, 1.0, 0.0).astype(BF16)
                gate = jnp.sum(jnp.where(where, ge_ref[pl.ds(e, 1), toks], 0.0), axis=1, keepdims=True)
                at = pl.ds(pl.multiple_of(e * cap, 16), cap)
                gate_ref[at, :] = gate_ref[at, :] + gate if add else gate
            at = pl.ds(pl.multiple_of(p * (PACK * cap), 16), PACK * cap)
            for n in range(d_model // step):
                cols = pl.ds(n * step, step)
                part = jnp.dot(oh_ref[:, pl.ds(0, count)], x_all[toks, cols], preferred_element_type=F32)
                if add:
                    part = part + packed[at, cols].astype(F32)
                packed[at, cols] = part.astype(BF16)
            if midway is not None:
                @pl.when(p == 1)
                def _():
                    midway()
            return carry

        lax.fori_loop(0, n_exp // PACK, body, 0)

    def early():
        landed(XN, 1)
        forward(XN, 1, [PC])
        landed(YN, 0)
        forward(YN, 0, [PC])

    def diagonal():
        for part in (0, 1):
            landed(DG, part)
            forward(DG, part, [PC])

    landed(PC, 0)
    landed(PC, 1)
    pack(4 * tok, 2 * tok, False, early)
    landed(YP, 0)
    landed(YP, 1)
    landed(XP, 0)
    landed(XP, 1)
    pack(0, 4 * tok, True, diagonal)
    landed(DP, 0)
    landed(DP, 1)

    def pack_late(e, count):
        toks = pl.ds(n_tok - 2 * tok, 2 * tok)
        picks = []
        for i in range(count):
            where = lax.broadcasted_iota(jnp.int32, (cap, 2 * tok), 0).astype(F32) == pos_ref[pl.ds(e + i, 1), toks]
            picks.append(jnp.where(where, 1.0, 0.0).astype(BF16))
            at = pl.ds(pl.multiple_of((e + i) * cap, 16), cap)
            gate_ref[at, :] += jnp.sum(jnp.where(where, ge_ref[pl.ds(e + i, 1), toks], 0.0), axis=1, keepdims=True)
        pick = jnp.concatenate(picks, axis=0)
        at = pl.ds(pl.multiple_of(e * cap, 16), count * cap)
        for n in range(d_model // step):
            cols = pl.ds(n * step, step)
            part = jnp.dot(pick, x_all[toks, cols], preferred_element_type=F32)
            packed[at, cols] = (part + packed[at, cols].astype(F32)).astype(BF16)

    pack_late(0, 2 * PAIR)

    def first_dot(e, i):
        at = pl.ds(pl.multiple_of(e * cap, 16), cap)
        uv = jnp.dot(packed[at, :], wgu[e % n_in], preferred_element_type=F32)
        return (jax.nn.silu(uv[:, :ff]) * uv[:, ff:]).astype(BF16)

    def second_dot(hid, e):
        at = pl.ds(pl.multiple_of(e * cap, 16), cap)
        out = jnp.dot(hid, wdn[e % n_out], preferred_element_type=F32) * gate_ref[at, :]
        hi = out.astype(BF16)
        rest = out - hi.astype(F32)
        mid = rest.astype(BF16)
        osp[0, at, :] = hi
        osp[1, at, :] = mid
        osp[2, at, :] = (rest - mid.astype(F32)).astype(BF16)

    def wait_in(e):
        for copy in in_copies(e):
            copy.wait()

    for i in range(PAIR):
        wait_in(i)
    for i in range(PAIR):
        hid_ref[i] = first_dot(i, i)

    def experts(p, late):
        now = [p * PAIR + i for i in range(PAIR)]
        for e in now:
            wait_in(e + PAIR)
            out_copy(e).wait()
        held = [hid_ref[i] for i in range(PAIR)]
        for i, e in enumerate(now):
            second_dot(held[i], e)
            hid_ref[i] = first_dot(e + PAIR, i)
        if late:
            pack_late((p + 2) * PAIR, PAIR)

        for e in now:
            @pl.when(e + PAIR + n_in < n_exp)
            def _():
                for copy in in_copies(e + PAIR + n_in):
                    copy.start()

            @pl.when(e + n_out < n_exp)
            def _():
                out_copy(e + n_out).start()

    for i in range(PAIR):
        if i + n_in < n_exp:
            for copy in in_copies(i + n_in):
                copy.start()
    def turn(p, carry):
        experts(p, True)
        return carry

    lax.fori_loop(0, n_exp // PAIR - 2, turn, 0)
    experts(n_exp // PAIR - 2, False)
    for i in range(PAIR):
        out_copy(n_exp - PAIR + i).wait()
    for i in range(PAIR):
        second_dot(hid_ref[i], n_exp - PAIR + i)

    def combine(q, buf, chunks):
        for n in chunks:
            at = pl.ds(n * step, step)
            total = jnp.dot(q[...], osp[0, :, at], preferred_element_type=F32)
            total += jnp.dot(q[...], osp[1, :, at], preferred_element_type=F32)
            total += jnp.dot(q[...], osp[2, :, at], preferred_element_type=F32)
            c_ref[buf, :, at] = total

    def swap_copy(h):
        return pltpu.make_async_remote_copy(
            src_ref=c_ref.at[n_dev // 2 + (h + 1) % 2], dst_ref=d_ref.at[h], send_sem=ds_sem.at[h], recv_sem=dr_sem.at[h],
            device_id=dev(PC), device_id_type=pl.DeviceIdType.MESH)

    everything = pl.ds(0, d_model)

    def split_rows(h, at):
        cols = cols_ref[pl.ds(pl.multiple_of(2 * h * tok, tok), tok), :]
        mine = c_ref[h, :, at]
        other = d_ref[h, :, at]
        c_ref[h, :, at] = jnp.where(cols[:, 6:7] > 0.5, mine, other)
        d_ref[h, :, at] = jnp.where(cols[:, 7:8] > 0.5, other, 0.0)

    def ship(i, src, dst, to):
        return Sent(src, dst, lambda: ts_sem.at[i], lambda: tr_sem.at[i], to)

    first_far = []
    hop = []
    far = ORDER.index(DG) // 2
    swaps = []
    for i, chunks in enumerate(PARTS):
        at = pl.ds(chunks[0] * step, len(chunks) * step)
        combine(qp_ref, n_dev // 2, chunks)
        swaps.append(send(c_ref.at[n_dev // 2, :, at], d_ref.at[far, :, at], ns_sem.at[i, 0], nr_sem.at[i, 0], PC))
        combine(qn_ref, far, chunks)
        swaps[i].wait_recv()
        split_rows(far, at)
        first_far.append(send(c_ref.at[far, :, at], rf_ref.at[1, :, at], ns_sem.at[i, 1], nr_sem.at[i, 1], YN))
        hop.append(send(d_ref.at[far, :, at], rs_ref.at[0, :, at], ns_sem.at[i, 2], nr_sem.at[i, 2], XN))
    for copy in swaps:
        copy.wait_send()
        pending.remove(copy)

    shipped = {}

    def others(i, carry):
        h = i // 2

        @pl.when(i == 4)
        def _():
            swap_copy(0).wait_send()

        qp_ref[...] = selection(i + 1 - 2 * (i % 2))
        combine(qp_ref, (i % 2) * h + (1 - i % 2) * (n_dev // 2 + (h + 1) % 2), range(d_model // step))

        @pl.when(i % 2 == 0)
        def _():
            swap_copy(h).start()

        @pl.when(i % 2 == 1)
        def _():
            swap_copy(h).wait_recv()
            split_rows(h, everything)

        @pl.when(i == 1)
        def _():
            shipped["first_own"] = ship(0, lambda: c_ref.at[0], lambda: rf_ref.at[0], YN)

        @pl.when(i == 3)
        def _():
            shipped["far_second"] = ship(4, lambda: d_ref.at[1], lambda: rs_ref.at[2], XN)
        return carry

    lax.fori_loop(0, n_dev - 2, others, 0)

    for copy in first_far:
        copy.wait_recv()
    gp_ref[...] = (c_ref[1] + rf_ref[1]).astype(BF16)
    far_first = ship(5, lambda: gp_ref, lambda: gx_ref, XN)
    for copy in hop:
        copy.wait_recv()
    d_ref[0] = d_ref[0] + rs_ref[0]
    second = ship(3, lambda: d_ref.at[0], lambda: rs_ref.at[1], YN)

    shipped["first_own"].wait_recv()
    c_ref[2] = (c_ref[2] + rf_ref[0]).astype(BF16).astype(F32)
    shipped["far_second"].wait_recv()
    d_ref[2] = d_ref[2] + rs_ref[2]
    far_first.wait_recv()
    c_ref[2] = c_ref[2] + gx_ref[...].astype(F32)
    second.wait_recv()
    y_ref[...] = (c_ref[2] + (d_ref[2] + rs_ref[1]).astype(BF16).astype(F32)).astype(BF16)
    for copy in pending:
        copy.wait_send()
    for h in range(1, n_dev // 2 - 1):
        swap_copy(h).wait_send()


def solution(mesh):
    n_grp = mesh.shape["grp"]
    n_loc = mesh.shape["loc"]
    tok_spec = P(("part", "grp", "loc"), None)
    w_spec = P(("grp", "loc"), None, None)

    def device_step(x_tok, expert_ids, gate_val, w_gate, w_up, w_down):
        tok, d_model = x_tok.shape
        top_k = expert_ids.shape[1]
        n_exp, _, ff = w_gate.shape
        n_dev = n_grp * n_loc
        n_tok = tok * n_dev
        cap = 8 * (n_tok * top_k // (4 * n_exp * n_dev) + 1)
        rows = n_exp * cap
        n_in, n_out = 11, 10
        vmem = pltpu.VMEM
        dma = pltpu.SemaphoreType.DMA
        dims = (n_loc, n_grp, n_exp, cap, top_k, n_in, n_out)
        return pl.pallas_call(
            functools.partial(moe_kernel, dims),
            out_shape=jax.ShapeDtypeStruct((tok, d_model), BF16),
            in_specs=[pl.BlockSpec(memory_space=pl.ANY)] * 6,
            out_specs=pl.BlockSpec(memory_space=vmem),
            scratch_shapes=[
                vmem((n_tok, d_model), BF16),
                vmem((top_k, tok), jnp.int32),
                vmem((top_k, tok), F32),
                vmem((n_dev, 16, tok), F32),
                vmem((32, n_tok), F32),
                vmem((32, n_tok), F32),
                vmem((n_tok, 8), F32),
                vmem((rows, 1), F32),
                vmem((PACK * cap, n_tok), BF16),
                vmem((rows, d_model), BF16),
                vmem((PAIR, cap, ff), BF16),
                vmem((3, rows, d_model), BF16),
                vmem((tok, rows), BF16),
                vmem((tok, rows), BF16),
                vmem((n_dev // 2 + 2, tok, d_model), F32),
                vmem((n_dev // 2, tok, d_model), F32),
                vmem((2, tok, d_model), F32),
                vmem((3, tok, d_model), F32),
                vmem((tok, d_model), BF16),
                vmem((tok, d_model), BF16),
                vmem((n_in, d_model, 2 * ff), BF16),
                vmem((n_out, ff, d_model), BF16),
                dma((3,)),
                dma((n_in, 2)),
                dma((n_out,)),
                dma((14,)),
                dma((16,)),
                dma((7,)),
                dma((7,)),
                dma((n_dev // 2,)),
                dma((n_dev // 2,)),
                dma((6,)),
                dma((6,)),
                dma((3, 3)),
                dma((3, 3)),
            ],
            compiler_params=pltpu.CompilerParams(
                collective_id=0, has_side_effects=True, vmem_limit_bytes=67043328),
            name="moe",
        )(x_tok, expert_ids.T, gate_val.T, w_gate, w_up, w_down)

    return jax.shard_map(device_step, mesh=mesh, in_specs=(tok_spec, tok_spec, tok_spec, w_spec, w_spec, w_spec), out_specs=tok_spec, check_vma=False)
```

```python
import functools

import jax
import jax.numpy as jnp
from jax import lax
from jax.experimental import pallas as pl
from jax.experimental.pallas import tpu as pltpu
from jax.sharding import PartitionSpec as P

F32 = jnp.float32
BF16 = jnp.bfloat16
PACK = 5
PAIR = 2
PARTS = [(0,), (1, 2), (3, 4)]


YN, YP, DG, DP = (0, 0, 1), (0, 1, 1), (1, 0, 1), (1, 1, 1)
XN, XP, ME, PC = (1, 0, 0), (1, 1, 0), (0, 0, 0), (0, 1, 0)
ORDER = [YN, YP, XN, XP, ME, PC, DG, DP]


def flip(a, b):
    return tuple((i + j) % 2 for i, j in zip(a, b))


def moe_kernel(dims, x_ref, ids_ref, gates_ref, wg_ref, wu_ref, wd_ref, y_ref,
               x_all, ids_own, gates_own, meta_all, pos_ref, ge_ref, cols_ref, gate_ref, oh_ref, packed, hid_ref, osp, qp_ref, qn_ref,
               c_ref, d_ref, rf_ref, rs_ref, gp_ref, gx_ref, wgu, wdn,
               in_sem, w_sem, o_sem, xs_sem, xr_sem, ms_sem, mr_sem, ds_sem, dr_sem, ts_sem, tr_sem, ns_sem, nr_sem):
    n_loc, n_grp, n_exp, cap, top_k, n_in, n_out = dims
    tok, d_model = x_ref.shape
    half = tok // 2
    own = ORDER.index(ME)
    ff = wg_ref.shape[2]
    n_dev = n_loc * n_grp
    n_tok = tok * n_dev
    rows = n_exp * cap
    l = lax.axis_index("loc")
    g = lax.axis_index("grp")
    gx, gc = g // 2, g % 2

    def dev(to):
        fx, fc, fl = to
        return {"grp": ((gx + fx) % 2) * 2 + (gc + fc) % 2, "loc": (l + fl) % 2}

    def in_copies(e):
        slot = e % n_in
        return (
            pltpu.make_async_copy(wg_ref.at[e], wgu.at[slot, :, pl.ds(0, ff)], w_sem.at[slot, 0]),
            pltpu.make_async_copy(wu_ref.at[e], wgu.at[slot, :, pl.ds(ff, ff)], w_sem.at[slot, 1]),
        )

    def out_copy(e):
        slot = e % n_out
        return pltpu.make_async_copy(wd_ref.at[e], wdn.at[slot], o_sem.at[slot])

    def start_weights(e, carry):
        for copy in in_copies(e):
            copy.start()

        @pl.when(e < n_out)
        def _():
            out_copy(e).start()
        return carry

    loads = [
        pltpu.make_async_copy(src, dst, in_sem.at[i]) for i, (src, dst) in enumerate((
            (x_ref, x_all.at[pl.ds(own * tok, tok), :]), (ids_ref, ids_own), (gates_ref, gates_own)))]
    for copy in loads:
        copy.start()

    peers = [r for r in ORDER if r != ME]
    barrier = pltpu.get_barrier_semaphore()
    for r in peers:
        pl.semaphore_signal(barrier, inc=1, device_id=dev(r), device_id_type=pl.DeviceIdType.MESH)
    lax.fori_loop(0, n_in, start_weights, 0)
    for copy in loads:
        copy.wait()
    meta_all[own] = jnp.zeros_like(meta_all[own])
    meta_all[own, 0:top_k, :] = ids_own[...].astype(F32)
    meta_all[own, 8:8 + top_k, :] = gates_own[...]
    pl.semaphore_wait(barrier, len(peers))

    pending = []

    class Sent:
        def __init__(self, *described):
            self.described = described
            self.copy().start()
            pending.append(self)

        def copy(self):
            src, dst, s_sem, r_sem, to = self.described
            return pltpu.make_async_remote_copy(
                src_ref=src(), dst_ref=dst(), send_sem=s_sem(), recv_sem=r_sem(),
                device_id=dev(to), device_id_type=pl.DeviceIdType.MESH)

        def wait_recv(self):
            self.copy().wait_recv()

        def wait_send(self):
            self.copy().wait_send()

    def send(src, dst, s_sem, r_sem, to):
        return Sent(lambda: src, lambda: dst, lambda: s_sem, lambda: r_sem, to)

    def x_rows(at, part):
        return x_all.at[pl.ds(ORDER.index(at) * tok + part * half, half), :]

    got = {}

    def send_x(src, part, to, at):
        i = len(got)
        got[at, part] = Sent(lambda: x_rows(*src), lambda: x_rows(at, part), lambda: xs_sem.at[i],
                             lambda: xr_sem.at[ORDER.index(at) * 2 + part], to)

    send_x((ME, 0), 0, XN, XN)
    send_x((ME, 1), 1, YN, YN)
    metas = [send(meta_all.at[own], meta_all.at[ORDER.index(r)], ms_sem.at[i], mr_sem.at[i], r)
             for i, r in enumerate(peers)]
    for part, to in ((1, XN), (0, YN), (0, PC), (1, PC)):
        send_x((ME, part), part, to, to)

    def forward(at, part, hops):
        for to in hops:
            send_x((at, part), part, to, flip(at, to))

    def landed(at, part):
        got[at, part].wait_recv()

    landed(XN, 0)
    forward(XN, 0, [YN, PC])
    landed(YN, 1)
    forward(YN, 1, [XN, PC])

    for copy in metas:
        copy.wait_recv()

    ids_t = jnp.concatenate([meta_all[d, 0:8, :] for d in range(n_dev)], axis=1)
    gts_t = jnp.concatenate([meta_all[d, 8:16, :] for d in range(n_dev)], axis=1)
    e_rows = 32
    e_iota = lax.broadcasted_iota(jnp.int32, (e_rows, n_tok), 0)
    e_ids = jnp.where(e_iota < n_exp, e_iota + (g * n_loc + l) * n_exp, -5).astype(F32)
    mask = jnp.zeros((e_rows, n_tok), F32)
    gate_e = jnp.zeros((e_rows, n_tok), F32)
    for j in range(top_k):
        eq = ids_t[j:j + 1, :] == e_ids
        mask = mask + jnp.where(eq, 1.0, 0.0)
        gate_e = gate_e + jnp.where(eq, gts_t[j:j + 1, :], 0.0)
    blocks = [mask[:, d * tok:(d + 1) * tok] for d in range(n_dev)]
    tri = (lax.broadcasted_iota(jnp.int32, (tok, tok), 0) < lax.broadcasted_iota(jnp.int32, (tok, tok), 1))
    tri = jnp.where(tri, 1.0, 0.0).astype(BF16)
    prefix = jnp.dot(jnp.concatenate(blocks, axis=0).astype(BF16), tri, preferred_element_type=F32)
    offset = jnp.zeros((e_rows, 1), F32)
    pos = []
    for d in range(n_dev):
        pos.append(prefix[d * e_rows:(d + 1) * e_rows, :] + offset)
        offset = offset + jnp.sum(blocks[d], axis=1, keepdims=True)
    pos = jnp.concatenate(pos, axis=1)
    pos_ref[...] = jnp.where(mask > 0.0, pos, -1.0)
    ge_ref[...] = gate_e
    slot_id = e_iota.astype(F32) * float(cap) + pos + 1.0
    slot_rows = [jnp.sum(jnp.where(ids_t[j:j + 1, :] == e_ids, slot_id, 0.0), axis=0, keepdims=True) - 1.0
                 for j in range(top_k)]

    def group_hit(grp):
        low = (lax.broadcasted_iota(jnp.int32, (1, n_tok), 1) * 0 + grp * (n_loc * n_exp)).astype(F32)
        hit = jnp.zeros((1, n_tok), F32)
        for j in range(top_k):
            inside = (ids_t[j:j + 1, :] >= low) & (ids_t[j:j + 1, :] < low + float(n_loc * n_exp))
            hit = jnp.where(inside, 1.0, hit)
        return hit

    own_hit = group_hit(g)
    slot_rows += [own_hit, own_hit * group_hit(gx * 2 + (gc + 1) % 2)]
    slot_t = jnp.concatenate(slot_rows, axis=0)
    for d in range(n_dev):
        cols_ref[pl.ds(d * tok, tok), :] = jnp.transpose(slot_t[:, d * tok:(d + 1) * tok])

    def selection(blk):
        cols = cols_ref[pl.ds(pl.multiple_of(blk * tok, tok), tok), :]
        lanes = lax.broadcasted_iota(jnp.int32, (tok, rows), 1).astype(F32)
        hit = cols[:, 0:1] == lanes
        for j in range(1, top_k):
            hit = hit | (cols[:, j:j + 1] == lanes)
        return jnp.where(hit, 1.0, 0.0).astype(BF16)

    qp_ref[...] = selection(ORDER.index(DP))

    step = 256

    def pack(first, count, add, midway, turn):
        toks = pl.ds(first, count)

        def body(p, carry):
            for i in range(PACK):
                e = p * PACK + i
                where = lax.broadcasted_iota(jnp.int32, (cap, count), 0).astype(F32) == pos_ref[pl.ds(e, 1), toks]
                oh_ref[pl.ds(i * cap, cap), pl.ds(0, count)] = jnp.where(where, 1.0, 0.0).astype(BF16)
                gate = jnp.sum(jnp.where(where, ge_ref[pl.ds(e, 1), toks], 0.0), axis=1, keepdims=True)
                at = pl.ds(pl.multiple_of(e * cap, 16), cap)
                gate_ref[at, :] = gate_ref[at, :] + gate if add else gate
            at = pl.ds(pl.multiple_of(p * (PACK * cap), 16), PACK * cap)
            for n in range(d_model // step):
                cols = pl.ds(n * step, step)
                part = jnp.dot(oh_ref[:, pl.ds(0, count)], x_all[toks, cols], preferred_element_type=F32)
                if add:
                    part = part + packed[at, cols].astype(F32)
                packed[at, cols] = part.astype(BF16)
            if midway is not None:
                @pl.when(p == turn)
                def _():
                    midway()
            return carry

        lax.fori_loop(0, n_exp // PACK, body, 0)

    def early():
        landed(XN, 1)
        forward(XN, 1, [PC])
        landed(YN, 0)
        forward(YN, 0, [PC])

    def diagonal():
        for part in (0, 1):
            landed(DG, part)
            forward(DG, part, [PC])

    landed(PC, 0)
    landed(PC, 1)
    pack(4 * tok, 2 * tok, False, early, 0)
    landed(YP, 0)
    landed(YP, 1)
    landed(XP, 0)
    landed(XP, 1)
    pack(0, 4 * tok, True, diagonal, 1)
    landed(DP, 0)
    landed(DP, 1)

    def pack_late(e, count):
        toks = pl.ds(n_tok - 2 * tok, 2 * tok)
        picks = []
        for i in range(count):
            where = lax.broadcasted_iota(jnp.int32, (cap, 2 * tok), 0).astype(F32) == pos_ref[pl.ds(e + i, 1), toks]
            picks.append(jnp.where(where, 1.0, 0.0).astype(BF16))
            at = pl.ds(pl.multiple_of((e + i) * cap, 16), cap)
            gate_ref[at, :] += jnp.sum(jnp.where(where, ge_ref[pl.ds(e + i, 1), toks], 0.0), axis=1, keepdims=True)
        pick = jnp.concatenate(picks, axis=0)
        at = pl.ds(pl.multiple_of(e * cap, 16), count * cap)
        for n in range(d_model // step):
            cols = pl.ds(n * step, step)
            part = jnp.dot(pick, x_all[toks, cols], preferred_element_type=F32)
            packed[at, cols] = (part + packed[at, cols].astype(F32)).astype(BF16)

    pack_late(0, 2 * PAIR)

    def first_dot(e, i):
        at = pl.ds(pl.multiple_of(e * cap, 16), cap)
        uv = jnp.dot(packed[at, :], wgu[e % n_in], preferred_element_type=F32)
        return (jax.nn.silu(uv[:, :ff]) * uv[:, ff:]).astype(BF16)

    def second_dot(hid, e):
        at = pl.ds(pl.multiple_of(e * cap, 16), cap)
        out = jnp.dot(hid, wdn[e % n_out], preferred_element_type=F32) * gate_ref[at, :]
        hi = out.astype(BF16)
        rest = out - hi.astype(F32)
        mid = rest.astype(BF16)
        osp[0, at, :] = hi
        osp[1, at, :] = mid
        osp[2, at, :] = (rest - mid.astype(F32)).astype(BF16)

    def wait_in(e):
        for copy in in_copies(e):
            copy.wait()

    for i in range(PAIR):
        wait_in(i)
    for i in range(PAIR):
        hid_ref[i] = first_dot(i, i)

    def experts(p, late):
        now = [p * PAIR + i for i in range(PAIR)]
        for e in now:
            wait_in(e + PAIR)
            out_copy(e).wait()
        held = [hid_ref[i] for i in range(PAIR)]
        for i, e in enumerate(now):
            second_dot(held[i], e)
            hid_ref[i] = first_dot(e + PAIR, i)
        if late:
            pack_late((p + 2) * PAIR, PAIR)

        for e in now:
            @pl.when(e + PAIR + n_in < n_exp)
            def _():
                for copy in in_copies(e + PAIR + n_in):
                    copy.start()

            @pl.when(e + n_out < n_exp)
            def _():
                out_copy(e + n_out).start()

    for i in range(PAIR):
        if i + n_in < n_exp:
            for copy in in_copies(i + n_in):
                copy.start()
    def turn(p, carry):
        experts(p, True)
        return carry

    lax.fori_loop(0, n_exp // PAIR - 2, turn, 0)
    experts(n_exp // PAIR - 2, False)
    for i in range(PAIR):
        out_copy(n_exp - PAIR + i).wait()
    for i in range(PAIR):
        second_dot(hid_ref[i], n_exp - PAIR + i)

    def combine(q, buf, chunks):
        for n in chunks:
            at = pl.ds(n * step, step)
            total = jnp.dot(q[...], osp[0, :, at], preferred_element_type=F32)
            total += jnp.dot(q[...], osp[1, :, at], preferred_element_type=F32)
            total += jnp.dot(q[...], osp[2, :, at], preferred_element_type=F32)
            c_ref[buf, :, at] = total

    def swap_copy(h):
        return pltpu.make_async_remote_copy(
            src_ref=c_ref.at[n_dev // 2 + (h + 1) % 2], dst_ref=d_ref.at[h], send_sem=ds_sem.at[h], recv_sem=dr_sem.at[h],
            device_id=dev(PC), device_id_type=pl.DeviceIdType.MESH)

    everything = pl.ds(0, d_model)

    def split_rows(h, at):
        cols = cols_ref[pl.ds(pl.multiple_of(2 * h * tok, tok), tok), :]
        mine = c_ref[h, :, at]
        other = d_ref[h, :, at]
        c_ref[h, :, at] = jnp.where(cols[:, 6:7] > 0.5, mine, other)
        d_ref[h, :, at] = jnp.where(cols[:, 7:8] > 0.5, other, 0.0)

    def ship(i, src, dst, to):
        return Sent(src, dst, lambda: ts_sem.at[i], lambda: tr_sem.at[i], to)

    first_far = []
    hop = []
    far = ORDER.index(DG) // 2
    swaps = []
    for i, chunks in enumerate(PARTS):
        at = pl.ds(chunks[0] * step, len(chunks) * step)
        combine(qp_ref, n_dev // 2, chunks)
        swaps.append(send(c_ref.at[n_dev // 2, :, at], d_ref.at[far, :, at], ns_sem.at[i, 0], nr_sem.at[i, 0], PC))
        if i == 0:
            qn_ref[...] = selection(ORDER.index(DG))
        combine(qn_ref, far, chunks)
        swaps[i].wait_recv()
        split_rows(far, at)
        first_far.append(send(c_ref.at[far, :, at], rf_ref.at[1, :, at], ns_sem.at[i, 1], nr_sem.at[i, 1], YN))
        hop.append(send(d_ref.at[far, :, at], rs_ref.at[0, :, at], ns_sem.at[i, 2], nr_sem.at[i, 2], XN))
    for copy in swaps:
        copy.wait_send()
        pending.remove(copy)

    shipped = {}

    def others(i, carry):
        h = i // 2

        @pl.when(i == 4)
        def _():
            swap_copy(0).wait_send()

        qp_ref[...] = selection(i + 1 - 2 * (i % 2))
        combine(qp_ref, (i % 2) * h + (1 - i % 2) * (n_dev // 2 + (h + 1) % 2), range(d_model // step))

        @pl.when(i % 2 == 0)
        def _():
            swap_copy(h).start()

        @pl.when(i % 2 == 1)
        def _():
            swap_copy(h).wait_recv()
            split_rows(h, everything)

        @pl.when(i == 1)
        def _():
            shipped["first_own"] = ship(0, lambda: c_ref.at[0], lambda: rf_ref.at[0], YN)

        @pl.when(i == 3)
        def _():
            shipped["far_second"] = ship(4, lambda: d_ref.at[1], lambda: rs_ref.at[2], XN)
        return carry

    lax.fori_loop(0, n_dev - 2, others, 0)

    for copy in first_far:
        copy.wait_recv()
    gp_ref[...] = (c_ref[1] + rf_ref[1]).astype(BF16)
    far_first = ship(5, lambda: gp_ref, lambda: gx_ref, XN)
    for copy in hop:
        copy.wait_recv()
    d_ref[0] = d_ref[0] + rs_ref[0]
    second = ship(3, lambda: d_ref.at[0], lambda: rs_ref.at[1], YN)

    shipped["first_own"].wait_recv()
    c_ref[2] = (c_ref[2] + rf_ref[0]).astype(BF16).astype(F32)
    shipped["far_second"].wait_recv()
    d_ref[2] = d_ref[2] + rs_ref[2]
    far_first.wait_recv()
    c_ref[2] = c_ref[2] + gx_ref[...].astype(F32)
    second.wait_recv()
    y_ref[...] = (c_ref[2] + (d_ref[2] + rs_ref[1]).astype(BF16).astype(F32)).astype(BF16)
    for copy in pending:
        copy.wait_send()
    for h in range(1, n_dev // 2 - 1):
        swap_copy(h).wait_send()


def solution(mesh):
    n_grp = mesh.shape["grp"]
    n_loc = mesh.shape["loc"]
    tok_spec = P(("part", "grp", "loc"), None)
    w_spec = P(("grp", "loc"), None, None)

    def device_step(x_tok, expert_ids, gate_val, w_gate, w_up, w_down):
        tok, d_model = x_tok.shape
        top_k = expert_ids.shape[1]
        n_exp, _, ff = w_gate.shape
        n_dev = n_grp * n_loc
        n_tok = tok * n_dev
        cap = 8 * (n_tok * top_k // (4 * n_exp * n_dev) + 1)
        rows = n_exp * cap
        n_in, n_out = 11, 10
        vmem = pltpu.VMEM
        dma = pltpu.SemaphoreType.DMA
        dims = (n_loc, n_grp, n_exp, cap, top_k, n_in, n_out)
        return pl.pallas_call(
            functools.partial(moe_kernel, dims),
            out_shape=jax.ShapeDtypeStruct((tok, d_model), BF16),
            in_specs=[pl.BlockSpec(memory_space=pl.ANY)] * 6,
            out_specs=pl.BlockSpec(memory_space=vmem),
            scratch_shapes=[
                vmem((n_tok, d_model), BF16),
                vmem((top_k, tok), jnp.int32),
                vmem((top_k, tok), F32),
                vmem((n_dev, 16, tok), F32),
                vmem((32, n_tok), F32),
                vmem((32, n_tok), F32),
                vmem((n_tok, 8), F32),
                vmem((rows, 1), F32),
                vmem((PACK * cap, n_tok), BF16),
                vmem((rows, d_model), BF16),
                vmem((PAIR, cap, ff), BF16),
                vmem((3, rows, d_model), BF16),
                vmem((tok, rows), BF16),
                vmem((tok, rows), BF16),
                vmem((n_dev // 2 + 2, tok, d_model), F32),
                vmem((n_dev // 2, tok, d_model), F32),
                vmem((2, tok, d_model), F32),
                vmem((3, tok, d_model), F32),
                vmem((tok, d_model), BF16),
                vmem((tok, d_model), BF16),
                vmem((n_in, d_model, 2 * ff), BF16),
                vmem((n_out, ff, d_model), BF16),
                dma((3,)),
                dma((n_in, 2)),
                dma((n_out,)),
                dma((14,)),
                dma((16,)),
                dma((7,)),
                dma((7,)),
                dma((n_dev // 2,)),
                dma((n_dev // 2,)),
                dma((6,)),
                dma((6,)),
                dma((3, 3)),
                dma((3, 3)),
            ],
            compiler_params=pltpu.CompilerParams(
                collective_id=0, has_side_effects=True, vmem_limit_bytes=67043328),
            name="moe",
        )(x_tok, expert_ids.T, gate_val.T, w_gate, w_up, w_down)

    return jax.shard_map(device_step, mesh=mesh, in_specs=(tok_spec, tok_spec, tok_spec, w_spec, w_spec, w_spec), out_specs=tok_spec, check_vma=False)
```

```python
import functools

import jax
import jax.numpy as jnp
from jax import lax
from jax.experimental import pallas as pl
from jax.experimental.pallas import tpu as pltpu
from jax.sharding import PartitionSpec as P

F32 = jnp.float32
BF16 = jnp.bfloat16
PACK = 5
PAIR = 2
PARTS = [(0,), (1, 2), (3, 4)]


YN, YP, DG, DP = (0, 0, 1), (0, 1, 1), (1, 0, 1), (1, 1, 1)
XN, XP, ME, PC = (1, 0, 0), (1, 1, 0), (0, 0, 0), (0, 1, 0)
ORDER = [YN, YP, XN, XP, ME, PC, DG, DP]


def flip(a, b):
    return tuple((i + j) % 2 for i, j in zip(a, b))


def moe_kernel(dims, x_ref, ids_ref, gates_ref, wg_ref, wu_ref, wd_ref, y_ref,
               x_all, ids_own, gates_own, meta_all, pos_ref, ge_ref, cols_ref, gate_ref, oh_ref, packed, hid_ref, osp, qp_ref, qn_ref,
               c_ref, d_ref, rf_ref, rs_ref, gp_ref, gx_ref, wgu, wdn,
               in_sem, w_sem, o_sem, xs_sem, xr_sem, ms_sem, mr_sem, ds_sem, dr_sem, ts_sem, tr_sem, ns_sem, nr_sem):
    n_loc, n_grp, n_exp, cap, top_k, n_in, n_out = dims
    tok, d_model = x_ref.shape
    half = tok // 2
    own = ORDER.index(ME)
    ff = wg_ref.shape[2]
    n_dev = n_loc * n_grp
    n_tok = tok * n_dev
    rows = n_exp * cap
    l = lax.axis_index("loc")
    g = lax.axis_index("grp")
    gx, gc = g // 2, g % 2

    def dev(to):
        fx, fc, fl = to
        return {"grp": ((gx + fx) % 2) * 2 + (gc + fc) % 2, "loc": (l + fl) % 2}

    def in_copies(e):
        slot = e % n_in
        return (
            pltpu.make_async_copy(wg_ref.at[e], wgu.at[slot, :, pl.ds(0, ff)], w_sem.at[slot, 0]),
            pltpu.make_async_copy(wu_ref.at[e], wgu.at[slot, :, pl.ds(ff, ff)], w_sem.at[slot, 1]),
        )

    def out_copy(e):
        slot = e % n_out
        return pltpu.make_async_copy(wd_ref.at[e], wdn.at[slot], o_sem.at[slot])

    def start_weights(e, carry):
        for copy in in_copies(e):
            copy.start()

        @pl.when(e < n_out)
        def _():
            out_copy(e).start()
        return carry

    loads = [
        pltpu.make_async_copy(src, dst, in_sem.at[i]) for i, (src, dst) in enumerate((
            (x_ref, x_all.at[pl.ds(own * tok, tok), :]), (ids_ref, ids_own), (gates_ref, gates_own)))]
    for copy in loads:
        copy.start()

    peers = [r for r in ORDER if r != ME]
    barrier = pltpu.get_barrier_semaphore()
    for r in peers:
        pl.semaphore_signal(barrier, inc=1, device_id=dev(r), device_id_type=pl.DeviceIdType.MESH)
    lax.fori_loop(0, n_in, start_weights, 0)
    for copy in loads:
        copy.wait()
    meta_all[own] = jnp.zeros_like(meta_all[own])
    meta_all[own, 0:top_k, :] = ids_own[...].astype(F32)
    meta_all[own, 8:8 + top_k, :] = gates_own[...]
    pl.semaphore_wait(barrier, len(peers))

    pending = []

    class Sent:
        def __init__(self, *described):
            self.described = described
            self.copy().start()
            pending.append(self)

        def copy(self):
            src, dst, s_sem, r_sem, to = self.described
            return pltpu.make_async_remote_copy(
                src_ref=src(), dst_ref=dst(), send_sem=s_sem(), recv_sem=r_sem(),
                device_id=dev(to), device_id_type=pl.DeviceIdType.MESH)

        def wait_recv(self):
            self.copy().wait_recv()

        def wait_send(self):
            self.copy().wait_send()

    def send(src, dst, s_sem, r_sem, to):
        return Sent(lambda: src, lambda: dst, lambda: s_sem, lambda: r_sem, to)

    def x_rows(at, part):
        return x_all.at[pl.ds(ORDER.index(at) * tok + part * half, half), :]

    got = {}

    def send_x(src, part, to, at):
        i = len(got)
        got[at, part] = Sent(lambda: x_rows(*src), lambda: x_rows(at, part), lambda: xs_sem.at[i],
                             lambda: xr_sem.at[ORDER.index(at) * 2 + part], to)

    send_x((ME, 0), 0, XN, XN)
    send_x((ME, 1), 1, YN, YN)
    metas = [send(meta_all.at[own], meta_all.at[ORDER.index(r)], ms_sem.at[i], mr_sem.at[i], r)
             for i, r in enumerate(peers)]
    for part, to in ((1, XN), (0, YN), (0, PC), (1, PC)):
        send_x((ME, part), part, to, to)

    def forward(at, part, hops):
        for to in hops:
            send_x((at, part), part, to, flip(at, to))

    def landed(at, part):
        got[at, part].wait_recv()

    landed(XN, 0)
    forward(XN, 0, [YN, PC])
    landed(YN, 1)
    forward(YN, 1, [XN, PC])

    for copy in metas:
        copy.wait_recv()

    ids_t = jnp.concatenate([meta_all[d, 0:8, :] for d in range(n_dev)], axis=1)
    gts_t = jnp.concatenate([meta_all[d, 8:16, :] for d in range(n_dev)], axis=1)
    e_rows = 32
    e_iota = lax.broadcasted_iota(jnp.int32, (e_rows, n_tok), 0)
    e_ids = jnp.where(e_iota < n_exp, e_iota + (g * n_loc + l) * n_exp, -5).astype(F32)
    mask = jnp.zeros((e_rows, n_tok), F32)
    gate_e = jnp.zeros((e_rows, n_tok), F32)
    for j in range(top_k):
        eq = ids_t[j:j + 1, :] == e_ids
        mask = mask + jnp.where(eq, 1.0, 0.0)
        gate_e = gate_e + jnp.where(eq, gts_t[j:j + 1, :], 0.0)
    blocks = [mask[:, d * tok:(d + 1) * tok] for d in range(n_dev)]
    tri = (lax.broadcasted_iota(jnp.int32, (tok, tok), 0) < lax.broadcasted_iota(jnp.int32, (tok, tok), 1))
    tri = jnp.where(tri, 1.0, 0.0).astype(BF16)
    prefix = jnp.dot(jnp.concatenate(blocks, axis=0).astype(BF16), tri, preferred_element_type=F32)
    offset = jnp.zeros((e_rows, 1), F32)
    pos = []
    for d in range(n_dev):
        pos.append(prefix[d * e_rows:(d + 1) * e_rows, :] + offset)
        offset = offset + jnp.sum(blocks[d], axis=1, keepdims=True)
    pos = jnp.concatenate(pos, axis=1)
    pos_ref[...] = jnp.where(mask > 0.0, pos, -1.0)
    ge_ref[...] = gate_e
    slot_id = e_iota.astype(F32) * float(cap) + pos + 1.0
    slot_rows = [jnp.sum(jnp.where(ids_t[j:j + 1, :] == e_ids, slot_id, 0.0), axis=0, keepdims=True) - 1.0
                 for j in range(top_k)]

    def group_hit(grp):
        low = (lax.broadcasted_iota(jnp.int32, (1, n_tok), 1) * 0 + grp * (n_loc * n_exp)).astype(F32)
        hit = jnp.zeros((1, n_tok), F32)
        for j in range(top_k):
            inside = (ids_t[j:j + 1, :] >= low) & (ids_t[j:j + 1, :] < low + float(n_loc * n_exp))
            hit = jnp.where(inside, 1.0, hit)
        return hit

    own_hit = group_hit(g)
    slot_rows += [own_hit, own_hit * group_hit(gx * 2 + (gc + 1) % 2)]
    slot_t = jnp.concatenate(slot_rows, axis=0)
    for d in range(n_dev):
        cols_ref[pl.ds(d * tok, tok), :] = jnp.transpose(slot_t[:, d * tok:(d + 1) * tok])

    def selection(blk):
        cols = cols_ref[pl.ds(pl.multiple_of(blk * tok, tok), tok), :]
        lanes = lax.broadcasted_iota(jnp.int32, (tok, rows), 1).astype(F32)
        hit = cols[:, 0:1] == lanes
        for j in range(1, top_k):
            hit = hit | (cols[:, j:j + 1] == lanes)
        return jnp.where(hit, 1.0, 0.0).astype(BF16)

    qp_ref[...] = selection(ORDER.index(DP))

    step = 256

    def pack(first, count, add, midway, turn):
        toks = pl.ds(first, count)

        def body(p, carry):
            for i in range(PACK):
                e = p * PACK + i
                where = lax.broadcasted_iota(jnp.int32, (cap, count), 0).astype(F32) == pos_ref[pl.ds(e, 1), toks]
                oh_ref[pl.ds(i * cap, cap), pl.ds(0, count)] = jnp.where(where, 1.0, 0.0).astype(BF16)
                gate = jnp.sum(jnp.where(where, ge_ref[pl.ds(e, 1), toks], 0.0), axis=1, keepdims=True)
                at = pl.ds(pl.multiple_of(e * cap, 16), cap)
                gate_ref[at, :] = gate_ref[at, :] + gate if add else gate
            at = pl.ds(pl.multiple_of(p * (PACK * cap), 16), PACK * cap)
            for n in range(d_model // step):
                cols = pl.ds(n * step, step)
                part = jnp.dot(oh_ref[:, pl.ds(0, count)], x_all[toks, cols], preferred_element_type=F32)
                if add:
                    part = part + packed[at, cols].astype(F32)
                packed[at, cols] = part.astype(BF16)
            if midway is not None:
                @pl.when(p == turn)
                def _():
                    midway()
            return carry

        lax.fori_loop(0, n_exp // PACK, body, 0)

    def early():
        landed(XN, 1)
        forward(XN, 1, [PC])
        landed(YN, 0)
        forward(YN, 0, [PC])

    def diagonal():
        for part in (0, 1):
            landed(DG, part)
            forward(DG, part, [PC])

    landed(PC, 0)
    landed(PC, 1)
    pack(4 * tok, 2 * tok, False, early, 1)
    landed(YP, 0)
    landed(YP, 1)
    landed(XP, 0)
    landed(XP, 1)
    pack(0, 4 * tok, True, diagonal, 1)
    landed(DP, 0)
    landed(DP, 1)

    def pack_late(e, count):
        toks = pl.ds(n_tok - 2 * tok, 2 * tok)
        picks = []
        for i in range(count):
            where = lax.broadcasted_iota(jnp.int32, (cap, 2 * tok), 0).astype(F32) == pos_ref[pl.ds(e + i, 1), toks]
            picks.append(jnp.where(where, 1.0, 0.0).astype(BF16))
            at = pl.ds(pl.multiple_of((e + i) * cap, 16), cap)
            gate_ref[at, :] += jnp.sum(jnp.where(where, ge_ref[pl.ds(e + i, 1), toks], 0.0), axis=1, keepdims=True)
        pick = jnp.concatenate(picks, axis=0)
        at = pl.ds(pl.multiple_of(e * cap, 16), count * cap)
        for n in range(d_model // step):
            cols = pl.ds(n * step, step)
            part = jnp.dot(pick, x_all[toks, cols], preferred_element_type=F32)
            packed[at, cols] = (part + packed[at, cols].astype(F32)).astype(BF16)

    pack_late(0, 2 * PAIR)

    def first_dot(e, i):
        at = pl.ds(pl.multiple_of(e * cap, 16), cap)
        uv = jnp.dot(packed[at, :], wgu[e % n_in], preferred_element_type=F32)
        return (jax.nn.silu(uv[:, :ff]) * uv[:, ff:]).astype(BF16)

    def second_dot(hid, e):
        at = pl.ds(pl.multiple_of(e * cap, 16), cap)
        out = jnp.dot(hid, wdn[e % n_out], preferred_element_type=F32) * gate_ref[at, :]
        hi = out.astype(BF16)
        rest = out - hi.astype(F32)
        mid = rest.astype(BF16)
        osp[0, at, :] = hi
        osp[1, at, :] = mid
        osp[2, at, :] = (rest - mid.astype(F32)).astype(BF16)

    def wait_in(e):
        for copy in in_copies(e):
            copy.wait()

    for i in range(PAIR):
        wait_in(i)
    for i in range(PAIR):
        hid_ref[i] = first_dot(i, i)

    def experts(p, late):
        now = [p * PAIR + i for i in range(PAIR)]
        for e in now:
            wait_in(e + PAIR)
            out_copy(e).wait()
        held = [hid_ref[i] for i in range(PAIR)]
        for i, e in enumerate(now):
            second_dot(held[i], e)
            hid_ref[i] = first_dot(e + PAIR, i)
        if late:
            pack_late((p + 2) * PAIR, PAIR)

        for e in now:
            @pl.when(e + PAIR + n_in < n_exp)
            def _():
                for copy in in_copies(e + PAIR + n_in):
                    copy.start()

            @pl.when(e + n_out < n_exp)
            def _():
                out_copy(e + n_out).start()

    for i in range(PAIR):
        if i + n_in < n_exp:
            for copy in in_copies(i + n_in):
                copy.start()
    def turn(p, carry):
        experts(p, True)
        return carry

    lax.fori_loop(0, n_exp // PAIR - 2, turn, 0)
    experts(n_exp // PAIR - 2, False)
    for i in range(PAIR):
        out_copy(n_exp - PAIR + i).wait()
    for i in range(PAIR):
        second_dot(hid_ref[i], n_exp - PAIR + i)

    def combine(q, buf, chunks):
        for n in chunks:
            at = pl.ds(n * step, step)
            total = jnp.dot(q[...], osp[0, :, at], preferred_element_type=F32)
            total += jnp.dot(q[...], osp[1, :, at], preferred_element_type=F32)
            total += jnp.dot(q[...], osp[2, :, at], preferred_element_type=F32)
            c_ref[buf, :, at] = total

    def swap_copy(h):
        return pltpu.make_async_remote_copy(
            src_ref=c_ref.at[n_dev // 2 + (h + 1) % 2], dst_ref=d_ref.at[h], send_sem=ds_sem.at[h], recv_sem=dr_sem.at[h],
            device_id=dev(PC), device_id_type=pl.DeviceIdType.MESH)

    everything = pl.ds(0, d_model)

    def split_rows(h, at):
        cols = cols_ref[pl.ds(pl.multiple_of(2 * h * tok, tok), tok), :]
        mine = c_ref[h, :, at]
        other = d_ref[h, :, at]
        c_ref[h, :, at] = jnp.where(cols[:, 6:7] > 0.5, mine, other)
        d_ref[h, :, at] = jnp.where(cols[:, 7:8] > 0.5, other, 0.0)

    def ship(i, src, dst, to):
        return Sent(src, dst, lambda: ts_sem.at[i], lambda: tr_sem.at[i], to)

    first_far = []
    hop = []
    far = ORDER.index(DG) // 2
    swaps = []
    for i, chunks in enumerate(PARTS):
        at = pl.ds(chunks[0] * step, len(chunks) * step)
        combine(qp_ref, n_dev // 2, chunks)
        swaps.append(send(c_ref.at[n_dev // 2, :, at], d_ref.at[far, :, at], ns_sem.at[i, 0], nr_sem.at[i, 0], PC))
        if i == 0:
            qn_ref[...] = selection(ORDER.index(DG))
        combine(qn_ref, far, chunks)
        swaps[i].wait_recv()
        split_rows(far, at)
        first_far.append(send(c_ref.at[far, :, at], rf_ref.at[1, :, at], ns_sem.at[i, 1], nr_sem.at[i, 1], YN))
        hop.append(send(d_ref.at[far, :, at], rs_ref.at[0, :, at], ns_sem.at[i, 2], nr_sem.at[i, 2], XN))
    for copy in swaps:
        copy.wait_send()
        pending.remove(copy)

    shipped = {}

    def others(i, carry):
        h = i // 2

        @pl.when(i == 4)
        def _():
            swap_copy(0).wait_send()

        qp_ref[...] = selection(i + 1 - 2 * (i % 2))
        combine(qp_ref, (i % 2) * h + (1 - i % 2) * (n_dev // 2 + (h + 1) % 2), range(d_model // step))

        @pl.when(i % 2 == 0)
        def _():
            swap_copy(h).start()

        @pl.when(i % 2 == 1)
        def _():
            swap_copy(h).wait_recv()
            split_rows(h, everything)

        @pl.when(i == 1)
        def _():
            shipped["first_own"] = ship(0, lambda: c_ref.at[0], lambda: rf_ref.at[0], YN)

        @pl.when(i == 3)
        def _():
            shipped["far_second"] = ship(4, lambda: d_ref.at[1], lambda: rs_ref.at[2], XN)
        return carry

    lax.fori_loop(0, n_dev - 2, others, 0)

    for copy in first_far:
        copy.wait_recv()
    gp_ref[...] = (c_ref[1] + rf_ref[1]).astype(BF16)
    far_first = ship(5, lambda: gp_ref, lambda: gx_ref, XN)
    for copy in hop:
        copy.wait_recv()
    d_ref[0] = d_ref[0] + rs_ref[0]
    second = ship(3, lambda: d_ref.at[0], lambda: rs_ref.at[1], YN)

    shipped["first_own"].wait_recv()
    c_ref[2] = (c_ref[2] + rf_ref[0]).astype(BF16).astype(F32)
    shipped["far_second"].wait_recv()
    d_ref[2] = d_ref[2] + rs_ref[2]
    far_first.wait_recv()
    c_ref[2] = c_ref[2] + gx_ref[...].astype(F32)
    second.wait_recv()
    y_ref[...] = (c_ref[2] + (d_ref[2] + rs_ref[1]).astype(BF16).astype(F32)).astype(BF16)
    for copy in pending:
        copy.wait_send()
    for h in range(1, n_dev // 2 - 1):
        swap_copy(h).wait_send()


def solution(mesh):
    n_grp = mesh.shape["grp"]
    n_loc = mesh.shape["loc"]
    tok_spec = P(("part", "grp", "loc"), None)
    w_spec = P(("grp", "loc"), None, None)

    def device_step(x_tok, expert_ids, gate_val, w_gate, w_up, w_down):
        tok, d_model = x_tok.shape
        top_k = expert_ids.shape[1]
        n_exp, _, ff = w_gate.shape
        n_dev = n_grp * n_loc
        n_tok = tok * n_dev
        cap = 8 * (n_tok * top_k // (4 * n_exp * n_dev) + 1)
        rows = n_exp * cap
        n_in, n_out = 11, 10
        vmem = pltpu.VMEM
        dma = pltpu.SemaphoreType.DMA
        dims = (n_loc, n_grp, n_exp, cap, top_k, n_in, n_out)
        return pl.pallas_call(
            functools.partial(moe_kernel, dims),
            out_shape=jax.ShapeDtypeStruct((tok, d_model), BF16),
            in_specs=[pl.BlockSpec(memory_space=pl.ANY)] * 6,
            out_specs=pl.BlockSpec(memory_space=vmem),
            scratch_shapes=[
                vmem((n_tok, d_model), BF16),
                vmem((top_k, tok), jnp.int32),
                vmem((top_k, tok), F32),
                vmem((n_dev, 16, tok), F32),
                vmem((32, n_tok), F32),
                vmem((32, n_tok), F32),
                vmem((n_tok, 8), F32),
                vmem((rows, 1), F32),
                vmem((PACK * cap, n_tok), BF16),
                vmem((rows, d_model), BF16),
                vmem((PAIR, cap, ff), BF16),
                vmem((3, rows, d_model), BF16),
                vmem((tok, rows), BF16),
                vmem((tok, rows), BF16),
                vmem((n_dev // 2 + 2, tok, d_model), F32),
                vmem((n_dev // 2, tok, d_model), F32),
                vmem((2, tok, d_model), F32),
                vmem((3, tok, d_model), F32),
                vmem((tok, d_model), BF16),
                vmem((tok, d_model), BF16),
                vmem((n_in, d_model, 2 * ff), BF16),
                vmem((n_out, ff, d_model), BF16),
                dma((3,)),
                dma((n_in, 2)),
                dma((n_out,)),
                dma((14,)),
                dma((16,)),
                dma((7,)),
                dma((7,)),
                dma((n_dev // 2,)),
                dma((n_dev // 2,)),
                dma((6,)),
                dma((6,)),
                dma((3, 3)),
                dma((3, 3)),
            ],
            compiler_params=pltpu.CompilerParams(
                collective_id=0, has_side_effects=True, vmem_limit_bytes=67043328),
            name="moe",
        )(x_tok, expert_ids.T, gate_val.T, w_gate, w_up, w_down)

    return jax.shard_map(device_step, mesh=mesh, in_specs=(tok_spec, tok_spec, tok_spec, w_spec, w_spec, w_spec), out_specs=tok_spec, check_vma=False)
```

```python
import functools

import jax
import jax.numpy as jnp
from jax import lax
from jax.experimental import pallas as pl
from jax.experimental.pallas import tpu as pltpu
from jax.sharding import PartitionSpec as P

F32 = jnp.float32
BF16 = jnp.bfloat16
PACK = 5
PAIR = 2
PARTS = [(0,), (1, 2), (3, 4)]


YN, YP, DG, DP = (0, 0, 1), (0, 1, 1), (1, 0, 1), (1, 1, 1)
XN, XP, ME, PC = (1, 0, 0), (1, 1, 0), (0, 0, 0), (0, 1, 0)
ORDER = [YN, YP, XN, XP, ME, PC, DG, DP]


def flip(a, b):
    return tuple((i + j) % 2 for i, j in zip(a, b))


def moe_kernel(dims, x_ref, ids_ref, gates_ref, wg_ref, wu_ref, wd_ref, y_ref,
               x_all, ids_own, gates_own, meta_all, pos_ref, ge_ref, cols_ref, gate_ref, oh_ref, packed, hid_ref, osp, qp_ref, qn_ref,
               c_ref, d_ref, rf_ref, rs_ref, gp_ref, gx_ref, wgu, wdn,
               in_sem, w_sem, o_sem, xs_sem, xr_sem, ms_sem, mr_sem, ds_sem, dr_sem, ts_sem, tr_sem, ns_sem, nr_sem):
    n_loc, n_grp, n_exp, cap, top_k, n_in, n_out = dims
    tok, d_model = x_ref.shape
    half = tok // 2
    own = ORDER.index(ME)
    ff = wg_ref.shape[2]
    n_dev = n_loc * n_grp
    n_tok = tok * n_dev
    rows = n_exp * cap
    l = lax.axis_index("loc")
    g = lax.axis_index("grp")
    gx, gc = g // 2, g % 2

    def dev(to):
        fx, fc, fl = to
        return {"grp": ((gx + fx) % 2) * 2 + (gc + fc) % 2, "loc": (l + fl) % 2}

    def in_copies(e):
        slot = e % n_in
        return (
            pltpu.make_async_copy(wg_ref.at[e], wgu.at[slot, :, pl.ds(0, ff)], w_sem.at[slot, 0]),
            pltpu.make_async_copy(wu_ref.at[e], wgu.at[slot, :, pl.ds(ff, ff)], w_sem.at[slot, 1]),
        )

    def out_copy(e):
        slot = e % n_out
        return pltpu.make_async_copy(wd_ref.at[e], wdn.at[slot], o_sem.at[slot])

    def start_weights(e, carry):
        for copy in in_copies(e):
            copy.start()

        @pl.when(e < n_out)
        def _():
            out_copy(e).start()
        return carry

    loads = [
        pltpu.make_async_copy(src, dst, in_sem.at[i]) for i, (src, dst) in enumerate((
            (x_ref, x_all.at[pl.ds(own * tok, tok), :]), (ids_ref, ids_own), (gates_ref, gates_own)))]
    for copy in loads:
        copy.start()

    peers = [r for r in ORDER if r != ME]
    barrier = pltpu.get_barrier_semaphore()
    for r in peers:
        pl.semaphore_signal(barrier, inc=1, device_id=dev(r), device_id_type=pl.DeviceIdType.MESH)
    lax.fori_loop(0, n_in, start_weights, 0)
    for copy in loads:
        copy.wait()
    meta_all[own] = jnp.zeros_like(meta_all[own])
    meta_all[own, 0:top_k, :] = ids_own[...].astype(F32)
    meta_all[own, 8:8 + top_k, :] = gates_own[...]
    pl.semaphore_wait(barrier, len(peers))

    pending = []

    class Sent:
        def __init__(self, *described):
            self.described = described
            self.copy().start()
            pending.append(self)

        def copy(self):
            src, dst, s_sem, r_sem, to = self.described
            return pltpu.make_async_remote_copy(
                src_ref=src(), dst_ref=dst(), send_sem=s_sem(), recv_sem=r_sem(),
                device_id=dev(to), device_id_type=pl.DeviceIdType.MESH)

        def wait_recv(self):
            self.copy().wait_recv()

        def wait_send(self):
            self.copy().wait_send()

    def send(src, dst, s_sem, r_sem, to):
        return Sent(lambda: src, lambda: dst, lambda: s_sem, lambda: r_sem, to)

    def x_rows(at, part):
        return x_all.at[pl.ds(ORDER.index(at) * tok + part * half, half), :]

    got = {}

    def send_x(src, part, to, at):
        i = len(got)
        got[at, part] = Sent(lambda: x_rows(*src), lambda: x_rows(at, part), lambda: xs_sem.at[i],
                             lambda: xr_sem.at[ORDER.index(at) * 2 + part], to)

    send_x((ME, 0), 0, XN, XN)
    send_x((ME, 1), 1, YN, YN)
    metas = [send(meta_all.at[own], meta_all.at[ORDER.index(r)], ms_sem.at[i], mr_sem.at[i], r)
             for i, r in enumerate(peers)]
    for part, to in ((1, XN), (0, YN), (0, PC), (1, PC)):
        send_x((ME, part), part, to, to)

    def forward(at, part, hops):
        for to in hops:
            send_x((at, part), part, to, flip(at, to))

    def landed(at, part):
        got[at, part].wait_recv()

    landed(XN, 0)
    forward(XN, 0, [YN, PC])
    landed(YN, 1)
    forward(YN, 1, [XN, PC])

    for copy in metas:
        copy.wait_recv()

    ids_t = jnp.concatenate([meta_all[d, 0:8, :] for d in range(n_dev)], axis=1)
    gts_t = jnp.concatenate([meta_all[d, 8:16, :] for d in range(n_dev)], axis=1)
    e_rows = 32
    e_iota = lax.broadcasted_iota(jnp.int32, (e_rows, n_tok), 0)
    e_ids = jnp.where(e_iota < n_exp, e_iota + (g * n_loc + l) * n_exp, -5).astype(F32)
    mask = jnp.zeros((e_rows, n_tok), F32)
    gate_e = jnp.zeros((e_rows, n_tok), F32)
    for j in range(top_k):
        eq = ids_t[j:j + 1, :] == e_ids
        mask = mask + jnp.where(eq, 1.0, 0.0)
        gate_e = gate_e + jnp.where(eq, gts_t[j:j + 1, :], 0.0)
    blocks = [mask[:, d * tok:(d + 1) * tok] for d in range(n_dev)]
    tri = (lax.broadcasted_iota(jnp.int32, (tok, tok), 0) < lax.broadcasted_iota(jnp.int32, (tok, tok), 1))
    tri = jnp.where(tri, 1.0, 0.0).astype(BF16)
    prefix = jnp.dot(jnp.concatenate(blocks, axis=0).astype(BF16), tri, preferred_element_type=F32)
    offset = jnp.zeros((e_rows, 1), F32)
    pos = []
    for d in range(n_dev):
        pos.append(prefix[d * e_rows:(d + 1) * e_rows, :] + offset)
        offset = offset + jnp.sum(blocks[d], axis=1, keepdims=True)
    pos = jnp.concatenate(pos, axis=1)
    pos_ref[...] = jnp.where(mask > 0.0, pos, -1.0)
    ge_ref[...] = gate_e
    slot_id = e_iota.astype(F32) * float(cap) + pos + 1.0
    slot_rows = [jnp.sum(jnp.where(ids_t[j:j + 1, :] == e_ids, slot_id, 0.0), axis=0, keepdims=True) - 1.0
                 for j in range(top_k)]

    def group_hit(grp):
        low = (lax.broadcasted_iota(jnp.int32, (1, n_tok), 1) * 0 + grp * (n_loc * n_exp)).astype(F32)
        hit = jnp.zeros((1, n_tok), F32)
        for j in range(top_k):
            inside = (ids_t[j:j + 1, :] >= low) & (ids_t[j:j + 1, :] < low + float(n_loc * n_exp))
            hit = jnp.where(inside, 1.0, hit)
        return hit

    own_hit = group_hit(g)
    slot_rows += [own_hit, own_hit * group_hit(gx * 2 + (gc + 1) % 2)]
    slot_t = jnp.concatenate(slot_rows, axis=0)
    for d in range(n_dev):
        cols_ref[pl.ds(d * tok, tok), :] = jnp.transpose(slot_t[:, d * tok:(d + 1) * tok])

    def selection(blk):
        cols = cols_ref[pl.ds(pl.multiple_of(blk * tok, tok), tok), :]
        lanes = lax.broadcasted_iota(jnp.int32, (tok, rows), 1).astype(F32)
        hit = cols[:, 0:1] == lanes
        for j in range(1, top_k):
            hit = hit | (cols[:, j:j + 1] == lanes)
        return jnp.where(hit, 1.0, 0.0).astype(BF16)

    qp_ref[...] = selection(ORDER.index(DP))
    qn_ref[...] = selection(ORDER.index(DG))

    step = 256

    def pack(first, count, add, midway, turn):
        toks = pl.ds(first, count)

        def body(p, carry):
            for i in range(PACK):
                e = p * PACK + i
                where = lax.broadcasted_iota(jnp.int32, (cap, count), 0).astype(F32) == pos_ref[pl.ds(e, 1), toks]
                oh_ref[pl.ds(i * cap, cap), pl.ds(0, count)] = jnp.where(where, 1.0, 0.0).astype(BF16)
                gate = jnp.sum(jnp.where(where, ge_ref[pl.ds(e, 1), toks], 0.0), axis=1, keepdims=True)
                at = pl.ds(pl.multiple_of(e * cap, 16), cap)
                gate_ref[at, :] = gate_ref[at, :] + gate if add else gate
            at = pl.ds(pl.multiple_of(p * (PACK * cap), 16), PACK * cap)
            for n in range(d_model // step):
                cols = pl.ds(n * step, step)
                part = jnp.dot(oh_ref[:, pl.ds(0, count)], x_all[toks, cols], preferred_element_type=F32)
                if add:
                    part = part + packed[at, cols].astype(F32)
                packed[at, cols] = part.astype(BF16)
            if midway is not None:
                @pl.when(p == turn)
                def _():
                    midway()
            return carry

        lax.fori_loop(0, n_exp // PACK, body, 0)

    def early():
        landed(XN, 1)
        forward(XN, 1, [PC])
        landed(YN, 0)
        forward(YN, 0, [PC])

    def diagonal():
        for part in (0, 1):
            landed(DG, part)
            forward(DG, part, [PC])

    landed(PC, 0)
    landed(PC, 1)
    pack(4 * tok, 2 * tok, False, early, 0)
    landed(YP, 0)
    landed(YP, 1)
    landed(XP, 0)
    landed(XP, 1)
    pack(0, 4 * tok, True, diagonal, 0)
    landed(DP, 0)
    landed(DP, 1)

    def pack_late(e, count):
        toks = pl.ds(n_tok - 2 * tok, 2 * tok)
        picks = []
        for i in range(count):
            where = lax.broadcasted_iota(jnp.int32, (cap, 2 * tok), 0).astype(F32) == pos_ref[pl.ds(e + i, 1), toks]
            picks.append(jnp.where(where, 1.0, 0.0).astype(BF16))
            at = pl.ds(pl.multiple_of((e + i) * cap, 16), cap)
            gate_ref[at, :] += jnp.sum(jnp.where(where, ge_ref[pl.ds(e + i, 1), toks], 0.0), axis=1, keepdims=True)
        pick = jnp.concatenate(picks, axis=0)
        at = pl.ds(pl.multiple_of(e * cap, 16), count * cap)
        for n in range(d_model // step):
            cols = pl.ds(n * step, step)
            part = jnp.dot(pick, x_all[toks, cols], preferred_element_type=F32)
            packed[at, cols] = (part + packed[at, cols].astype(F32)).astype(BF16)

    pack_late(0, 2 * PAIR)

    def first_dot(e, i):
        at = pl.ds(pl.multiple_of(e * cap, 16), cap)
        uv = jnp.dot(packed[at, :], wgu[e % n_in], preferred_element_type=F32)
        return (jax.nn.silu(uv[:, :ff]) * uv[:, ff:]).astype(BF16)

    def second_dot(hid, e):
        at = pl.ds(pl.multiple_of(e * cap, 16), cap)
        out = jnp.dot(hid, wdn[e % n_out], preferred_element_type=F32) * gate_ref[at, :]
        hi = out.astype(BF16)
        rest = out - hi.astype(F32)
        mid = rest.astype(BF16)
        osp[0, at, :] = hi
        osp[1, at, :] = mid
        osp[2, at, :] = (rest - mid.astype(F32)).astype(BF16)

    def wait_in(e):
        for copy in in_copies(e):
            copy.wait()

    for i in range(PAIR):
        wait_in(i)
    for i in range(PAIR):
        hid_ref[i] = first_dot(i, i)

    def experts(p, late):
        now = [p * PAIR + i for i in range(PAIR)]
        for e in now:
            wait_in(e + PAIR)
            out_copy(e).wait()
        held = [hid_ref[i] for i in range(PAIR)]
        for i, e in enumerate(now):
            second_dot(held[i], e)
            hid_ref[i] = first_dot(e + PAIR, i)
        if late:
            pack_late((p + 2) * PAIR, PAIR)

        for e in now:
            @pl.when(e + PAIR + n_in < n_exp)
            def _():
                for copy in in_copies(e + PAIR + n_in):
                    copy.start()

            @pl.when(e + n_out < n_exp)
            def _():
                out_copy(e + n_out).start()

    for i in range(PAIR):
        if i + n_in < n_exp:
            for copy in in_copies(i + n_in):
                copy.start()
    def turn(p, carry):
        experts(p, True)
        return carry

    lax.fori_loop(0, n_exp // PAIR - 2, turn, 0)
    experts(n_exp // PAIR - 2, False)
    for i in range(PAIR):
        out_copy(n_exp - PAIR + i).wait()
    for i in range(PAIR):
        second_dot(hid_ref[i], n_exp - PAIR + i)

    def combine(q, buf, chunks):
        for n in chunks:
            at = pl.ds(n * step, step)
            total = jnp.dot(q[...], osp[0, :, at], preferred_element_type=F32)
            total += jnp.dot(q[...], osp[1, :, at], preferred_element_type=F32)
            total += jnp.dot(q[...], osp[2, :, at], preferred_element_type=F32)
            c_ref[buf, :, at] = total

    def swap_copy(h):
        return pltpu.make_async_remote_copy(
            src_ref=c_ref.at[n_dev // 2 + (h + 1) % 2], dst_ref=d_ref.at[h], send_sem=ds_sem.at[h], recv_sem=dr_sem.at[h],
            device_id=dev(PC), device_id_type=pl.DeviceIdType.MESH)

    everything = pl.ds(0, d_model)

    def split_rows(h, at):
        cols = cols_ref[pl.ds(pl.multiple_of(2 * h * tok, tok), tok), :]
        mine = c_ref[h, :, at]
        other = d_ref[h, :, at]
        c_ref[h, :, at] = jnp.where(cols[:, 6:7] > 0.5, mine, other)
        d_ref[h, :, at] = jnp.where(cols[:, 7:8] > 0.5, other, 0.0)

    def ship(i, src, dst, to):
        return Sent(src, dst, lambda: ts_sem.at[i], lambda: tr_sem.at[i], to)

    first_far = []
    hop = []
    far = ORDER.index(DG) // 2
    swaps = []
    for i, chunks in enumerate(PARTS):
        at = pl.ds(chunks[0] * step, len(chunks) * step)
        combine(qp_ref, n_dev // 2, chunks)
        swaps.append(send(c_ref.at[n_dev // 2, :, at], d_ref.at[far, :, at], ns_sem.at[i, 0], nr_sem.at[i, 0], PC))
        combine(qn_ref, far, chunks)
        swaps[i].wait_recv()
        split_rows(far, at)
        first_far.append(send(c_ref.at[far, :, at], rf_ref.at[1, :, at], ns_sem.at[i, 1], nr_sem.at[i, 1], YN))
        hop.append(send(d_ref.at[far, :, at], rs_ref.at[0, :, at], ns_sem.at[i, 2], nr_sem.at[i, 2], XN))
    for copy in swaps:
        copy.wait_send()
        pending.remove(copy)

    shipped = {}

    def others(i, carry):
        h = i // 2

        @pl.when(i == 4)
        def _():
            swap_copy(0).wait_send()

        qp_ref[...] = selection(i + 1 - 2 * (i % 2))
        combine(qp_ref, (i % 2) * h + (1 - i % 2) * (n_dev // 2 + (h + 1) % 2), range(d_model // step))

        @pl.when(i % 2 == 0)
        def _():
            swap_copy(h).start()

        @pl.when(i % 2 == 1)
        def _():
            swap_copy(h).wait_recv()
            split_rows(h, everything)

        @pl.when(i == 1)
        def _():
            shipped["first_own"] = ship(0, lambda: c_ref.at[0], lambda: rf_ref.at[0], YN)

        @pl.when(i == 3)
        def _():
            shipped["far_second"] = ship(4, lambda: d_ref.at[1], lambda: rs_ref.at[2], XN)
        return carry

    lax.fori_loop(0, n_dev - 2, others, 0)

    for copy in first_far:
        copy.wait_recv()
    gp_ref[...] = (c_ref[1] + rf_ref[1]).astype(BF16)
    far_first = ship(5, lambda: gp_ref, lambda: gx_ref, XN)
    for copy in hop:
        copy.wait_recv()
    d_ref[0] = d_ref[0] + rs_ref[0]
    second = ship(3, lambda: d_ref.at[0], lambda: rs_ref.at[1], YN)

    shipped["first_own"].wait_recv()
    c_ref[2] = (c_ref[2] + rf_ref[0]).astype(BF16).astype(F32)
    shipped["far_second"].wait_recv()
    d_ref[2] = d_ref[2] + rs_ref[2]
    far_first.wait_recv()
    c_ref[2] = c_ref[2] + gx_ref[...].astype(F32)
    second.wait_recv()
    y_ref[...] = (c_ref[2] + (d_ref[2] + rs_ref[1]).astype(BF16).astype(F32)).astype(BF16)
    for copy in pending:
        copy.wait_send()
    for h in range(1, n_dev // 2 - 1):
        swap_copy(h).wait_send()


def solution(mesh):
    n_grp = mesh.shape["grp"]
    n_loc = mesh.shape["loc"]
    tok_spec = P(("part", "grp", "loc"), None)
    w_spec = P(("grp", "loc"), None, None)

    def device_step(x_tok, expert_ids, gate_val, w_gate, w_up, w_down):
        tok, d_model = x_tok.shape
        top_k = expert_ids.shape[1]
        n_exp, _, ff = w_gate.shape
        n_dev = n_grp * n_loc
        n_tok = tok * n_dev
        cap = 8 * (n_tok * top_k // (4 * n_exp * n_dev) + 1)
        rows = n_exp * cap
        n_in, n_out = 11, 10
        vmem = pltpu.VMEM
        dma = pltpu.SemaphoreType.DMA
        dims = (n_loc, n_grp, n_exp, cap, top_k, n_in, n_out)
        return pl.pallas_call(
            functools.partial(moe_kernel, dims),
            out_shape=jax.ShapeDtypeStruct((tok, d_model), BF16),
            in_specs=[pl.BlockSpec(memory_space=pl.ANY)] * 6,
            out_specs=pl.BlockSpec(memory_space=vmem),
            scratch_shapes=[
                vmem((n_tok, d_model), BF16),
                vmem((top_k, tok), jnp.int32),
                vmem((top_k, tok), F32),
                vmem((n_dev, 16, tok), F32),
                vmem((32, n_tok), F32),
                vmem((32, n_tok), F32),
                vmem((n_tok, 8), F32),
                vmem((rows, 1), F32),
                vmem((PACK * cap, n_tok), BF16),
                vmem((rows, d_model), BF16),
                vmem((PAIR, cap, ff), BF16),
                vmem((3, rows, d_model), BF16),
                vmem((tok, rows), BF16),
                vmem((tok, rows), BF16),
                vmem((n_dev // 2 + 2, tok, d_model), F32),
                vmem((n_dev // 2, tok, d_model), F32),
                vmem((2, tok, d_model), F32),
                vmem((3, tok, d_model), F32),
                vmem((tok, d_model), BF16),
                vmem((tok, d_model), BF16),
                vmem((n_in, d_model, 2 * ff), BF16),
                vmem((n_out, ff, d_model), BF16),
                dma((3,)),
                dma((n_in, 2)),
                dma((n_out,)),
                dma((14,)),
                dma((16,)),
                dma((7,)),
                dma((7,)),
                dma((n_dev // 2,)),
                dma((n_dev // 2,)),
                dma((6,)),
                dma((6,)),
                dma((3, 3)),
                dma((3, 3)),
            ],
            compiler_params=pltpu.CompilerParams(
                collective_id=0, has_side_effects=True, vmem_limit_bytes=67043328),
            name="moe",
        )(x_tok, expert_ids.T, gate_val.T, w_gate, w_up, w_down)

    return jax.shard_map(device_step, mesh=mesh, in_specs=(tok_spec, tok_spec, tok_spec, w_spec, w_spec, w_spec), out_specs=tok_spec, check_vma=False)
```

```python
import functools

import jax
import jax.numpy as jnp
from jax import lax
from jax.experimental import pallas as pl
from jax.experimental.pallas import tpu as pltpu
from jax.sharding import PartitionSpec as P

F32 = jnp.float32
BF16 = jnp.bfloat16
PACK = 5
PAIR = 2
PARTS = [(0,), (1, 2), (3, 4)]


YN, YP, DG, DP = (0, 0, 1), (0, 1, 1), (1, 0, 1), (1, 1, 1)
XN, XP, ME, PC = (1, 0, 0), (1, 1, 0), (0, 0, 0), (0, 1, 0)
ORDER = [YN, YP, XN, XP, ME, PC, DG, DP]


def flip(a, b):
    return tuple((i + j) % 2 for i, j in zip(a, b))


def moe_kernel(dims, x_ref, ids_ref, gates_ref, wg_ref, wu_ref, wd_ref, y_ref,
               x_all, ids_own, gates_own, meta_all, pos_ref, ge_ref, cols_ref, gate_ref, oh_ref, packed, hid_ref, osp, qp_ref, qn_ref,
               c_ref, d_ref, rf_ref, rs_ref, gp_ref, gx_ref, wgu, wdn,
               in_sem, w_sem, o_sem, xs_sem, xr_sem, ms_sem, mr_sem, ds_sem, dr_sem, ts_sem, tr_sem, ns_sem, nr_sem):
    n_loc, n_grp, n_exp, cap, top_k, n_in, n_out = dims
    tok, d_model = x_ref.shape
    half = tok // 2
    own = ORDER.index(ME)
    ff = wg_ref.shape[2]
    n_dev = n_loc * n_grp
    n_tok = tok * n_dev
    rows = n_exp * cap
    l = lax.axis_index("loc")
    g = lax.axis_index("grp")
    gx, gc = g // 2, g % 2

    def dev(to):
        fx, fc, fl = to
        return {"grp": ((gx + fx) % 2) * 2 + (gc + fc) % 2, "loc": (l + fl) % 2}

    def in_copies(e):
        slot = e % n_in
        return (
            pltpu.make_async_copy(wg_ref.at[e], wgu.at[slot, :, pl.ds(0, ff)], w_sem.at[slot, 0]),
            pltpu.make_async_copy(wu_ref.at[e], wgu.at[slot, :, pl.ds(ff, ff)], w_sem.at[slot, 1]),
        )

    def out_copy(e):
        slot = e % n_out
        return pltpu.make_async_copy(wd_ref.at[e], wdn.at[slot], o_sem.at[slot])

    def start_weights(e, carry):
        for copy in in_copies(e):
            copy.start()

        @pl.when(e < n_out)
        def _():
            out_copy(e).start()
        return carry

    loads = [
        pltpu.make_async_copy(src, dst, in_sem.at[i]) for i, (src, dst) in enumerate((
            (x_ref, x_all.at[pl.ds(own * tok, tok), :]), (ids_ref, ids_own), (gates_ref, gates_own)))]
    for copy in loads:
        copy.start()

    peers = [r for r in ORDER if r != ME]
    barrier = pltpu.get_barrier_semaphore()
    for r in peers:
        pl.semaphore_signal(barrier, inc=1, device_id=dev(r), device_id_type=pl.DeviceIdType.MESH)
    lax.fori_loop(0, n_in, start_weights, 0)
    for copy in loads:
        copy.wait()
    meta_all[own] = jnp.zeros_like(meta_all[own])
    meta_all[own, 0:top_k, :] = ids_own[...].astype(F32)
    meta_all[own, 8:8 + top_k, :] = gates_own[...]
    pl.semaphore_wait(barrier, len(peers))

    pending = []

    class Sent:
        def __init__(self, *described):
            self.described = described
            self.copy().start()
            pending.append(self)

        def copy(self):
            src, dst, s_sem, r_sem, to = self.described
            return pltpu.make_async_remote_copy(
                src_ref=src(), dst_ref=dst(), send_sem=s_sem(), recv_sem=r_sem(),
                device_id=dev(to), device_id_type=pl.DeviceIdType.MESH)

        def wait_recv(self):
            self.copy().wait_recv()

        def wait_send(self):
            self.copy().wait_send()

    def send(src, dst, s_sem, r_sem, to):
        return Sent(lambda: src, lambda: dst, lambda: s_sem, lambda: r_sem, to)

    def x_rows(at, part):
        return x_all.at[pl.ds(ORDER.index(at) * tok + part * half, half), :]

    got = {}

    def send_x(src, part, to, at):
        i = len(got)
        got[at, part] = Sent(lambda: x_rows(*src), lambda: x_rows(at, part), lambda: xs_sem.at[i],
                             lambda: xr_sem.at[ORDER.index(at) * 2 + part], to)

    send_x((ME, 0), 0, XN, XN)
    send_x((ME, 1), 1, YN, YN)
    metas = [send(meta_all.at[own], meta_all.at[ORDER.index(r)], ms_sem.at[i], mr_sem.at[i], r)
             for i, r in enumerate(peers)]
    for part, to in ((1, XN), (0, YN), (0, PC), (1, PC)):
        send_x((ME, part), part, to, to)

    def forward(at, part, hops):
        for to in hops:
            send_x((at, part), part, to, flip(at, to))

    def landed(at, part):
        got[at, part].wait_recv()

    landed(XN, 0)
    forward(XN, 0, [YN, PC])
    landed(YN, 1)
    forward(YN, 1, [XN, PC])

    for copy in metas:
        copy.wait_recv()

    ids_t = jnp.concatenate([meta_all[d, 0:8, :] for d in range(n_dev)], axis=1)
    gts_t = jnp.concatenate([meta_all[d, 8:16, :] for d in range(n_dev)], axis=1)
    e_rows = 32
    e_iota = lax.broadcasted_iota(jnp.int32, (e_rows, n_tok), 0)
    e_ids = jnp.where(e_iota < n_exp, e_iota + (g * n_loc + l) * n_exp, -5).astype(F32)
    mask = jnp.zeros((e_rows, n_tok), F32)
    gate_e = jnp.zeros((e_rows, n_tok), F32)
    for j in range(top_k):
        eq = ids_t[j:j + 1, :] == e_ids
        mask = mask + jnp.where(eq, 1.0, 0.0)
        gate_e = gate_e + jnp.where(eq, gts_t[j:j + 1, :], 0.0)
    blocks = [mask[:, d * tok:(d + 1) * tok] for d in range(n_dev)]
    tri = (lax.broadcasted_iota(jnp.int32, (tok, tok), 0) < lax.broadcasted_iota(jnp.int32, (tok, tok), 1))
    tri = jnp.where(tri, 1.0, 0.0).astype(BF16)
    prefix = jnp.dot(jnp.concatenate(blocks, axis=0).astype(BF16), tri, preferred_element_type=F32)
    offset = jnp.zeros((e_rows, 1), F32)
    pos = []
    for d in range(n_dev):
        pos.append(prefix[d * e_rows:(d + 1) * e_rows, :] + offset)
        offset = offset + jnp.sum(blocks[d], axis=1, keepdims=True)
    pos = jnp.concatenate(pos, axis=1)
    pos_ref[...] = jnp.where(mask > 0.0, pos, -1.0)
    ge_ref[...] = gate_e
    slot_id = e_iota.astype(F32) * float(cap) + pos + 1.0
    slot_rows = [jnp.sum(jnp.where(ids_t[j:j + 1, :] == e_ids, slot_id, 0.0), axis=0, keepdims=True) - 1.0
                 for j in range(top_k)]

    def group_hit(grp):
        low = (lax.broadcasted_iota(jnp.int32, (1, n_tok), 1) * 0 + grp * (n_loc * n_exp)).astype(F32)
        hit = jnp.zeros((1, n_tok), F32)
        for j in range(top_k):
            inside = (ids_t[j:j + 1, :] >= low) & (ids_t[j:j + 1, :] < low + float(n_loc * n_exp))
            hit = jnp.where(inside, 1.0, hit)
        return hit

    own_hit = group_hit(g)
    slot_rows += [own_hit, own_hit * group_hit(gx * 2 + (gc + 1) % 2)]
    slot_t = jnp.concatenate(slot_rows, axis=0)
    for d in range(n_dev):
        cols_ref[pl.ds(d * tok, tok), :] = jnp.transpose(slot_t[:, d * tok:(d + 1) * tok])

    def selection(blk):
        cols = cols_ref[pl.ds(pl.multiple_of(blk * tok, tok), tok), :]
        lanes = lax.broadcasted_iota(jnp.int32, (tok, rows), 1).astype(F32)
        hit = cols[:, 0:1] == lanes
        for j in range(1, top_k):
            hit = hit | (cols[:, j:j + 1] == lanes)
        return jnp.where(hit, 1.0, 0.0).astype(BF16)

    qp_ref[...] = selection(ORDER.index(DP))
    qn_ref[...] = selection(ORDER.index(DG))

    step = 256

    def pack(first, count, add, midway, turn):
        toks = pl.ds(first, count)

        def body(p, carry):
            for i in range(PACK):
                e = p * PACK + i
                where = lax.broadcasted_iota(jnp.int32, (cap, count), 0).astype(F32) == pos_ref[pl.ds(e, 1), toks]
                oh_ref[pl.ds(i * cap, cap), pl.ds(0, count)] = jnp.where(where, 1.0, 0.0).astype(BF16)
                gate = jnp.sum(jnp.where(where, ge_ref[pl.ds(e, 1), toks], 0.0), axis=1, keepdims=True)
                at = pl.ds(pl.multiple_of(e * cap, 16), cap)
                gate_ref[at, :] = gate_ref[at, :] + gate if add else gate
            at = pl.ds(pl.multiple_of(p * (PACK * cap), 16), PACK * cap)
            for n in range(d_model // step):
                cols = pl.ds(n * step, step)
                part = jnp.dot(oh_ref[:, pl.ds(0, count)], x_all[toks, cols], preferred_element_type=F32)
                if add:
                    part = part + packed[at, cols].astype(F32)
                packed[at, cols] = part.astype(BF16)
            if midway is not None:
                @pl.when(p == turn)
                def _():
                    midway()
            return carry

        lax.fori_loop(0, n_exp // PACK, body, 0)

    def early():
        landed(XN, 1)
        forward(XN, 1, [PC])
        landed(YN, 0)
        forward(YN, 0, [PC])

    def diagonal():
        for part in (0, 1):
            landed(DG, part)
            forward(DG, part, [PC])

    landed(PC, 0)
    landed(PC, 1)
    pack(4 * tok, 2 * tok, False, early, 1)
    landed(YP, 0)
    landed(YP, 1)
    landed(XP, 0)
    landed(XP, 1)
    pack(0, 4 * tok, True, diagonal, 2)
    landed(DP, 0)
    landed(DP, 1)

    def pack_late(e, count):
        toks = pl.ds(n_tok - 2 * tok, 2 * tok)
        picks = []
        for i in range(count):
            where = lax.broadcasted_iota(jnp.int32, (cap, 2 * tok), 0).astype(F32) == pos_ref[pl.ds(e + i, 1), toks]
            picks.append(jnp.where(where, 1.0, 0.0).astype(BF16))
            at = pl.ds(pl.multiple_of((e + i) * cap, 16), cap)
            gate_ref[at, :] += jnp.sum(jnp.where(where, ge_ref[pl.ds(e + i, 1), toks], 0.0), axis=1, keepdims=True)
        pick = jnp.concatenate(picks, axis=0)
        at = pl.ds(pl.multiple_of(e * cap, 16), count * cap)
        for n in range(d_model // step):
            cols = pl.ds(n * step, step)
            part = jnp.dot(pick, x_all[toks, cols], preferred_element_type=F32)
            packed[at, cols] = (part + packed[at, cols].astype(F32)).astype(BF16)

    pack_late(0, 2 * PAIR)

    def first_dot(e, i):
        at = pl.ds(pl.multiple_of(e * cap, 16), cap)
        uv = jnp.dot(packed[at, :], wgu[e % n_in], preferred_element_type=F32)
        return (jax.nn.silu(uv[:, :ff]) * uv[:, ff:]).astype(BF16)

    def second_dot(hid, e):
        at = pl.ds(pl.multiple_of(e * cap, 16), cap)
        out = jnp.dot(hid, wdn[e % n_out], preferred_element_type=F32) * gate_ref[at, :]
        hi = out.astype(BF16)
        rest = out - hi.astype(F32)
        mid = rest.astype(BF16)
        osp[0, at, :] = hi
        osp[1, at, :] = mid
        osp[2, at, :] = (rest - mid.astype(F32)).astype(BF16)

    def wait_in(e):
        for copy in in_copies(e):
            copy.wait()

    for i in range(PAIR):
        wait_in(i)
    for i in range(PAIR):
        hid_ref[i] = first_dot(i, i)

    def experts(p, late):
        now = [p * PAIR + i for i in range(PAIR)]
        for e in now:
            wait_in(e + PAIR)
            out_copy(e).wait()
        held = [hid_ref[i] for i in range(PAIR)]
        for i, e in enumerate(now):
            second_dot(held[i], e)
            hid_ref[i] = first_dot(e + PAIR, i)
        if late:
            pack_late((p + 2) * PAIR, PAIR)

        for e in now:
            @pl.when(e + PAIR + n_in < n_exp)
            def _():
                for copy in in_copies(e + PAIR + n_in):
                    copy.start()

            @pl.when(e + n_out < n_exp)
            def _():
                out_copy(e + n_out).start()

    for i in range(PAIR):
        if i + n_in < n_exp:
            for copy in in_copies(i + n_in):
                copy.start()
    def turn(p, carry):
        experts(p, True)
        return carry

    lax.fori_loop(0, n_exp // PAIR - 2, turn, 0)
    experts(n_exp // PAIR - 2, False)
    for i in range(PAIR):
        out_copy(n_exp - PAIR + i).wait()
    for i in range(PAIR):
        second_dot(hid_ref[i], n_exp - PAIR + i)

    def combine(q, buf, chunks):
        for n in chunks:
            at = pl.ds(n * step, step)
            total = jnp.dot(q[...], osp[0, :, at], preferred_element_type=F32)
            total += jnp.dot(q[...], osp[1, :, at], preferred_element_type=F32)
            total += jnp.dot(q[...], osp[2, :, at], preferred_element_type=F32)
            c_ref[buf, :, at] = total

    def swap_copy(h):
        return pltpu.make_async_remote_copy(
            src_ref=c_ref.at[n_dev // 2 + (h + 1) % 2], dst_ref=d_ref.at[h], send_sem=ds_sem.at[h], recv_sem=dr_sem.at[h],
            device_id=dev(PC), device_id_type=pl.DeviceIdType.MESH)

    everything = pl.ds(0, d_model)

    def split_rows(h, at):
        cols = cols_ref[pl.ds(pl.multiple_of(2 * h * tok, tok), tok), :]
        mine = c_ref[h, :, at]
        other = d_ref[h, :, at]
        c_ref[h, :, at] = jnp.where(cols[:, 6:7] > 0.5, mine, other)
        d_ref[h, :, at] = jnp.where(cols[:, 7:8] > 0.5, other, 0.0)

    def ship(i, src, dst, to):
        return Sent(src, dst, lambda: ts_sem.at[i], lambda: tr_sem.at[i], to)

    first_far = []
    hop = []
    far = ORDER.index(DG) // 2
    swaps = []
    for i, chunks in enumerate(PARTS):
        at = pl.ds(chunks[0] * step, len(chunks) * step)
        combine(qp_ref, n_dev // 2, chunks)
        swaps.append(send(c_ref.at[n_dev // 2, :, at], d_ref.at[far, :, at], ns_sem.at[i, 0], nr_sem.at[i, 0], PC))
        combine(qn_ref, far, chunks)
        swaps[i].wait_recv()
        split_rows(far, at)
        first_far.append(send(c_ref.at[far, :, at], rf_ref.at[1, :, at], ns_sem.at[i, 1], nr_sem.at[i, 1], YN))
        hop.append(send(d_ref.at[far, :, at], rs_ref.at[0, :, at], ns_sem.at[i, 2], nr_sem.at[i, 2], XN))
    for copy in swaps:
        copy.wait_send()
        pending.remove(copy)

    shipped = {}

    def others(i, carry):
        h = i // 2

        @pl.when(i == 4)
        def _():
            swap_copy(0).wait_send()

        qp_ref[...] = selection(i + 1 - 2 * (i % 2))
        combine(qp_ref, (i % 2) * h + (1 - i % 2) * (n_dev // 2 + (h + 1) % 2), range(d_model // step))

        @pl.when(i % 2 == 0)
        def _():
            swap_copy(h).start()

        @pl.when(i % 2 == 1)
        def _():
            swap_copy(h).wait_recv()
            split_rows(h, everything)

        @pl.when(i == 1)
        def _():
            shipped["first_own"] = ship(0, lambda: c_ref.at[0], lambda: rf_ref.at[0], YN)

        @pl.when(i == 3)
        def _():
            shipped["far_second"] = ship(4, lambda: d_ref.at[1], lambda: rs_ref.at[2], XN)
        return carry

    lax.fori_loop(0, n_dev - 2, others, 0)

    for copy in first_far:
        copy.wait_recv()
    gp_ref[...] = (c_ref[1] + rf_ref[1]).astype(BF16)
    far_first = ship(5, lambda: gp_ref, lambda: gx_ref, XN)
    for copy in hop:
        copy.wait_recv()
    d_ref[0] = d_ref[0] + rs_ref[0]
    second = ship(3, lambda: d_ref.at[0], lambda: rs_ref.at[1], YN)

    shipped["first_own"].wait_recv()
    c_ref[2] = (c_ref[2] + rf_ref[0]).astype(BF16).astype(F32)
    shipped["far_second"].wait_recv()
    d_ref[2] = d_ref[2] + rs_ref[2]
    far_first.wait_recv()
    c_ref[2] = c_ref[2] + gx_ref[...].astype(F32)
    second.wait_recv()
    y_ref[...] = (c_ref[2] + (d_ref[2] + rs_ref[1]).astype(BF16).astype(F32)).astype(BF16)
    for copy in pending:
        copy.wait_send()
    for h in range(1, n_dev // 2 - 1):
        swap_copy(h).wait_send()


def solution(mesh):
    n_grp = mesh.shape["grp"]
    n_loc = mesh.shape["loc"]
    tok_spec = P(("part", "grp", "loc"), None)
    w_spec = P(("grp", "loc"), None, None)

    def device_step(x_tok, expert_ids, gate_val, w_gate, w_up, w_down):
        tok, d_model = x_tok.shape
        top_k = expert_ids.shape[1]
        n_exp, _, ff = w_gate.shape
        n_dev = n_grp * n_loc
        n_tok = tok * n_dev
        cap = 8 * (n_tok * top_k // (4 * n_exp * n_dev) + 1)
        rows = n_exp * cap
        n_in, n_out = 11, 10
        vmem = pltpu.VMEM
        dma = pltpu.SemaphoreType.DMA
        dims = (n_loc, n_grp, n_exp, cap, top_k, n_in, n_out)
        return pl.pallas_call(
            functools.partial(moe_kernel, dims),
            out_shape=jax.ShapeDtypeStruct((tok, d_model), BF16),
            in_specs=[pl.BlockSpec(memory_space=pl.ANY)] * 6,
            out_specs=pl.BlockSpec(memory_space=vmem),
            scratch_shapes=[
                vmem((n_tok, d_model), BF16),
                vmem((top_k, tok), jnp.int32),
                vmem((top_k, tok), F32),
                vmem((n_dev, 16, tok), F32),
                vmem((32, n_tok), F32),
                vmem((32, n_tok), F32),
                vmem((n_tok, 8), F32),
                vmem((rows, 1), F32),
                vmem((PACK * cap, n_tok), BF16),
                vmem((rows, d_model), BF16),
                vmem((PAIR, cap, ff), BF16),
                vmem((3, rows, d_model), BF16),
                vmem((tok, rows), BF16),
                vmem((tok, rows), BF16),
                vmem((n_dev // 2 + 2, tok, d_model), F32),
                vmem((n_dev // 2, tok, d_model), F32),
                vmem((2, tok, d_model), F32),
                vmem((3, tok, d_model), F32),
                vmem((tok, d_model), BF16),
                vmem((tok, d_model), BF16),
                vmem((n_in, d_model, 2 * ff), BF16),
                vmem((n_out, ff, d_model), BF16),
                dma((3,)),
                dma((n_in, 2)),
                dma((n_out,)),
                dma((14,)),
                dma((16,)),
                dma((7,)),
                dma((7,)),
                dma((n_dev // 2,)),
                dma((n_dev // 2,)),
                dma((6,)),
                dma((6,)),
                dma((3, 3)),
                dma((3, 3)),
            ],
            compiler_params=pltpu.CompilerParams(
                collective_id=0, has_side_effects=True, vmem_limit_bytes=67043328),
            name="moe",
        )(x_tok, expert_ids.T, gate_val.T, w_gate, w_up, w_down)

    return jax.shard_map(device_step, mesh=mesh, in_specs=(tok_spec, tok_spec, tok_spec, w_spec, w_spec, w_spec), out_specs=tok_spec, check_vma=False)
```
